512 devices in a mesh: batch: 8 (over y_lo, x), rows: 8 (over z), chan: 8 (over y_hi, core).
Axes of the slice: x: 4, y: 8 (y_hi: 4, y_lo: 2; y = y_hi * 2 + y_lo), z: 8, core: 2. Of those that a mesh axis runs over, the one named last changes fastest.
Arguments:
- images: float32 [64, 24, 64, 32], P('batch', None, ('rows', 'chan')), may hold values from -6 to 6
- shift_mid: float32 [3, 24], replicated, may hold values from -1.75 to 1.75
- gain_mid: float32 [3, 24], replicated, may hold values from -0.3 to 0.3
- lower_mid: float32 [3, 24, 24], replicated, may hold values from -1.25 to 1.25
- upper_mid: float32 [3, 24, 24], replicated, may hold values from -1.25 to 1.25
- diag_mid: float32 [3, 24], replicated, may hold values from -0.3 to 0.3
- first_mid: bfloat16 [3, 9, 12, 512], replicated, may hold values from -0.625 to 0.625
- first_bias_mid: bfloat16 [3, 512], replicated, may hold values from -3 to 3
- second_mid: bfloat16 [3, 512, 512], replicated, may hold values from -0.25 to 0.25
- second_bias_mid: float32 [3, 512], replicated, may hold values from -3 to 3
- third_mid: bfloat16 [3, 9, 512, 24], replicated, may hold values from -0.09375 to 0.09375
- third_bias_mid: float32 [3, 24], replicated, may hold values from -3 to 3
- shift_top: float32 [2, 48], replicated, may hold values from -1.75 to 1.75
- gain_top: float32 [2, 48], replicated, may hold values from -0.3 to 0.3
- lower_top: float32 [2, 48, 48], replicated, may hold values from -0.875 to 0.875
- upper_top: float32 [2, 48, 48], replicated, may hold values from -0.875 to 0.875
- diag_top: float32 [2, 48], replicated, may hold values from -0.3 to 0.3
- first_top: bfloat16 [2, 9, 24, 512], replicated, may hold values from -0.4375 to 0.4375
- first_bias_top: bfloat16 [2, 512], replicated, may hold values from -3 to 3
- second_top: bfloat16 [2, 512, 512], replicated, may hold values from -0.25 to 0.25
- second_bias_top: float32 [2, 512], replicated, may hold values from -3 to 3
- third_top: bfloat16 [2, 9, 512, 48], replicated, may hold values from -0.09375 to 0.09375
- third_bias_top: float32 [2, 48], replicated, may hold values from -3 to 3
Outputs:
- latent_mid: float32 [64, 12, 64, 32], P('batch', None, ('rows', 'chan'))
- latent_top: float32 [64, 48, 32, 16], P(('batch', 'chan'), None, 'rows')
- loglik: float32 [64], P(('batch', 'chan'))
The draws below stay inside these ranges and needn't reach their ends.
All inputs are finite; a program needn't handle non-finite values.
Results may differ from the reference program's by a relative error of at most 0.008.
Values may be sent and summed in bfloat16 or wider, within the bound.
A program may use at most 64 MiB of HBM per device.

```python
import math
import jax
import jax.numpy as jnp
from jax import lax

HID = 512
C2 = 24
W2 = 32
STEPS2 = 3
STEPS3 = 2
B = 64
H2 = 64
C3 = 48


def level_of(rng, extent, split, least, high):
    gain, own = 1.0, jax.random.fold_in(rng, 6)
    for axis_at, shards_of in split:
        draws = jnp.exp(jax.random.uniform(jax.random.fold_in(own, axis_at), (shards_of,), jnp.float32, least / len(split), high / len(split)))
        gain = gain * jnp.repeat(draws, extent[axis_at] // shards_of).reshape([-1 if axis == axis_at else 1 for axis in range(len(extent))])
    return gain


def centred(rng, dims, width, bound, shards=(), held_as=jnp.bfloat16):
    array = width * jax.random.normal(rng, dims, jnp.float32)
    if shards:
        array = array * level_of(rng, dims, shards, -0.22, 0.18)
    return jnp.clip(array, -bound, bound).astype(held_as)


def setup_inputs(seed: int = 0) -> dict:
    keys = jax.random.split(jax.random.key(seed), 24)
    return {
        "images": centred(keys[0], (B, C2, H2, W2), 1.0, 6.0, ((0, 8), (2, 64)), jnp.float32),
        "shift_mid": centred(keys[1], (STEPS2, C2), 0.3, 1.75, (), jnp.float32),
        "gain_mid": jnp.clip(jax.random.uniform(keys[2], (STEPS2, C2), jnp.float32, -0.3, 0.3), -0.3, 0.3),
        "lower_mid": centred(keys[3], (STEPS2, C2, C2), C2 ** -0.5, 1.25, (), jnp.float32),
        "upper_mid": centred(keys[4], (STEPS2, C2, C2), C2 ** -0.5, 1.25, (), jnp.float32),
        "diag_mid": jnp.clip(jax.random.uniform(keys[5], (STEPS2, C2), jnp.float32, -0.3, 0.3), -0.3, 0.3),
        "first_mid": centred(keys[6], (STEPS2, 9, C2 // 2, HID), (9 * C2 // 2) ** -0.5, 0.625),
        "first_bias_mid": centred(keys[7], (STEPS2, HID), 0.5, 3.0),
        "second_mid": centred(keys[8], (STEPS2, HID, HID), HID ** -0.5, 0.25),
        "second_bias_mid": centred(keys[9], (STEPS2, HID), 0.5, 3.0, (), jnp.float32),
        "third_mid": centred(keys[10], (STEPS2, 9, HID, C2), (9 * HID) ** -0.5, 0.09375),
        "third_bias_mid": centred(keys[11], (STEPS2, C2), 0.5, 3.0, (), jnp.float32),
        "shift_top": centred(keys[12], (STEPS3, C3), 0.3, 1.75, (), jnp.float32),
        "gain_top": jnp.clip(jax.random.uniform(keys[13], (STEPS3, C3), jnp.float32, -0.3, 0.3), -0.3, 0.3),
        "lower_top": centred(keys[14], (STEPS3, C3, C3), C3 ** -0.5, 0.875, (), jnp.float32),
        "upper_top": centred(keys[15], (STEPS3, C3, C3), C3 ** -0.5, 0.875, (), jnp.float32),
        "diag_top": jnp.clip(jax.random.uniform(keys[16], (STEPS3, C3), jnp.float32, -0.3, 0.3), -0.3, 0.3),
        "first_top": centred(keys[17], (STEPS3, 9, C2, HID), (9 * C2) ** -0.5, 0.4375),
        "first_bias_top": centred(keys[18], (STEPS3, HID), 0.5, 3.0),
        "second_top": centred(keys[19], (STEPS3, HID, HID), HID ** -0.5, 0.25),
        "second_bias_top": centred(keys[20], (STEPS3, HID), 0.5, 3.0, (), jnp.float32),
        "third_top": centred(keys[21], (STEPS3, 9, HID, C3), (9 * HID) ** -0.5, 0.09375),
        "third_bias_top": centred(keys[22], (STEPS3, C3), 0.5, 3.0, (), jnp.float32),
    }


log_two_pi = math.log(2.0 * math.pi)


def spatial_conv(source, weights):
    height = source.shape[1]
    columns = source.shape[2]
    padded = jnp.pad(source, ((0, 0), (1, 1), (1, 1))).astype(jnp.float32)
    summed = jnp.zeros((weights.shape[2], height, columns), jnp.float32)
    for tap_idx in range(9):
        row_off = tap_idx // 3
        col_off = tap_idx % 3
        window = padded[:, row_off:row_off + height, col_off:col_off + columns]
        summed = summed + jnp.einsum('chw,co->ohw', window, weights[tap_idx].astype(jnp.float32))
    return summed


def flow_step(flow_state, params):
    shift_vec, gain_vec, lower_raw, upper_raw, diag_log, first_w, first_b, second_w, second_b, third_w, third_b = params
    channels = flow_state.shape[0]
    half_chan = channels // 2
    cell_count = flow_state.shape[1] * flow_state.shape[2]
    mixed_state = (flow_state + shift_vec[:, None, None]) * jnp.exp(gain_vec)[:, None, None]
    lower_mat = jnp.tril(lower_raw, -1) + jnp.eye(channels, dtype=jnp.float32)
    upper_mat = jnp.triu(upper_raw, 1) + jnp.diag(jnp.exp(diag_log))
    matrix = jnp.dot(lower_mat, upper_mat, precision=lax.Precision.HIGHEST)
    mixed_state = jnp.einsum('oc,chw->ohw', matrix, mixed_state, precision=lax.Precision.HIGHEST)
    part_a = mixed_state[:half_chan]
    part_b = mixed_state[half_chan:]
    coupled = part_a.astype(jnp.bfloat16)
    inner = jax.nn.relu(spatial_conv(coupled, first_w) + first_b.astype(jnp.float32)[:, None, None]).astype(jnp.bfloat16)
    middle = jnp.einsum('chw,co->ohw', inner.astype(jnp.float32), second_w.astype(jnp.float32))
    middle = jax.nn.relu(middle + second_b[:, None, None]).astype(jnp.bfloat16)
    output = spatial_conv(middle, third_w) + third_b[:, None, None]
    gate_pre = output[:half_chan] + 2.0
    updated = (part_b + output[half_chan:]) * jax.nn.sigmoid(gate_pre)
    step_term = cell_count * (jnp.sum(gain_vec) + jnp.sum(diag_log)) + jnp.sum(jax.nn.log_sigmoid(gate_pre))
    return jnp.concatenate([part_a, updated], axis=0), step_term


def image_flow(picture, params_mid, params_top):
    flow_state = picture
    logdet = jnp.zeros((), jnp.float32)
    for step_num in range(params_mid[0].shape[0]):
        flow_state, step_term = flow_step(flow_state, tuple(p[step_num] for p in params_mid))
        logdet = logdet + step_term
    half_chan = flow_state.shape[0] // 2
    latent_mid = flow_state[:half_chan]
    kept_chan = flow_state[half_chan:]
    count_chan, height, columns = kept_chan.shape
    squeezed = kept_chan.reshape(count_chan, height // 2, 2, columns // 2, 2).transpose(0, 2, 4, 1, 3)
    flow_state = squeezed.reshape(count_chan * 4, height // 2, columns // 2)
    for step_num in range(params_top[0].shape[0]):
        flow_state, step_term = flow_step(flow_state, tuple(p[step_num] for p in params_top))
        logdet = logdet + step_term
    latent_top = flow_state
    latent_count = latent_mid.size + latent_top.size
    logprob = -0.5 * (jnp.sum(latent_mid * latent_mid) + jnp.sum(latent_top * latent_top)) - 0.5 * log_two_pi * latent_count
    total_dims = picture.shape[0] * picture.shape[1] * picture.shape[2]
    return latent_mid, latent_top, (logprob + logdet) / total_dims


def reference(images, shift_mid, gain_mid, lower_mid, upper_mid, diag_mid, first_mid, first_bias_mid, second_mid, second_bias_mid, third_mid, third_bias_mid, shift_top, gain_top, lower_top, upper_top, diag_top, first_top, first_bias_top, second_top, second_bias_top, third_top, third_bias_top):
    params_mid = (shift_mid, gain_mid, lower_mid, upper_mid, diag_mid, first_mid, first_bias_mid, second_mid, second_bias_mid, third_mid, third_bias_mid)
    params_top = (shift_top, gain_top, lower_top, upper_top, diag_top, first_top, first_bias_top, second_top, second_bias_top, third_top, third_bias_top)
    latent_mid, latent_top, loglik = lax.map(lambda picture: image_flow(picture, params_mid, params_top), images)
    return (latent_mid, latent_top, loglik)
```

```python
import functools
import math

import jax
import jax.numpy as jnp
from jax import lax
from jax.experimental import pallas as pl
from jax.experimental.pallas import tpu as pltpu
from jax.sharding import PartitionSpec as P

MESH = pl.DeviceIdType.MESH
LANES = 128
CHUNK = 1024
FINE = lax.Precision.HIGHEST
log_two_pi = math.log(2.0 * math.pi)
f32 = jnp.float32
bf16 = jnp.bfloat16


def iota(shape, dim):
    return lax.broadcasted_iota(jnp.int32, shape, dim)


def dot_nt(a, b, precision=None):
    return lax.dot_general(
        a, b, (((1,), (1,)), ((), ())), preferred_element_type=f32, precision=precision
    )


def roll(x, amount):
    n = x.shape[1]
    amount = amount % n
    return x if amount == 0 else pltpu.roll(x, amount, 1)


def keep(x, ok):
    return jnp.where(ok, x, 0.0)


def mid_map(channels):
    i = iota((channels, channels), 0)
    j = iota((channels, channels), 1)
    source = jnp.where(i < 12, i, jnp.where(i < 16, i + 8, i - 4))
    return jnp.where(source == j, 1.0, 0.0)


def eye_map(channels):
    return jnp.where(iota((channels, channels), 0) == iota((channels, channels), 1), 1.0, 0.0)


def squeeze_map(channels):
    i = iota((channels, channels), 0)
    j = iota((channels, channels), 1)
    low = 4 * lax.rem(i, 8) + lax.div(i, 8)
    k = i - 32
    place = 2 * lax.div(k, 8) + 1 - lax.div(lax.rem(k + 64, 8), 4)
    high = 4 * (8 + lax.rem(k + 64, 4)) + place
    return jnp.where(jnp.where(i < 32, low, high) == j, 1.0, 0.0)


def split_two(x):
    high = x.astype(bf16).astype(f32)
    return high, x - high


def mixing(lower, upper, diag_row, gain_row, shift_row, out_map, in_map, exact):
    channels = lower.shape[0]
    i = iota((channels, channels), 0)
    j = iota((channels, channels), 1)
    eye = jnp.where(i == j, 1.0, 0.0)
    low = jnp.where(i > j, lower, 0.0) + eye
    upp = (jnp.where(i < j, upper, 0.0) + eye * jnp.exp(diag_row)) * jnp.exp(gain_row)
    rows = jnp.dot(out_map, low, precision=FINE, preferred_element_type=f32)
    mat = jnp.dot(rows, upp, precision=FINE, preferred_element_type=f32)
    bias = jnp.sum(mat * shift_row, axis=1, keepdims=True)
    if in_map is not None:
        mat = dot_nt(mat, in_map, FINE)
    high, rest = split_two(mat)
    parts = [high, rest] if exact else [high, high, rest]
    return jnp.concatenate(parts, axis=1).astype(bf16), bias


def mapped_column(row, mapping):
    return jnp.sum(mapping * row, axis=1, keepdims=True)


def prepare(p, s):
    steps_mid, channels = p["shift_mid"].shape
    steps_top, top_channels = p["shift_top"].shape
    hidden = p["w2_mid"].shape[1]
    half = channels // 2
    mapping = mid_map(channels)
    natural = eye_map(top_channels)
    for k in range(steps_mid):
        mat, bias = mixing(
            p["lower_mid"][k],
            p["upper_mid"][k],
            p["diag_mid"][k : k + 1, :],
            p["gain_mid"][k : k + 1, :],
            p["shift_mid"][k : k + 1, :],
            mapping,
            None if k == 0 else mapping,
            k == 0,
        )
        s["mix_mid"][k, :, : mat.shape[1]] = mat
        s["mix_bias_mid"][k] = jnp.broadcast_to(bias, (channels, LANES))
        s["b3_mid"][k] = jnp.broadcast_to(
            mapped_column(p["third_bias_mid"][k : k + 1, :], mapping), (channels, LANES)
        )
    for k in range(steps_top):
        mat, bias = mixing(
            p["lower_top"][k],
            p["upper_top"][k],
            p["diag_top"][k : k + 1, :],
            p["gain_top"][k : k + 1, :],
            p["shift_top"][k : k + 1, :],
            natural,
            squeeze_map(top_channels) if k == 0 else None,
            False,
        )
        s["mix_top"][k, :, : mat.shape[1]] = mat
        s["mix_bias_top"][k] = jnp.broadcast_to(bias, (top_channels, LANES))
        s["b3_top"][k] = jnp.broadcast_to(
            mapped_column(p["third_bias_top"][k : k + 1, :], natural), (top_channels, LANES)
        )
    for k in range(steps_mid):
        taps = []
        for tap in range(9):
            extra = [jnp.zeros((16 - half, hidden), f32)]
            if tap == 4:
                row = p["first_bias_mid"][k : k + 1, :].astype(f32)
                extra = [row, jnp.zeros((15 - half, hidden), f32)]
            taps.append(jnp.concatenate([p["w1_mid"][k, tap].astype(f32)] + extra, axis=0))
        s["w1t_mid"][k] = jnp.transpose(jnp.concatenate(taps, axis=0)).astype(bf16)
        s["w2t_mid"][k] = jnp.transpose(p["w2_mid"][k].astype(f32)).astype(bf16)
        s["b2_mid"][k] = jnp.transpose(
            jnp.broadcast_to(p["second_bias_mid"][k : k + 1, :], (LANES, hidden))
        )
        for tap in range(9):
            w = p["w3_mid"][k, tap * channels : (tap + 1) * channels, :].astype(f32)
            w = jnp.concatenate([w[:12], w[20:24], w[12:20]], axis=0)
            s["w3f_mid"][tap * channels : (tap + 1) * channels, :] = w
        s["w3p_mid"][k] = s["w3f_mid"][...].astype(bf16)
    for k in range(steps_top):
        row = p["first_bias_top"][k : k + 1, :].astype(f32)
        w = jnp.concatenate(
            [p["w1_top"][k].astype(f32), row, jnp.zeros((7, hidden), f32)], axis=0
        )
        s["w1t_top"][k] = jnp.transpose(w).astype(bf16)
        s["w2t_top"][k] = jnp.transpose(p["w2_top"][k].astype(f32)).astype(bf16)
        s["b2_top"][k] = jnp.transpose(
            jnp.broadcast_to(p["second_bias_top"][k : k + 1, :], (LANES, hidden))
        )


def wide(x, n):
    return jnp.concatenate([x] * (n // LANES), axis=1)


def lane_of(n):
    return lax.rem(iota((1, n), 1), LANES)


def edge_mid(x, dr):
    lane = iota((1, LANES), 1)
    if dr > 0:
        return keep(roll(x, -32), lane < 96)
    return keep(roll(x, 32), lane >= 32)


def edge_top(x, dr):
    lane = iota((1, LANES), 1)
    odd = lax.rem(lane, 2) == 1
    if dr > 0:
        return jnp.where(odd, keep(roll(x, -31), lane < 96), roll(x, -1))
    return jnp.where(odd, roll(x, 1), keep(roll(x, 31), lane >= 32))


def shift_col(x, dc, stride):
    n = x.shape[1]
    col = lax.rem(iota((1, n), 1), 32)
    if dc > 0:
        return keep(roll(x, -stride), col < 32 - stride)
    return keep(roll(x, stride), col >= stride)


def gather(y_ref, tap_rows, lo, hi, n, edge, stride):
    total = None
    for dc in (0, -1, 1):
        base = 4 + dc
        part = y_ref[base * tap_rows : (base + 1) * tap_rows, lo:hi]
        for dr in (-1, 1):
            tap = base + 3 * dr
            rows = slice(tap * tap_rows, (tap + 1) * tap_rows)
            if dr > 0 and hi == n:
                moved = [edge(y_ref[rows, :LANES], dr)]
                if hi - lo > LANES:
                    moved = [y_ref[rows, lo + LANES : hi]] + moved
                moved = jnp.concatenate(moved, axis=1) if len(moved) > 1 else moved[0]
            elif dr < 0 and lo == 0:
                moved = [edge(y_ref[rows, n - LANES : n], dr)]
                if hi - lo > LANES:
                    moved = moved + [y_ref[rows, : hi - LANES]]
                moved = jnp.concatenate(moved, axis=1) if len(moved) > 1 else moved[0]
            else:
                moved = y_ref[rows, lo + dr * LANES : hi + dr * LANES]
            part = part + moved
        if dc != 0:
            part = shift_col(part, dc, stride)
        total = part if total is None else total + part
    return total


def gated(g):
    e = jnp.exp(-jnp.abs(g))
    inv = 1.0 / (1.0 + e)
    gate = jnp.where(g >= 0, inv, e * inv)
    return gate, jnp.minimum(g, 0.0) - jnp.log(1.0 + e)


def fold(x):
    total = x[:, :LANES]
    for at in range(LANES, x.shape[1], LANES):
        total = total + x[:, at : at + LANES]
    return total


def mix(mat, bias, x, exact):
    n = x.shape[1]
    if exact:
        stack = [x, x]
    else:
        high, rest = split_two(x)
        stack = [high, rest, high]
    stack = jnp.concatenate(stack, axis=0).astype(bf16)
    return jnp.dot(mat, stack, preferred_element_type=f32) + wide(bias, n)


def product(first, second, third, bias, spread, y_ref, rows, lo):
    n = spread.shape[1]
    h = jnp.dot(first[...], spread, preferred_element_type=f32)
    h = jnp.maximum(h, 0.0).astype(bf16)
    h = jnp.dot(second[...], h, preferred_element_type=f32)
    h = jnp.maximum(h + wide(bias[...], n), 0.0).astype(bf16)
    y_ref[:rows, lo : lo + n] = jnp.dot(third[...], h, preferred_element_type=f32)


def mid_step(s, k, exact):
    state, u_ref, q_ref, y_ref = s["state"], s["u"], s["q"], s["y"]
    channels, n = state.shape
    block = 4 * LANES
    sub = iota((8, 1), 0)
    mat = s["mix_mid"][k, :, : (2 if exact else 3) * channels]
    for lo in range(0, n, block):
        u_ref[:, lo : lo + block] = mix(
            mat, s["mix_bias_mid"][k], state[:, lo : lo + block], exact
        )
    for lo in range(0, n, block):
        q = u_ref[:16, lo : lo + block]
        q = jnp.concatenate([q[:8], jnp.where(sub == 4, 1.0, q[8:])], axis=0)
        for dc in (-1, 0, 1):
            x = q if dc == 0 else shift_col(q, dc, 1)
            q_ref[dc + 1, :, LANES + lo : LANES + lo + block] = x.astype(bf16)
            if lo == 0:
                q_ref[dc + 1, :, LANES + n :] = edge_mid(x[:, :LANES], 1).astype(bf16)
            if lo + block == n:
                q_ref[dc + 1, :, :LANES] = edge_mid(x[:, block - LANES :], -1).astype(bf16)
    for lo in range(0, n, min(CHUNK, n)):
        taps = []
        for dr in (-1, 0, 1):
            at = lo + LANES * (1 + dr)
            for dc in (-1, 0, 1):
                taps.append(q_ref[dc + 1, :, at : at + min(CHUNK, n)])
        product(
            s["w1t_mid"].at[k],
            s["w2t_mid"].at[k],
            s["w3p_mid"].at[k],
            s["b2_mid"].at[k],
            jnp.concatenate(taps, axis=0),
            y_ref,
            9 * channels,
            lo,
        )
    score = None
    width = 2 * LANES
    for lo in range(0, n, width):
        out = gather(y_ref, channels, lo, lo + width, n, edge_mid, 1) + wide(s["b3_mid"][k], width)
        gate, logs = gated(out[:16] + 2.0)
        logs = fold(logs)
        score = logs if score is None else score + logs
        u = u_ref[:, lo : lo + width]
        state[:8, lo : lo + width] = u[:8]
        late = (u[8:16] + out[8:16]) * pltpu.roll(gate[8:16], 4, 0)
        state[8:16, lo : lo + width] = jnp.where(sub < 4, u[8:16], late)
        state[16:, lo : lo + width] = (u[16:] + out[16:]) * gate[:8]
    return keep(score, iota((16, 1), 0) < channels // 2)


def squeeze(s):
    state, top = s["state"], s["top"]
    odd = lax.rem(iota((1, LANES), 1), 2) == 1
    sub = iota((8, 1), 0)
    for v in range(4):
        tails = []
        for i in range(2):
            t = (2 * v + i) * LANES
            a = state[8:, t : t + LANES]
            t = t + 8 * LANES
            b = state[8:, t : t + LANES]
            even_col = jnp.where(odd, roll(b, 1), a)
            odd_col = jnp.where(odd, b, roll(a, -1))
            cols = slice(v * LANES, (v + 1) * LANES)
            top[16 * i : 16 * i + 8, cols] = even_col[8:]
            top[16 * i + 8 : 16 * i + 16, cols] = odd_col[8:]
            top[32 + 8 * i : 40 + 8 * i, cols] = jnp.where(
                sub < 4, pltpu.roll(odd_col[:8], 4, 0), even_col[:8]
            )


def top_step(s, k):
    state, u_ref, q_ref, y_ref = s["top"], s["u_top"], s["q_top"], s["y_top"]
    channels, n = state.shape
    half = channels // 2
    mat = s["mix_top"][k, :, : 3 * channels]
    u_ref[...] = mix(mat, s["mix_bias_top"][k], state[...], False)
    q = u_ref[:half, :]
    for dc in (-1, 0, 1):
        x = q if dc == 0 else shift_col(q, dc, 2)
        q_ref[dc + 1, :, LANES : LANES + n] = x
        q_ref[dc + 1, :, LANES + n :] = edge_top(x[:, :LANES], 1)
        q_ref[dc + 1, :, :LANES] = edge_top(x[:, n - LANES :], -1)
    ones = jnp.where(iota((8, min(CHUNK, n)), 0) == 0, 1.0, 0.0)
    for lo in range(0, n, min(CHUNK, n)):
        taps = []
        for dr in (-1, 0, 1):
            at = lo + LANES * (1 + dr)
            for dc in (-1, 0, 1):
                taps.append(q_ref[dc + 1, :, at : at + min(CHUNK, n)])
        product(
            s["w1t_top"].at[k],
            s["w2t_top"].at[k],
            s["w3_top"].at[k],
            s["b2_top"].at[k],
            jnp.concatenate(taps + [ones], axis=0).astype(bf16),
            y_ref,
            9 * channels,
            lo,
        )
    score = None
    width = LANES
    for lo in range(0, n, width):
        out = gather(y_ref, channels, lo, lo + width, n, edge_top, 2) + wide(s["b3_top"][k], width)
        gate, logs = gated(out[:half] + 2.0)
        score = logs if score is None else score + logs
        state[:half, lo : lo + width] = u_ref[:half, lo : lo + width]
        state[half:, lo : lo + width] = (u_ref[half:, lo : lo + width] + out[half:]) * gate
    return score


def work_scratch(steps_mid, steps_top, hidden, channels, top_channels, cells):
    n_top = cells // 4
    return {
        "mix_mid": pltpu.VMEM((steps_mid, channels, 3 * channels), bf16),
        "mix_bias_mid": pltpu.VMEM((steps_mid, channels, LANES), f32),
        "b3_mid": pltpu.VMEM((steps_mid, channels, LANES), f32),
        "mix_top": pltpu.VMEM((steps_top, top_channels, 3 * top_channels), bf16),
        "mix_bias_top": pltpu.VMEM((steps_top, top_channels, LANES), f32),
        "b3_top": pltpu.VMEM((steps_top, top_channels, LANES), f32),
        "w1t_mid": pltpu.VMEM((steps_mid, hidden, 144), bf16),
        "w2t_mid": pltpu.VMEM((steps_mid, hidden, hidden), bf16),
        "b2_mid": pltpu.VMEM((steps_mid, hidden, LANES), f32),
        "w3f_mid": pltpu.VMEM((9 * channels, hidden), f32),
        "w3p_mid": pltpu.VMEM((steps_mid, 9 * channels, hidden), bf16),
        "w1t_top": pltpu.VMEM((steps_top, hidden, 9 * top_channels // 2 + 8), bf16),
        "w2t_top": pltpu.VMEM((steps_top, hidden, hidden), bf16),
        "b2_top": pltpu.VMEM((steps_top, hidden, LANES), f32),
        "state": pltpu.VMEM((channels, cells), f32),
        "u": pltpu.VMEM((channels, cells), f32),
        "q": pltpu.VMEM((3, 16, cells + 2 * LANES), bf16),
        "y": pltpu.VMEM((9 * channels, cells), f32),
        "top": pltpu.VMEM((top_channels, n_top), f32),
        "u_top": pltpu.VMEM((top_channels, n_top), f32),
        "q_top": pltpu.VMEM((3, top_channels // 2, n_top + 2 * LANES), f32),
        "y_top": pltpu.VMEM((9 * top_channels, n_top), f32),
        "turned": pltpu.VMEM((n_top, LANES), f32),
    }


NAMES = (
    "shift_mid",
    "gain_mid",
    "lower_mid",
    "upper_mid",
    "diag_mid",
    "w1_mid",
    "first_bias_mid",
    "w2_mid",
    "second_bias_mid",
    "w3_mid",
    "third_bias_mid",
    "shift_top",
    "gain_top",
    "lower_top",
    "upper_top",
    "diag_top",
    "w1_top",
    "first_bias_top",
    "w2_top",
    "second_bias_top",
    "w3_top",
    "third_bias_top",
)


def parameters(params):
    (
        shift_mid, gain_mid, lower_mid, upper_mid, diag_mid, first_mid, first_bias_mid, second_mid,
        second_bias_mid, third_mid, third_bias_mid, shift_top, gain_top, lower_top, upper_top,
        diag_top, first_top, first_bias_top, second_top, second_bias_top, third_top, third_bias_top,
    ) = params
    steps_mid, hidden = first_bias_mid.shape
    steps_top = first_bias_top.shape[0]
    w1_top = first_top.reshape(steps_top, -1, hidden)
    w3_mid = third_mid.transpose(0, 1, 3, 2).reshape(steps_mid, -1, hidden)
    w3_top = third_top.transpose(0, 1, 3, 2).reshape(steps_top, -1, hidden)
    return (
        shift_mid, gain_mid, lower_mid, upper_mid, diag_mid, first_mid, first_bias_mid, second_mid,
        second_bias_mid, w3_mid, third_bias_mid, shift_top, gain_top, lower_top, upper_top,
        diag_top, w1_top, first_bias_top, second_top, second_bias_top, w3_top, third_bias_top,
    )


def kernel(dims, keys, *refs):
    n_rows, n_chan, height, width, count = dims
    sources, refs = refs[:count], refs[count:]
    (mid_out, top_out, lik_out), refs = refs[:3], refs[3:]
    held, refs = refs[:count], refs[count:]
    s, refs = dict(zip(keys, refs)), refs[len(keys) :]
    outbox, inbox, z_send, z_recv, w_sem, send_sem, recv_sem, z_send_sem, z_recv_sem = refs
    images = held[0]
    p = dict(zip(NAMES, held[1:]))
    s["w3_top"] = p["w3_top"]
    peers = n_rows * n_chan
    b = lax.axis_index("batch")
    r = lax.axis_index("rows")
    c = lax.axis_index("chan")
    me = r * n_chan + c
    quad = lax.div(r, 2)
    side = lax.rem(r, 2)

    def device(row, chan):
        return {"batch": b, "rows": row, "chan": chan}

    def swap(y):
        return y + lax.div(y, 2) * (5 - 2 * y)

    def place(q):
        at = lax.rem(q, n_chan)
        return lax.div(q, n_chan), 2 * swap(lax.div(at, 2)) + 1 - lax.rem(at, 2)

    rank = r * n_chan + 2 * swap(lax.div(c, 2)) + 1 - lax.rem(c, 2)

    first = pltpu.make_async_copy(sources[0], held[0], w_sem.at[0])
    first.start()
    barrier = pltpu.get_barrier_semaphore()

    def greet(q, carry):
        row, chan = place(q)
        pl.semaphore_signal(barrier, inc=1, device_id=device(row, chan), device_id_type=MESH)
        return carry

    lax.fori_loop(rank + 1, peers, greet, 0)
    first.wait()
    for dest in range(n_chan):
        x = images[dest]
        x = jnp.concatenate([x[:8], x[8:16], x[16:], jnp.zeros((8, width), f32)], axis=1)
        outbox[dest] = pltpu.roll(x, quad * 32, 1).astype(bf16)
    @pl.when(rank > 0)
    def _():
        pl.semaphore_wait(barrier, rank)

    def send(q, carry):
        row, chan = place(q)
        pltpu.make_async_remote_copy(
            src_ref=outbox.at[chan],
            dst_ref=inbox.at[me],
            send_sem=send_sem,
            recv_sem=recv_sem.at[me],
            device_id=device(row, chan),
            device_id_type=MESH,
        ).start()
        return carry

    def arrive(q, carry):
        row, chan = place(q)
        slot = row * n_chan + chan
        pltpu.make_async_remote_copy(
            src_ref=outbox.at[0],
            dst_ref=inbox.at[slot],
            send_sem=send_sem,
            recv_sem=recv_sem.at[slot],
            device_id=device(r, c),
            device_id_type=MESH,
        ).wait_recv()
        return carry

    lax.fori_loop(0, rank, send, 0)
    copies = []
    for at in range(1, count):
        copy = pltpu.make_async_copy(sources[at], held[at], w_sem.at[at])
        copy.start()
        copies.append(copy)
    inbox[me] = outbox[c]
    for copy in copies:
        copy.wait()
    prepare(p, s)
    channels = p["shift_mid"].shape[1]
    top_channels = p["shift_top"].shape[1]
    half = channels // 2
    cells = height * width
    fixed = cells * (jnp.sum(p["gain_mid"][...]) + jnp.sum(p["diag_mid"][...]))
    fixed = fixed + cells // 4 * (jnp.sum(p["gain_top"][...]) + jnp.sum(p["diag_top"][...]))
    fixed = fixed - 0.5 * log_two_pi * channels * cells

    lax.fori_loop(rank + 1, peers, lambda q, x: send(q, arrive(q, x)), 0)
    lax.fori_loop(0, rank, arrive, 0)

    state = s["state"]
    lane = iota((1, LANES), 1)
    for t in range(height // 4):
        letters = [inbox[16 * k + t].astype(f32) for k in range(4)]
        for slab in range(3):
            x = letters[(3 - slab) % 4]
            for k in range(3):
                x = jnp.where(lax.div(lane, 32) == k, letters[(k - slab) % 4], x)
            state[8 * slab : 8 * slab + 8, t * LANES : (t + 1) * LANES] = roll(x, -32 * slab)

    score = None
    for k in range(p["shift_mid"].shape[0]):
        logs = mid_step(s, k, k == 0)
        score = logs if score is None else score + logs

    for to in range(n_chan):
        start = pl.multiple_of((side * n_chan + to) * LANES, LANES)
        z = state[:16, pl.ds(start, LANES)]
        z_send[to] = jnp.where(
            lane < 32,
            pltpu.roll(z[:8], LANES - quad * 32, 1),
            pltpu.roll(z[8:], LANES + 32 - quad * 32, 1),
        )
    z_copies = []
    for d in range(1, n_chan):
        other = lax.rem(c + d, n_chan)
        copy = pltpu.make_async_remote_copy(
            src_ref=z_send.at[other],
            dst_ref=z_recv.at[c],
            send_sem=z_send_sem.at[d],
            recv_sem=z_recv_sem.at[d],
            device_id=device(r, other),
            device_id_type=MESH,
        )
        copy.start()
        z_copies.append(copy)
    z_recv[c] = z_send[c]

    squares = fold(state[:16, :] * state[:16, :])
    score = score - 0.5 * keep(squares, iota((16, 1), 0) < half)
    squeeze(s)
    score_top = None
    for k in range(p["shift_top"].shape[0]):
        logs = top_step(s, k)
        score_top = logs if score_top is None else score_top + logs
    top = s["top"]
    squares = fold(top[...] * top[...])
    total = jnp.sum(score, axis=0, keepdims=True) + jnp.sum(score_top, axis=0, keepdims=True)
    total = total - 0.5 * jnp.sum(squares, axis=0, keepdims=True)
    lik_out[0] = (jnp.sum(total) + fixed) / (channels * cells)
    turned = s["turned"]
    for v in range(4):
        turned[v * LANES : (v + 1) * LANES, :top_channels] = jnp.transpose(
            top[:, v * LANES : (v + 1) * LANES]
        )
    for v in range(4):
        start = v * LANES + quad * 32 + side
        top_out[0, v * 16 : (v + 1) * 16, :] = turned[pl.ds(start, 16, stride=2), :][
            :, :top_channels
        ]

    for d in range(1, n_chan):
        pltpu.make_async_remote_copy(
            src_ref=z_send.at[0],
            dst_ref=z_recv.at[lax.rem(c + n_chan - d, n_chan)],
            send_sem=z_send_sem.at[d],
            recv_sem=z_recv_sem.at[d],
            device_id=device(r, c),
            device_id_type=MESH,
        ).wait_recv()
    for img in range(n_chan):
        z = z_recv[img]
        mid_out[img, :8, :] = z[:, :width]
        mid_out[img, 8:, :] = z[:4, width : 2 * width]
    for copy in z_copies:
        copy.wait_send()
    pltpu.make_async_remote_copy(
        src_ref=inbox.at[pl.ds(0, peers - 1)],
        dst_ref=inbox.at[pl.ds(0, peers - 1)],
        send_sem=send_sem,
        recv_sem=recv_sem.at[0],
        device_id=device(r, c),
        device_id_type=MESH,
    ).wait_send()


def deliver(mid, top, lik, mid_out, top_out, lik_out):
    for img in range(mid.shape[0]):
        mid_out[img, :, 0, :] = mid[img]
    top_out[...] = top[...]
    lik_out[0] = lik[0]


def body(sizes, images, *params):
    n_rows, n_chan = sizes
    n_imgs, channels, own_rows, width = images.shape
    peers = n_rows * n_chan
    height = own_rows * peers
    params = parameters(params)
    hidden = params[6].shape[1]
    steps_mid, steps_top = params[0].shape[0], params[11].shape[0]
    top_channels = params[11].shape[1]
    half = channels // 2
    cells = height * width
    own = cells // 4 // n_rows
    operands = (images.reshape(n_imgs, channels, width),) + params
    vmem = pl.BlockSpec(memory_space=pltpu.VMEM)
    smem = pl.BlockSpec(memory_space=pltpu.SMEM)
    count = len(operands)
    work = work_scratch(steps_mid, steps_top, hidden, channels, top_channels, cells)
    mid, top, lik = pl.pallas_call(
        functools.partial(kernel, (n_rows, n_chan, height, width, count), list(work)),
        out_shape=(
            jax.ShapeDtypeStruct((n_imgs, half, width), f32),
            jax.ShapeDtypeStruct((1, own, top_channels), f32),
            jax.ShapeDtypeStruct((1,), f32),
        ),
        in_specs=[pl.BlockSpec(memory_space=pl.ANY)] * count,
        out_specs=(vmem, vmem, smem),
        scratch_shapes=[pltpu.VMEM(x.shape, x.dtype) for x in operands]
        + list(work.values())
        + [
            pltpu.VMEM((n_chan, 8, LANES), bf16),
            pltpu.VMEM((peers, 8, LANES), bf16),
            pltpu.VMEM((n_chan, 8, LANES), f32),
            pltpu.VMEM((n_chan, 8, LANES), f32),
            pltpu.SemaphoreType.DMA((count,)),
            pltpu.SemaphoreType.DMA,
            pltpu.SemaphoreType.DMA((peers,)),
            pltpu.SemaphoreType.DMA((n_chan,)),
            pltpu.SemaphoreType.DMA((n_chan,)),
        ],
        compiler_params=pltpu.CompilerParams(
            collective_id=0, has_side_effects=True, vmem_limit_bytes=56 * 1024 * 1024
        ),
        name="flow",
    )(*operands)
    latent_mid, top, lik = pl.pallas_call(
        deliver,
        out_shape=(
            jax.ShapeDtypeStruct((n_imgs, half, own_rows, width), f32),
            jax.ShapeDtypeStruct(top.shape, f32),
            jax.ShapeDtypeStruct(lik.shape, f32),
        ),
        in_specs=[vmem, vmem, smem],
        out_specs=(vmem, vmem, smem),
        name="deliver",
    )(mid, top, lik)
    latent_top = top.reshape(1, -1, width // 2, top_channels).transpose(0, 3, 1, 2)
    return latent_mid, latent_top, lik


def solution(mesh):
    sizes = (mesh.shape["rows"], mesh.shape["chan"])
    placed = (P("batch", None, ("rows", "chan"), None),) + (P(),) * 22
    return jax.shard_map(
        functools.partial(body, sizes),
        mesh=mesh,
        in_specs=placed,
        out_specs=(
            P("batch", None, ("rows", "chan"), None),
            P(("batch", "chan"), None, "rows", None),
            P(("batch", "chan")),
        ),
        check_vma=False,
    )
```

```python
import functools
import math

import jax
import jax.numpy as jnp
from jax import lax
from jax.experimental import pallas as pl
from jax.experimental.pallas import tpu as pltpu
from jax.sharding import PartitionSpec as P

MESH = pl.DeviceIdType.MESH
LANES = 128
CHUNK = 1024
FINE = lax.Precision.HIGHEST
log_two_pi = math.log(2.0 * math.pi)
f32 = jnp.float32
bf16 = jnp.bfloat16


def iota(shape, dim):
    return lax.broadcasted_iota(jnp.int32, shape, dim)


def dot_nt(a, b, precision=None):
    return lax.dot_general(
        a, b, (((1,), (1,)), ((), ())), preferred_element_type=f32, precision=precision
    )


def roll(x, amount):
    n = x.shape[1]
    amount = amount % n
    return x if amount == 0 else pltpu.roll(x, amount, 1)


def keep(x, ok):
    return jnp.where(ok, x, 0.0)


def mid_map(channels):
    i = iota((channels, channels), 0)
    j = iota((channels, channels), 1)
    source = jnp.where(i < 12, i, jnp.where(i < 16, i + 8, i - 4))
    return jnp.where(source == j, 1.0, 0.0)


def eye_map(channels):
    return jnp.where(iota((channels, channels), 0) == iota((channels, channels), 1), 1.0, 0.0)


def squeeze_map(channels):
    i = iota((channels, channels), 0)
    j = iota((channels, channels), 1)
    low = 4 * lax.rem(i, 8) + lax.div(i, 8)
    k = i - 32
    place = 2 * lax.div(k, 8) + 1 - lax.div(lax.rem(k + 64, 8), 4)
    high = 4 * (8 + lax.rem(k + 64, 4)) + place
    return jnp.where(jnp.where(i < 32, low, high) == j, 1.0, 0.0)


def split_two(x):
    high = x.astype(bf16).astype(f32)
    return high, x - high


def mixing(lower, upper, diag_row, gain_row, shift_row, out_map, in_map, exact):
    channels = lower.shape[0]
    i = iota((channels, channels), 0)
    j = iota((channels, channels), 1)
    eye = jnp.where(i == j, 1.0, 0.0)
    low = jnp.where(i > j, lower, 0.0) + eye
    upp = (jnp.where(i < j, upper, 0.0) + eye * jnp.exp(diag_row)) * jnp.exp(gain_row)
    rows = jnp.dot(out_map, low, precision=FINE, preferred_element_type=f32)
    mat = jnp.dot(rows, upp, precision=FINE, preferred_element_type=f32)
    bias = jnp.sum(mat * shift_row, axis=1, keepdims=True)
    if in_map is not None:
        mat = dot_nt(mat, in_map, FINE)
    high, rest = split_two(mat)
    parts = [high, rest] if exact else [high, high, rest]
    return jnp.concatenate(parts, axis=1).astype(bf16), bias


def mapped_column(row, mapping):
    return jnp.sum(mapping * row, axis=1, keepdims=True)


def prepare(p, s):
    steps_mid, channels = p["shift_mid"].shape
    steps_top, top_channels = p["shift_top"].shape
    hidden = p["w2_mid"].shape[1]
    half = channels // 2
    mapping = mid_map(channels)
    natural = eye_map(top_channels)
    for k in range(steps_mid):
        mat, bias = mixing(
            p["lower_mid"][k],
            p["upper_mid"][k],
            p["diag_mid"][k : k + 1, :],
            p["gain_mid"][k : k + 1, :],
            p["shift_mid"][k : k + 1, :],
            mapping,
            None if k == 0 else mapping,
            k == 0,
        )
        s["mix_mid"][k, :, : mat.shape[1]] = mat
        s["mix_bias_mid"][k] = jnp.broadcast_to(bias, (channels, LANES))
        s["b3_mid"][k] = jnp.broadcast_to(
            mapped_column(p["third_bias_mid"][k : k + 1, :], mapping), (channels, LANES)
        )
    for k in range(steps_top):
        mat, bias = mixing(
            p["lower_top"][k],
            p["upper_top"][k],
            p["diag_top"][k : k + 1, :],
            p["gain_top"][k : k + 1, :],
            p["shift_top"][k : k + 1, :],
            natural,
            squeeze_map(top_channels) if k == 0 else None,
            False,
        )
        s["mix_top"][k, :, : mat.shape[1]] = mat
        s["mix_bias_top"][k] = jnp.broadcast_to(bias, (top_channels, LANES))
        s["b3_top"][k] = jnp.broadcast_to(
            mapped_column(p["third_bias_top"][k : k + 1, :], natural), (top_channels, LANES)
        )
    for k in range(steps_mid):
        taps = []
        for tap in range(9):
            extra = [jnp.zeros((16 - half, hidden), f32)]
            if tap == 4:
                row = p["first_bias_mid"][k : k + 1, :].astype(f32)
                extra = [row, jnp.zeros((15 - half, hidden), f32)]
            taps.append(jnp.concatenate([p["w1_mid"][k, tap].astype(f32)] + extra, axis=0))
        s["w1t_mid"][k] = jnp.transpose(jnp.concatenate(taps, axis=0)).astype(bf16)
        s["w2t_mid"][k] = jnp.transpose(p["w2_mid"][k].astype(f32)).astype(bf16)
        s["b2_mid"][k] = jnp.transpose(
            jnp.broadcast_to(p["second_bias_mid"][k : k + 1, :], (LANES, hidden))
        )
        for tap in range(9):
            w = p["w3_mid"][k, tap * channels : (tap + 1) * channels, :].astype(f32)
            w = jnp.concatenate([w[:12], w[20:24], w[12:20]], axis=0)
            s["w3f_mid"][tap * channels : (tap + 1) * channels, :] = w
        s["w3p_mid"][k] = s["w3f_mid"][...].astype(bf16)
    for k in range(steps_top):
        row = p["first_bias_top"][k : k + 1, :].astype(f32)
        w = jnp.concatenate(
            [p["w1_top"][k].astype(f32), row, jnp.zeros((7, hidden), f32)], axis=0
        )
        s["w1t_top"][k] = jnp.transpose(w).astype(bf16)
        s["w2t_top"][k] = jnp.transpose(p["w2_top"][k].astype(f32)).astype(bf16)
        s["b2_top"][k] = jnp.transpose(
            jnp.broadcast_to(p["second_bias_top"][k : k + 1, :], (LANES, hidden))
        )


def wide(x, n):
    return jnp.concatenate([x] * (n // LANES), axis=1)


def lane_of(n):
    return lax.rem(iota((1, n), 1), LANES)


def edge_mid(x, dr):
    lane = iota((1, LANES), 1)
    if dr > 0:
        return keep(roll(x, -32), lane < 96)
    return keep(roll(x, 32), lane >= 32)


def edge_top(x, dr):
    lane = iota((1, LANES), 1)
    odd = lax.rem(lane, 2) == 1
    if dr > 0:
        return jnp.where(odd, keep(roll(x, -31), lane < 96), roll(x, -1))
    return jnp.where(odd, roll(x, 1), keep(roll(x, 31), lane >= 32))


def shift_col(x, dc, stride):
    n = x.shape[1]
    col = lax.rem(iota((1, n), 1), 32)
    if dc > 0:
        return keep(roll(x, -stride), col < 32 - stride)
    return keep(roll(x, stride), col >= stride)


def gather(y_ref, tap_rows, lo, hi, n, edge, stride):
    total = None
    for dc in (0, -1, 1):
        base = 4 + dc
        part = y_ref[base * tap_rows : (base + 1) * tap_rows, lo:hi]
        for dr in (-1, 1):
            tap = base + 3 * dr
            rows = slice(tap * tap_rows, (tap + 1) * tap_rows)
            if dr > 0 and hi == n:
                moved = [edge(y_ref[rows, :LANES], dr)]
                if hi - lo > LANES:
                    moved = [y_ref[rows, lo + LANES : hi]] + moved
                moved = jnp.concatenate(moved, axis=1) if len(moved) > 1 else moved[0]
            elif dr < 0 and lo == 0:
                moved = [edge(y_ref[rows, n - LANES : n], dr)]
                if hi - lo > LANES:
                    moved = moved + [y_ref[rows, : hi - LANES]]
                moved = jnp.concatenate(moved, axis=1) if len(moved) > 1 else moved[0]
            else:
                moved = y_ref[rows, lo + dr * LANES : hi + dr * LANES]
            part = part + moved
        if dc != 0:
            part = shift_col(part, dc, stride)
        total = part if total is None else total + part
    return total


def gated(g):
    e = jnp.exp(-jnp.abs(g))
    inv = 1.0 / (1.0 + e)
    gate = jnp.where(g >= 0, inv, e * inv)
    return gate, jnp.minimum(g, 0.0) - jnp.log(1.0 + e)


def fold(x):
    total = x[:, :LANES]
    for at in range(LANES, x.shape[1], LANES):
        total = total + x[:, at : at + LANES]
    return total


def mix(mat, bias, x, exact):
    n = x.shape[1]
    if exact:
        stack = [x, x]
    else:
        high, rest = split_two(x)
        stack = [high, rest, high]
    stack = jnp.concatenate(stack, axis=0).astype(bf16)
    return jnp.dot(mat, stack, preferred_element_type=f32) + wide(bias, n)


def product(first, second, third, bias, spread, y_ref, rows, lo):
    n = spread.shape[1]
    h = jnp.dot(first[...], spread, preferred_element_type=f32)
    h = jnp.maximum(h, 0.0).astype(bf16)
    h = jnp.dot(second[...], h, preferred_element_type=f32)
    h = jnp.maximum(h + wide(bias[...], n), 0.0).astype(bf16)
    y_ref[:rows, lo : lo + n] = jnp.dot(third[...], h, preferred_element_type=f32)


def mid_step(s, k, exact):
    state, u_ref, q_ref, y_ref = s["state"], s["u"], s["q"], s["y"]
    channels, n = state.shape
    block = 4 * LANES
    sub = iota((8, 1), 0)
    mat = s["mix_mid"][k, :, : (2 if exact else 3) * channels]
    for lo in range(0, n, block):
        u_ref[:, lo : lo + block] = mix(
            mat, s["mix_bias_mid"][k], state[:, lo : lo + block], exact
        )
    for lo in range(0, n, block):
        q = u_ref[:16, lo : lo + block]
        q = jnp.concatenate([q[:8], jnp.where(sub == 4, 1.0, q[8:])], axis=0)
        for dc in (-1, 0, 1):
            x = q if dc == 0 else shift_col(q, dc, 1)
            q_ref[dc + 1, :, LANES + lo : LANES + lo + block] = x.astype(bf16)
            if lo == 0:
                q_ref[dc + 1, :, LANES + n :] = edge_mid(x[:, :LANES], 1).astype(bf16)
            if lo + block == n:
                q_ref[dc + 1, :, :LANES] = edge_mid(x[:, block - LANES :], -1).astype(bf16)
    for lo in range(0, n, min(CHUNK, n)):
        taps = []
        for dr in (-1, 0, 1):
            at = lo + LANES * (1 + dr)
            for dc in (-1, 0, 1):
                taps.append(q_ref[dc + 1, :, at : at + min(CHUNK, n)])
        product(
            s["w1t_mid"].at[k],
            s["w2t_mid"].at[k],
            s["w3p_mid"].at[k],
            s["b2_mid"].at[k],
            jnp.concatenate(taps, axis=0),
            y_ref,
            9 * channels,
            lo,
        )
    score = None
    width = 2 * LANES
    for lo in range(0, n, width):
        out = gather(y_ref, channels, lo, lo + width, n, edge_mid, 1) + wide(s["b3_mid"][k], width)
        gate, logs = gated(out[:16] + 2.0)
        logs = fold(logs)
        score = logs if score is None else score + logs
        u = u_ref[:, lo : lo + width]
        state[:8, lo : lo + width] = u[:8]
        late = (u[8:16] + out[8:16]) * pltpu.roll(gate[8:16], 4, 0)
        state[8:16, lo : lo + width] = jnp.where(sub < 4, u[8:16], late)
        state[16:, lo : lo + width] = (u[16:] + out[16:]) * gate[:8]
    return keep(score, iota((16, 1), 0) < channels // 2)


def squeeze(s):
    state, top = s["state"], s["top"]
    odd = lax.rem(iota((1, LANES), 1), 2) == 1
    sub = iota((8, 1), 0)
    for v in range(4):
        tails = []
        for i in range(2):
            t = (2 * v + i) * LANES
            a = state[8:, t : t + LANES]
            t = t + 8 * LANES
            b = state[8:, t : t + LANES]
            even_col = jnp.where(odd, roll(b, 1), a)
            odd_col = jnp.where(odd, b, roll(a, -1))
            cols = slice(v * LANES, (v + 1) * LANES)
            top[16 * i : 16 * i + 8, cols] = even_col[8:]
            top[16 * i + 8 : 16 * i + 16, cols] = odd_col[8:]
            top[32 + 8 * i : 40 + 8 * i, cols] = jnp.where(
                sub < 4, pltpu.roll(odd_col[:8], 4, 0), even_col[:8]
            )


def top_step(s, k):
    state, u_ref, q_ref, y_ref = s["top"], s["u_top"], s["q_top"], s["y_top"]
    channels, n = state.shape
    half = channels // 2
    mat = s["mix_top"][k, :, : 3 * channels]
    u_ref[...] = mix(mat, s["mix_bias_top"][k], state[...], False)
    q = u_ref[:half, :]
    for dc in (-1, 0, 1):
        x = q if dc == 0 else shift_col(q, dc, 2)
        q_ref[dc + 1, :, LANES : LANES + n] = x
        q_ref[dc + 1, :, LANES + n :] = edge_top(x[:, :LANES], 1)
        q_ref[dc + 1, :, :LANES] = edge_top(x[:, n - LANES :], -1)
    ones = jnp.where(iota((8, min(CHUNK, n)), 0) == 0, 1.0, 0.0)
    for lo in range(0, n, min(CHUNK, n)):
        taps = []
        for dr in (-1, 0, 1):
            at = lo + LANES * (1 + dr)
            for dc in (-1, 0, 1):
                taps.append(q_ref[dc + 1, :, at : at + min(CHUNK, n)])
        product(
            s["w1t_top"].at[k],
            s["w2t_top"].at[k],
            s["w3_top"].at[k],
            s["b2_top"].at[k],
            jnp.concatenate(taps + [ones], axis=0).astype(bf16),
            y_ref,
            9 * channels,
            lo,
        )
    score = None
    width = LANES
    for lo in range(0, n, width):
        out = gather(y_ref, channels, lo, lo + width, n, edge_top, 2) + wide(s["b3_top"][k], width)
        gate, logs = gated(out[:half] + 2.0)
        score = logs if score is None else score + logs
        state[:half, lo : lo + width] = u_ref[:half, lo : lo + width]
        state[half:, lo : lo + width] = (u_ref[half:, lo : lo + width] + out[half:]) * gate
    return score


def work_scratch(steps_mid, steps_top, hidden, channels, top_channels, cells):
    n_top = cells // 4
    return {
        "mix_mid": pltpu.VMEM((steps_mid, channels, 3 * channels), bf16),
        "mix_bias_mid": pltpu.VMEM((steps_mid, channels, LANES), f32),
        "b3_mid": pltpu.VMEM((steps_mid, channels, LANES), f32),
        "mix_top": pltpu.VMEM((steps_top, top_channels, 3 * top_channels), bf16),
        "mix_bias_top": pltpu.VMEM((steps_top, top_channels, LANES), f32),
        "b3_top": pltpu.VMEM((steps_top, top_channels, LANES), f32),
        "w1t_mid": pltpu.VMEM((steps_mid, hidden, 144), bf16),
        "w2t_mid": pltpu.VMEM((steps_mid, hidden, hidden), bf16),
        "b2_mid": pltpu.VMEM((steps_mid, hidden, LANES), f32),
        "w3f_mid": pltpu.VMEM((9 * channels, hidden), f32),
        "w3p_mid": pltpu.VMEM((steps_mid, 9 * channels, hidden), bf16),
        "w1t_top": pltpu.VMEM((steps_top, hidden, 9 * top_channels // 2 + 8), bf16),
        "w2t_top": pltpu.VMEM((steps_top, hidden, hidden), bf16),
        "b2_top": pltpu.VMEM((steps_top, hidden, LANES), f32),
        "state": pltpu.VMEM((channels, cells), f32),
        "u": pltpu.VMEM((channels, cells), f32),
        "q": pltpu.VMEM((3, 16, cells + 2 * LANES), bf16),
        "y": pltpu.VMEM((9 * channels, cells), f32),
        "top": pltpu.VMEM((top_channels, n_top), f32),
        "u_top": pltpu.VMEM((top_channels, n_top), f32),
        "q_top": pltpu.VMEM((3, top_channels // 2, n_top + 2 * LANES), f32),
        "y_top": pltpu.VMEM((9 * top_channels, n_top), f32),
        "turned": pltpu.VMEM((n_top, LANES), f32),
    }


NAMES = (
    "shift_mid",
    "gain_mid",
    "lower_mid",
    "upper_mid",
    "diag_mid",
    "w1_mid",
    "first_bias_mid",
    "w2_mid",
    "second_bias_mid",
    "w3_mid",
    "third_bias_mid",
    "shift_top",
    "gain_top",
    "lower_top",
    "upper_top",
    "diag_top",
    "w1_top",
    "first_bias_top",
    "w2_top",
    "second_bias_top",
    "w3_top",
    "third_bias_top",
)


def parameters(params):
    (
        shift_mid, gain_mid, lower_mid, upper_mid, diag_mid, first_mid, first_bias_mid, second_mid,
        second_bias_mid, third_mid, third_bias_mid, shift_top, gain_top, lower_top, upper_top,
        diag_top, first_top, first_bias_top, second_top, second_bias_top, third_top, third_bias_top,
    ) = params
    steps_mid, hidden = first_bias_mid.shape
    steps_top = first_bias_top.shape[0]
    w1_top = first_top.reshape(steps_top, -1, hidden)
    w3_mid = third_mid.transpose(0, 1, 3, 2).reshape(steps_mid, -1, hidden)
    w3_top = third_top.transpose(0, 1, 3, 2).reshape(steps_top, -1, hidden)
    return (
        shift_mid, gain_mid, lower_mid, upper_mid, diag_mid, first_mid, first_bias_mid, second_mid,
        second_bias_mid, w3_mid, third_bias_mid, shift_top, gain_top, lower_top, upper_top,
        diag_top, w1_top, first_bias_top, second_top, second_bias_top, w3_top, third_bias_top,
    )


def kernel(dims, keys, *refs):
    n_rows, n_chan, height, width, count = dims
    sources, refs = refs[:count], refs[count:]
    (mid_out, top_out, lik_out), refs = refs[:3], refs[3:]
    held, refs = refs[:count], refs[count:]
    s, refs = dict(zip(keys, refs)), refs[len(keys) :]
    outbox, inbox, z_send, z_recv, w_sem, send_sem, recv_sem, z_send_sem, z_recv_sem = refs
    images = held[0]
    p = dict(zip(NAMES, held[1:]))
    s["w3_top"] = p["w3_top"]
    peers = n_rows * n_chan
    b = lax.axis_index("batch")
    r = lax.axis_index("rows")
    c = lax.axis_index("chan")
    me = r * n_chan + c
    quad = lax.div(r, 2)
    side = lax.rem(r, 2)

    def device(row, chan):
        return {"batch": b, "rows": row, "chan": chan}

    def key(row, chan):
        y = chan // 2
        far = row // 4
        when = 15 * row * (1 - far) + (53 + 4 * row) * far + 12 * (y + y // 2 * (5 - 2 * y))
        return ((when + 3 * (1 - chan % 2)) * n_rows + row) * n_chan + chan

    order = sorted((key(row, chan), row, chan) for row in range(n_rows) for chan in range(n_chan))
    mine = key(r, c)

    first = pltpu.make_async_copy(sources[0], held[0], w_sem.at[0])
    first.start()
    barrier = pltpu.get_barrier_semaphore()

    for at, row, chan in order[1:]:

        @pl.when(at > mine)
        def _():
            pl.semaphore_signal(barrier, inc=1, device_id=device(row, chan), device_id_type=MESH)

    earlier = 0
    for at, _, _ in order:
        earlier = earlier + jnp.where(at < mine, 1, 0)
    first.wait()
    for dest in range(n_chan):
        x = images[dest]
        x = jnp.concatenate([x[:8], x[8:16], x[16:], jnp.zeros((8, width), f32)], axis=1)
        outbox[dest] = pltpu.roll(x, quad * 32, 1).astype(bf16)
    @pl.when(earlier > 0)
    def _():
        pl.semaphore_wait(barrier, earlier)

    def send(row, chan):
        pltpu.make_async_remote_copy(
            src_ref=outbox.at[chan],
            dst_ref=inbox.at[me],
            send_sem=send_sem,
            recv_sem=recv_sem.at[me],
            device_id=device(row, chan),
            device_id_type=MESH,
        ).start()

    def arrive(row, chan):
        slot = row * n_chan + chan
        pltpu.make_async_remote_copy(
            src_ref=outbox.at[0],
            dst_ref=inbox.at[slot],
            send_sem=send_sem,
            recv_sem=recv_sem.at[slot],
            device_id=device(r, c),
            device_id_type=MESH,
        ).wait_recv()

    for at, row, chan in order[:-1]:

        @pl.when(at < mine)
        def _():
            send(row, chan)

    copies = []
    for at in range(1, count):
        copy = pltpu.make_async_copy(sources[at], held[at], w_sem.at[at])
        copy.start()
        copies.append(copy)
    inbox[me] = outbox[c]
    for copy in copies:
        copy.wait()
    prepare(p, s)
    channels = p["shift_mid"].shape[1]
    top_channels = p["shift_top"].shape[1]
    half = channels // 2
    cells = height * width
    fixed = cells * (jnp.sum(p["gain_mid"][...]) + jnp.sum(p["diag_mid"][...]))
    fixed = fixed + cells // 4 * (jnp.sum(p["gain_top"][...]) + jnp.sum(p["diag_top"][...]))
    fixed = fixed - 0.5 * log_two_pi * channels * cells

    for at, row, chan in order[1:]:

        @pl.when(at > mine)
        def _():
            arrive(row, chan)
            send(row, chan)

    for at, row, chan in order[:-1]:

        @pl.when(at < mine)
        def _():
            arrive(row, chan)


    state = s["state"]
    lane = iota((1, LANES), 1)
    for t in range(height // 4):
        letters = [inbox[16 * k + t].astype(f32) for k in range(4)]
        for slab in range(3):
            x = letters[(3 - slab) % 4]
            for k in range(3):
                x = jnp.where(lax.div(lane, 32) == k, letters[(k - slab) % 4], x)
            state[8 * slab : 8 * slab + 8, t * LANES : (t + 1) * LANES] = roll(x, -32 * slab)

    score = None
    for k in range(p["shift_mid"].shape[0]):
        logs = mid_step(s, k, k == 0)
        score = logs if score is None else score + logs

    for to in range(n_chan):
        start = pl.multiple_of((side * n_chan + to) * LANES, LANES)
        z = state[:16, pl.ds(start, LANES)]
        z_send[to] = jnp.where(
            lane < 32,
            pltpu.roll(z[:8], LANES - quad * 32, 1),
            pltpu.roll(z[8:], LANES + 32 - quad * 32, 1),
        )
    z_copies = []
    for d in range(1, n_chan):
        other = lax.rem(c + d, n_chan)
        copy = pltpu.make_async_remote_copy(
            src_ref=z_send.at[other],
            dst_ref=z_recv.at[c],
            send_sem=z_send_sem.at[d],
            recv_sem=z_recv_sem.at[d],
            device_id=device(r, other),
            device_id_type=MESH,
        )
        copy.start()
        z_copies.append(copy)
    z_recv[c] = z_send[c]

    squares = fold(state[:16, :] * state[:16, :])
    score = score - 0.5 * keep(squares, iota((16, 1), 0) < half)
    squeeze(s)
    score_top = None
    for k in range(p["shift_top"].shape[0]):
        logs = top_step(s, k)
        score_top = logs if score_top is None else score_top + logs
    top = s["top"]
    squares = fold(top[...] * top[...])
    total = jnp.sum(score, axis=0, keepdims=True) + jnp.sum(score_top, axis=0, keepdims=True)
    total = total - 0.5 * jnp.sum(squares, axis=0, keepdims=True)
    lik_out[0] = (jnp.sum(total) + fixed) / (channels * cells)
    turned = s["turned"]
    for v in range(4):
        turned[v * LANES : (v + 1) * LANES, :top_channels] = jnp.transpose(
            top[:, v * LANES : (v + 1) * LANES]
        )
    for v in range(4):
        start = v * LANES + quad * 32 + side
        top_out[0, v * 16 : (v + 1) * 16, :] = turned[pl.ds(start, 16, stride=2), :][
            :, :top_channels
        ]

    for d in range(1, n_chan):
        pltpu.make_async_remote_copy(
            src_ref=z_send.at[0],
            dst_ref=z_recv.at[lax.rem(c + n_chan - d, n_chan)],
            send_sem=z_send_sem.at[d],
            recv_sem=z_recv_sem.at[d],
            device_id=device(r, c),
            device_id_type=MESH,
        ).wait_recv()
    for img in range(n_chan):
        z = z_recv[img]
        mid_out[img, :8, :] = z[:, :width]
        mid_out[img, 8:, :] = z[:4, width : 2 * width]
    for copy in z_copies:
        copy.wait_send()
    pltpu.make_async_remote_copy(
        src_ref=inbox.at[pl.ds(0, peers - 1)],
        dst_ref=inbox.at[pl.ds(0, peers - 1)],
        send_sem=send_sem,
        recv_sem=recv_sem.at[0],
        device_id=device(r, c),
        device_id_type=MESH,
    ).wait_send()


def deliver(mid, top, lik, mid_out, top_out, lik_out):
    for img in range(mid.shape[0]):
        mid_out[img, :, 0, :] = mid[img]
    top_out[...] = top[...]
    lik_out[0] = lik[0]


def body(sizes, images, *params):
    n_rows, n_chan = sizes
    n_imgs, channels, own_rows, width = images.shape
    peers = n_rows * n_chan
    height = own_rows * peers
    params = parameters(params)
    hidden = params[6].shape[1]
    steps_mid, steps_top = params[0].shape[0], params[11].shape[0]
    top_channels = params[11].shape[1]
    half = channels // 2
    cells = height * width
    own = cells // 4 // n_rows
    operands = (images.reshape(n_imgs, channels, width),) + params
    vmem = pl.BlockSpec(memory_space=pltpu.VMEM)
    smem = pl.BlockSpec(memory_space=pltpu.SMEM)
    count = len(operands)
    work = work_scratch(steps_mid, steps_top, hidden, channels, top_channels, cells)
    mid, top, lik = pl.pallas_call(
        functools.partial(kernel, (n_rows, n_chan, height, width, count), list(work)),
        out_shape=(
            pltpu.VMEM((n_imgs, half, width), f32),
            pltpu.VMEM((1, own, top_channels), f32),
            jax.ShapeDtypeStruct((1,), f32),
        ),
        in_specs=[pl.BlockSpec(memory_space=pl.ANY)] * count,
        out_specs=(vmem, vmem, smem),
        scratch_shapes=[pltpu.VMEM(x.shape, x.dtype) for x in operands]
        + list(work.values())
        + [
            pltpu.VMEM((n_chan, 8, LANES), bf16),
            pltpu.VMEM((peers, 8, LANES), bf16),
            pltpu.VMEM((n_chan, 8, LANES), f32),
            pltpu.VMEM((n_chan, 8, LANES), f32),
            pltpu.SemaphoreType.DMA((count,)),
            pltpu.SemaphoreType.DMA,
            pltpu.SemaphoreType.DMA((peers,)),
            pltpu.SemaphoreType.DMA((n_chan,)),
            pltpu.SemaphoreType.DMA((n_chan,)),
        ],
        compiler_params=pltpu.CompilerParams(
            collective_id=0, has_side_effects=True, vmem_limit_bytes=56 * 1024 * 1024
        ),
        name="flow",
    )(*operands)
    latent_mid, top, lik = pl.pallas_call(
        deliver,
        out_shape=(
            jax.ShapeDtypeStruct((n_imgs, half, own_rows, width), f32),
            jax.ShapeDtypeStruct(top.shape, f32),
            jax.ShapeDtypeStruct(lik.shape, f32),
        ),
        in_specs=[vmem, vmem, smem],
        out_specs=(vmem, vmem, smem),
        compiler_params=pltpu.CompilerParams(vmem_limit_bytes=4 * 1024 * 1024),
        name="deliver",
    )(mid, top, lik)
    latent_top = top.reshape(1, -1, width // 2, top_channels).transpose(0, 3, 1, 2)
    return latent_mid, latent_top, lik


def solution(mesh):
    sizes = (mesh.shape["rows"], mesh.shape["chan"])
    placed = (P("batch", None, ("rows", "chan"), None),) + (P(),) * 22
    return jax.shard_map(
        functools.partial(body, sizes),
        mesh=mesh,
        in_specs=placed,
        out_specs=(
            P("batch", None, ("rows", "chan"), None),
            P(("batch", "chan"), None, "rows", None),
            P(("batch", "chan")),
        ),
        check_vma=False,
    )
```

```python
import functools
import math

import jax
import jax.numpy as jnp
from jax import lax
from jax.experimental import pallas as pl
from jax.experimental.pallas import tpu as pltpu
from jax.sharding import PartitionSpec as P

MESH = pl.DeviceIdType.MESH
LANES = 128
CHUNK = 1024
FINE = lax.Precision.HIGHEST
log_two_pi = math.log(2.0 * math.pi)
f32 = jnp.float32
bf16 = jnp.bfloat16


def iota(shape, dim):
    return lax.broadcasted_iota(jnp.int32, shape, dim)


def dot_nt(a, b, precision=None):
    return lax.dot_general(
        a, b, (((1,), (1,)), ((), ())), preferred_element_type=f32, precision=precision
    )


def roll(x, amount):
    n = x.shape[1]
    amount = amount % n
    return x if amount == 0 else pltpu.roll(x, amount, 1)


def keep(x, ok):
    return jnp.where(ok, x, 0.0)


def mid_map(channels):
    i = iota((channels, channels), 0)
    j = iota((channels, channels), 1)
    source = jnp.where(i < 12, i, jnp.where(i < 16, i + 8, i - 4))
    return jnp.where(source == j, 1.0, 0.0)


def eye_map(channels):
    return jnp.where(iota((channels, channels), 0) == iota((channels, channels), 1), 1.0, 0.0)


def squeeze_map(channels):
    i = iota((channels, channels), 0)
    j = iota((channels, channels), 1)
    low = 4 * lax.rem(i, 8) + lax.div(i, 8)
    k = i - 32
    place = 2 * lax.div(k, 8) + 1 - lax.div(lax.rem(k + 64, 8), 4)
    high = 4 * (8 + lax.rem(k + 64, 4)) + place
    return jnp.where(jnp.where(i < 32, low, high) == j, 1.0, 0.0)


def split_two(x):
    high = x.astype(bf16).astype(f32)
    return high, x - high


def mixing(lower, upper, diag_row, gain_row, shift_row, out_map, in_map, exact):
    channels = lower.shape[0]
    i = iota((channels, channels), 0)
    j = iota((channels, channels), 1)
    eye = jnp.where(i == j, 1.0, 0.0)
    low = jnp.where(i > j, lower, 0.0) + eye
    upp = (jnp.where(i < j, upper, 0.0) + eye * jnp.exp(diag_row)) * jnp.exp(gain_row)
    rows = jnp.dot(out_map, low, precision=FINE, preferred_element_type=f32)
    mat = jnp.dot(rows, upp, precision=FINE, preferred_element_type=f32)
    bias = jnp.sum(mat * shift_row, axis=1, keepdims=True)
    if in_map is not None:
        mat = dot_nt(mat, in_map, FINE)
    high, rest = split_two(mat)
    parts = [high, rest] if exact else [high, high, rest]
    return jnp.concatenate(parts, axis=1).astype(bf16), bias


def mapped_column(row, mapping):
    return jnp.sum(mapping * row, axis=1, keepdims=True)


def prepare(p, s):
    steps_mid, channels = p["shift_mid"].shape
    steps_top, top_channels = p["shift_top"].shape
    hidden = p["w2_mid"].shape[1]
    half = channels // 2
    mapping = mid_map(channels)
    natural = eye_map(top_channels)
    for k in range(steps_mid):
        mat, bias = mixing(
            p["lower_mid"][k],
            p["upper_mid"][k],
            p["diag_mid"][k : k + 1, :],
            p["gain_mid"][k : k + 1, :],
            p["shift_mid"][k : k + 1, :],
            mapping,
            None if k == 0 else mapping,
            k == 0,
        )
        s["mix_mid"][k, :, : mat.shape[1]] = mat
        s["mix_bias_mid"][k] = jnp.broadcast_to(bias, (channels, LANES))
        s["b3_mid"][k] = jnp.broadcast_to(
            mapped_column(p["third_bias_mid"][k : k + 1, :], mapping), (channels, LANES)
        )
    for k in range(steps_top):
        mat, bias = mixing(
            p["lower_top"][k],
            p["upper_top"][k],
            p["diag_top"][k : k + 1, :],
            p["gain_top"][k : k + 1, :],
            p["shift_top"][k : k + 1, :],
            natural,
            squeeze_map(top_channels) if k == 0 else None,
            False,
        )
        s["mix_top"][k, :, : mat.shape[1]] = mat
        s["mix_bias_top"][k] = jnp.broadcast_to(bias, (top_channels, LANES))
        s["b3_top"][k] = jnp.broadcast_to(
            mapped_column(p["third_bias_top"][k : k + 1, :], natural), (top_channels, LANES)
        )
    for k in range(steps_mid):
        taps = []
        for tap in range(9):
            extra = [jnp.zeros((16 - half, hidden), f32)]
            if tap == 4:
                row = p["first_bias_mid"][k : k + 1, :].astype(f32)
                extra = [row, jnp.zeros((15 - half, hidden), f32)]
            taps.append(jnp.concatenate([p["w1_mid"][k, tap].astype(f32)] + extra, axis=0))
        s["w1t_mid"][k] = jnp.transpose(jnp.concatenate(taps, axis=0)).astype(bf16)
        s["w2t_mid"][k] = jnp.transpose(p["w2_mid"][k].astype(f32)).astype(bf16)
        s["b2_mid"][k] = jnp.transpose(
            jnp.broadcast_to(p["second_bias_mid"][k : k + 1, :], (LANES, hidden))
        )
        for tap in range(9):
            w = p["w3_mid"][k, tap * channels : (tap + 1) * channels, :].astype(f32)
            w = jnp.concatenate([w[:12], w[20:24], w[12:20]], axis=0)
            s["w3f_mid"][tap * channels : (tap + 1) * channels, :] = w
        s["w3p_mid"][k] = s["w3f_mid"][...].astype(bf16)
    for k in range(steps_top):
        row = p["first_bias_top"][k : k + 1, :].astype(f32)
        w = jnp.concatenate(
            [p["w1_top"][k].astype(f32), row, jnp.zeros((7, hidden), f32)], axis=0
        )
        s["w1t_top"][k] = jnp.transpose(w).astype(bf16)
        s["w2t_top"][k] = jnp.transpose(p["w2_top"][k].astype(f32)).astype(bf16)
        s["b2_top"][k] = jnp.transpose(
            jnp.broadcast_to(p["second_bias_top"][k : k + 1, :], (LANES, hidden))
        )


def wide(x, n):
    return jnp.concatenate([x] * (n // LANES), axis=1)


def lane_of(n):
    return lax.rem(iota((1, n), 1), LANES)


def edge_mid(x, dr):
    lane = iota((1, LANES), 1)
    if dr > 0:
        return keep(roll(x, -32), lane < 96)
    return keep(roll(x, 32), lane >= 32)


def edge_top(x, dr):
    lane = iota((1, LANES), 1)
    odd = lax.rem(lane, 2) == 1
    if dr > 0:
        return jnp.where(odd, keep(roll(x, -31), lane < 96), roll(x, -1))
    return jnp.where(odd, roll(x, 1), keep(roll(x, 31), lane >= 32))


def shift_col(x, dc, stride):
    n = x.shape[1]
    col = lax.rem(iota((1, n), 1), 32)
    if dc > 0:
        return keep(roll(x, -stride), col < 32 - stride)
    return keep(roll(x, stride), col >= stride)


def gather(y_ref, tap_rows, lo, hi, n, edge, stride):
    total = None
    for dc in (0, -1, 1):
        base = 4 + dc
        part = y_ref[base * tap_rows : (base + 1) * tap_rows, lo:hi]
        for dr in (-1, 1):
            tap = base + 3 * dr
            rows = slice(tap * tap_rows, (tap + 1) * tap_rows)
            if dr > 0 and hi == n:
                moved = [edge(y_ref[rows, :LANES], dr)]
                if hi - lo > LANES:
                    moved = [y_ref[rows, lo + LANES : hi]] + moved
                moved = jnp.concatenate(moved, axis=1) if len(moved) > 1 else moved[0]
            elif dr < 0 and lo == 0:
                moved = [edge(y_ref[rows, n - LANES : n], dr)]
                if hi - lo > LANES:
                    moved = moved + [y_ref[rows, : hi - LANES]]
                moved = jnp.concatenate(moved, axis=1) if len(moved) > 1 else moved[0]
            else:
                moved = y_ref[rows, lo + dr * LANES : hi + dr * LANES]
            part = part + moved
        if dc != 0:
            part = shift_col(part, dc, stride)
        total = part if total is None else total + part
    return total


def gated(g):
    e = jnp.exp(-jnp.abs(g))
    inv = 1.0 / (1.0 + e)
    gate = jnp.where(g >= 0, inv, e * inv)
    return gate, jnp.minimum(g, 0.0) - jnp.log(1.0 + e)


def fold(x):
    total = x[:, :LANES]
    for at in range(LANES, x.shape[1], LANES):
        total = total + x[:, at : at + LANES]
    return total


def mix(mat, bias, x, exact):
    n = x.shape[1]
    if exact:
        stack = [x, x]
    else:
        high, rest = split_two(x)
        stack = [high, rest, high]
    stack = jnp.concatenate(stack, axis=0).astype(bf16)
    return jnp.dot(mat, stack, preferred_element_type=f32) + wide(bias, n)


def product(first, second, third, bias, spread, y_ref, rows, lo):
    n = spread.shape[1]
    h = jnp.dot(first[...], spread, preferred_element_type=f32)
    h = jnp.maximum(h, 0.0).astype(bf16)
    h = jnp.dot(second[...], h, preferred_element_type=f32)
    h = jnp.maximum(h + wide(bias[...], n), 0.0).astype(bf16)
    y_ref[:rows, lo : lo + n] = jnp.dot(third[...], h, preferred_element_type=f32)


def mid_step(s, k, exact):
    state, u_ref, q_ref, y_ref = s["state"], s["u"], s["q"], s["y"]
    channels, n = state.shape
    block = 4 * LANES
    sub = iota((8, 1), 0)
    mat = s["mix_mid"][k, :, : (2 if exact else 3) * channels]
    for lo in range(0, n, block):
        u_ref[:, lo : lo + block] = mix(
            mat, s["mix_bias_mid"][k], state[:, lo : lo + block], exact
        )
    for lo in range(0, n, block):
        q = u_ref[:16, lo : lo + block]
        q = jnp.concatenate([q[:8], jnp.where(sub == 4, 1.0, q[8:])], axis=0)
        for dc in (-1, 0, 1):
            x = q if dc == 0 else shift_col(q, dc, 1)
            q_ref[dc + 1, :, LANES + lo : LANES + lo + block] = x.astype(bf16)
            if lo == 0:
                q_ref[dc + 1, :, LANES + n :] = edge_mid(x[:, :LANES], 1).astype(bf16)
            if lo + block == n:
                q_ref[dc + 1, :, :LANES] = edge_mid(x[:, block - LANES :], -1).astype(bf16)
    for lo in range(0, n, min(CHUNK, n)):
        taps = []
        for dr in (-1, 0, 1):
            at = lo + LANES * (1 + dr)
            for dc in (-1, 0, 1):
                taps.append(q_ref[dc + 1, :, at : at + min(CHUNK, n)])
        product(
            s["w1t_mid"].at[k],
            s["w2t_mid"].at[k],
            s["w3p_mid"].at[k],
            s["b2_mid"].at[k],
            jnp.concatenate(taps, axis=0),
            y_ref,
            9 * channels,
            lo,
        )
    score = None
    width = 2 * LANES
    for lo in range(0, n, width):
        out = gather(y_ref, channels, lo, lo + width, n, edge_mid, 1) + wide(s["b3_mid"][k], width)
        gate, logs = gated(out[:16] + 2.0)
        logs = fold(logs)
        score = logs if score is None else score + logs
        u = u_ref[:, lo : lo + width]
        state[:8, lo : lo + width] = u[:8]
        late = (u[8:16] + out[8:16]) * pltpu.roll(gate[8:16], 4, 0)
        state[8:16, lo : lo + width] = jnp.where(sub < 4, u[8:16], late)
        state[16:, lo : lo + width] = (u[16:] + out[16:]) * gate[:8]
    return keep(score, iota((16, 1), 0) < channels // 2)


def squeeze(s):
    state, top = s["state"], s["top"]
    odd = lax.rem(iota((1, LANES), 1), 2) == 1
    sub = iota((8, 1), 0)
    for v in range(4):
        tails = []
        for i in range(2):
            t = (2 * v + i) * LANES
            a = state[8:, t : t + LANES]
            t = t + 8 * LANES
            b = state[8:, t : t + LANES]
            even_col = jnp.where(odd, roll(b, 1), a)
            odd_col = jnp.where(odd, b, roll(a, -1))
            cols = slice(v * LANES, (v + 1) * LANES)
            top[16 * i : 16 * i + 8, cols] = even_col[8:]
            top[16 * i + 8 : 16 * i + 16, cols] = odd_col[8:]
            top[32 + 8 * i : 40 + 8 * i, cols] = jnp.where(
                sub < 4, pltpu.roll(odd_col[:8], 4, 0), even_col[:8]
            )


def top_step(s, k):
    state, u_ref, q_ref, y_ref = s["top"], s["u_top"], s["q_top"], s["y_top"]
    channels, n = state.shape
    half = channels // 2
    mat = s["mix_top"][k, :, : 3 * channels]
    u_ref[...] = mix(mat, s["mix_bias_top"][k], state[...], False)
    q = u_ref[:half, :]
    for dc in (-1, 0, 1):
        x = q if dc == 0 else shift_col(q, dc, 2)
        q_ref[dc + 1, :, LANES : LANES + n] = x
        q_ref[dc + 1, :, LANES + n :] = edge_top(x[:, :LANES], 1)
        q_ref[dc + 1, :, :LANES] = edge_top(x[:, n - LANES :], -1)
    ones = jnp.where(iota((8, min(CHUNK, n)), 0) == 0, 1.0, 0.0)
    for lo in range(0, n, min(CHUNK, n)):
        taps = []
        for dr in (-1, 0, 1):
            at = lo + LANES * (1 + dr)
            for dc in (-1, 0, 1):
                taps.append(q_ref[dc + 1, :, at : at + min(CHUNK, n)])
        product(
            s["w1t_top"].at[k],
            s["w2t_top"].at[k],
            s["w3_top"].at[k],
            s["b2_top"].at[k],
            jnp.concatenate(taps + [ones], axis=0).astype(bf16),
            y_ref,
            9 * channels,
            lo,
        )
    score = None
    width = LANES
    for lo in range(0, n, width):
        out = gather(y_ref, channels, lo, lo + width, n, edge_top, 2) + wide(s["b3_top"][k], width)
        gate, logs = gated(out[:half] + 2.0)
        score = logs if score is None else score + logs
        state[:half, lo : lo + width] = u_ref[:half, lo : lo + width]
        state[half:, lo : lo + width] = (u_ref[half:, lo : lo + width] + out[half:]) * gate
    return score


def work_scratch(steps_mid, steps_top, hidden, channels, top_channels, cells):
    n_top = cells // 4
    return {
        "mix_mid": pltpu.VMEM((steps_mid, channels, 3 * channels), bf16),
        "mix_bias_mid": pltpu.VMEM((steps_mid, channels, LANES), f32),
        "b3_mid": pltpu.VMEM((steps_mid, channels, LANES), f32),
        "mix_top": pltpu.VMEM((steps_top, top_channels, 3 * top_channels), bf16),
        "mix_bias_top": pltpu.VMEM((steps_top, top_channels, LANES), f32),
        "b3_top": pltpu.VMEM((steps_top, top_channels, LANES), f32),
        "w1t_mid": pltpu.VMEM((steps_mid, hidden, 144), bf16),
        "w2t_mid": pltpu.VMEM((steps_mid, hidden, hidden), bf16),
        "b2_mid": pltpu.VMEM((steps_mid, hidden, LANES), f32),
        "w3f_mid": pltpu.VMEM((9 * channels, hidden), f32),
        "w3p_mid": pltpu.VMEM((steps_mid, 9 * channels, hidden), bf16),
        "w1t_top": pltpu.VMEM((steps_top, hidden, 9 * top_channels // 2 + 8), bf16),
        "w2t_top": pltpu.VMEM((steps_top, hidden, hidden), bf16),
        "b2_top": pltpu.VMEM((steps_top, hidden, LANES), f32),
        "state": pltpu.VMEM((channels, cells), f32),
        "u": pltpu.VMEM((channels, cells), f32),
        "q": pltpu.VMEM((3, 16, cells + 2 * LANES), bf16),
        "y": pltpu.VMEM((9 * channels, cells), f32),
        "top": pltpu.VMEM((top_channels, n_top), f32),
        "u_top": pltpu.VMEM((top_channels, n_top), f32),
        "q_top": pltpu.VMEM((3, top_channels // 2, n_top + 2 * LANES), f32),
        "y_top": pltpu.VMEM((9 * top_channels, n_top), f32),
        "turned": pltpu.VMEM((n_top, LANES), f32),
    }


NAMES = (
    "shift_mid",
    "gain_mid",
    "lower_mid",
    "upper_mid",
    "diag_mid",
    "w1_mid",
    "first_bias_mid",
    "w2_mid",
    "second_bias_mid",
    "w3_mid",
    "third_bias_mid",
    "shift_top",
    "gain_top",
    "lower_top",
    "upper_top",
    "diag_top",
    "w1_top",
    "first_bias_top",
    "w2_top",
    "second_bias_top",
    "w3_top",
    "third_bias_top",
)


def parameters(params):
    (
        shift_mid, gain_mid, lower_mid, upper_mid, diag_mid, first_mid, first_bias_mid, second_mid,
        second_bias_mid, third_mid, third_bias_mid, shift_top, gain_top, lower_top, upper_top,
        diag_top, first_top, first_bias_top, second_top, second_bias_top, third_top, third_bias_top,
    ) = params
    steps_mid, hidden = first_bias_mid.shape
    steps_top = first_bias_top.shape[0]
    w1_top = first_top.reshape(steps_top, -1, hidden)
    w3_mid = third_mid.transpose(0, 1, 3, 2).reshape(steps_mid, -1, hidden)
    w3_top = third_top.transpose(0, 1, 3, 2).reshape(steps_top, -1, hidden)
    return (
        shift_mid, gain_mid, lower_mid, upper_mid, diag_mid, first_mid, first_bias_mid, second_mid,
        second_bias_mid, w3_mid, third_bias_mid, shift_top, gain_top, lower_top, upper_top,
        diag_top, w1_top, first_bias_top, second_top, second_bias_top, w3_top, third_bias_top,
    )


def kernel(dims, keys, *refs):
    n_rows, n_chan, height, width, count = dims
    sources, refs = refs[:count], refs[count:]
    (mid_out, top_out, lik_out), refs = refs[:3], refs[3:]
    held, refs = refs[:count], refs[count:]
    s, refs = dict(zip(keys, refs)), refs[len(keys) :]
    outbox, stage, inbox, z_send, z_recv, w_sem, refs = *refs[:6], refs[6:]
    stage_send, piece_send, stage_sem, hello_sem, piece_sem, z_send_sem, z_recv_sem = refs
    images = held[0]
    p = dict(zip(NAMES, held[1:]))
    s["w3_top"] = p["w3_top"]
    b = lax.axis_index("batch")
    r = lax.axis_index("rows")
    c = lax.axis_index("chan")
    quad = lax.div(r, 2)
    side = lax.rem(r, 2)

    def device(row, chan):
        return {"batch": b, "rows": row, "chan": chan}

    chans = []
    for q in range(n_chan):
        y = q // 2
        chans.append(2 * (y + y // 2 * (5 - 2 * y)) + 1 - q % 2)
    y = lax.div(c, 2)
    spot = 2 * (y + lax.div(y, 2) * (5 - 2 * y)) + 1 - lax.rem(c, 2)

    first = pltpu.make_async_copy(sources[0], held[0], w_sem.at[0])
    first.start()
    barrier = pltpu.get_barrier_semaphore()
    for row in range(1, n_rows):

        @pl.when(row > r)
        def _():
            pl.semaphore_signal(barrier, inc=1, device_id=device(row, c), device_id_type=MESH)

    for q in range(1, n_chan):

        @pl.when(q > spot)
        def _():
            pl.semaphore_signal(
                barrier, inc=1, device_id=device(r, chans[q]), device_id_type=MESH
            )

    first.wait()
    for dest in range(n_chan):
        x = images[dest]
        x = jnp.concatenate([x[:8], x[8:16], x[16:], jnp.zeros((8, width), f32)], axis=1)
        outbox[dest] = pltpu.roll(x, quad * 32, 1).astype(bf16)

    @pl.when(r + spot > 0)
    def _():
        pl.semaphore_wait(barrier, r + spot)

    def send_row(row):
        pltpu.make_async_remote_copy(
            src_ref=outbox,
            dst_ref=stage.at[r],
            send_sem=stage_send,
            recv_sem=stage_sem.at[r],
            device_id=device(row, c),
            device_id_type=MESH,
        ).start()

    def send_hello(q):
        pltpu.make_async_remote_copy(
            src_ref=outbox.at[chans[q]],
            dst_ref=inbox.at[c, r],
            send_sem=piece_send,
            recv_sem=hello_sem.at[c],
            device_id=device(r, chans[q]),
            device_id_type=MESH,
        ).start()

    def send_piece(row, q):
        pltpu.make_async_remote_copy(
            src_ref=stage.at[row, chans[q]],
            dst_ref=inbox.at[c, row],
            send_sem=piece_send,
            recv_sem=piece_sem.at[c],
            device_id=device(r, chans[q]),
            device_id_type=MESH,
        ).start()

    def await_copy(ref, sem):
        pltpu.make_async_remote_copy(
            src_ref=ref,
            dst_ref=ref,
            send_sem=stage_send,
            recv_sem=sem,
            device_id=device(r, c),
            device_id_type=MESH,
        ).wait_recv()

    for row in range(n_rows - 1):
        pl.when(row < r)(functools.partial(send_row, row))
    for q in range(n_chan - 1):
        pl.when(q < spot)(functools.partial(send_hello, q))
    copies = []
    for at in range(1, count):
        copy = pltpu.make_async_copy(sources[at], held[at], w_sem.at[at])
        copy.start()
        copies.append(copy)
    stage[r] = outbox[...]
    for copy in copies:
        copy.wait()
    prepare(p, s)
    channels = p["shift_mid"].shape[1]
    top_channels = p["shift_top"].shape[1]
    half = channels // 2
    cells = height * width
    fixed = cells * (jnp.sum(p["gain_mid"][...]) + jnp.sum(p["diag_mid"][...]))
    fixed = fixed + cells // 4 * (jnp.sum(p["gain_top"][...]) + jnp.sum(p["diag_top"][...]))
    fixed = fixed - 0.5 * log_two_pi * channels * cells

    for q in range(1, n_chan):

        @pl.when(q > spot)
        def _():
            await_copy(inbox.at[chans[q], 0], hello_sem.at[chans[q]])
            send_hello(q)

    for row in range(n_rows):

        @pl.when(row != r)
        def _():
            await_copy(stage.at[row], stage_sem.at[row])
            pl.when(row > r)(functools.partial(send_row, row))
            for q in range(n_chan):
                pl.when(q != spot)(functools.partial(send_piece, row, q))

    for row in range(n_rows):
        inbox[c, row] = stage[row, c]
    for q in range(n_chan):

        @pl.when(q < spot)
        def _():
            await_copy(inbox.at[chans[q], 0], hello_sem.at[chans[q]])

        @pl.when(q != spot)
        def _():
            await_copy(inbox.at[chans[q], pl.ds(0, n_rows - 1)], piece_sem.at[chans[q]])

    state = s["state"]
    lane = iota((1, LANES), 1)
    for t in range(height // 4):
        letters = [inbox[t % 8, 2 * k + t // 8].astype(f32) for k in range(4)]
        for slab in range(3):
            x = letters[(3 - slab) % 4]
            for k in range(3):
                x = jnp.where(lax.div(lane, 32) == k, letters[(k - slab) % 4], x)
            state[8 * slab : 8 * slab + 8, t * LANES : (t + 1) * LANES] = roll(x, -32 * slab)

    score = None
    for k in range(p["shift_mid"].shape[0]):
        logs = mid_step(s, k, k == 0)
        score = logs if score is None else score + logs

    for to in range(n_chan):
        start = pl.multiple_of((side * n_chan + to) * LANES, LANES)
        z = state[:16, pl.ds(start, LANES)]
        z_send[to] = jnp.where(
            lane < 32,
            pltpu.roll(z[:8], LANES - quad * 32, 1),
            pltpu.roll(z[8:], LANES + 32 - quad * 32, 1),
        )
    z_copies = []
    for d in range(1, n_chan):
        other = lax.rem(c + d, n_chan)
        copy = pltpu.make_async_remote_copy(
            src_ref=z_send.at[other],
            dst_ref=z_recv.at[c],
            send_sem=z_send_sem.at[d],
            recv_sem=z_recv_sem.at[d],
            device_id=device(r, other),
            device_id_type=MESH,
        )
        copy.start()
        z_copies.append(copy)
    z_recv[c] = z_send[c]

    squares = fold(state[:16, :] * state[:16, :])
    score = score - 0.5 * keep(squares, iota((16, 1), 0) < half)
    squeeze(s)
    score_top = None
    for k in range(p["shift_top"].shape[0]):
        logs = top_step(s, k)
        score_top = logs if score_top is None else score_top + logs
    top = s["top"]
    squares = fold(top[...] * top[...])
    total = jnp.sum(score, axis=0, keepdims=True) + jnp.sum(score_top, axis=0, keepdims=True)
    total = total - 0.5 * jnp.sum(squares, axis=0, keepdims=True)
    total = jnp.sum(total, axis=1, keepdims=True)
    lik_out[...] = jnp.broadcast_to((total + fixed) / (channels * cells), (8, LANES))
    turned = s["turned"]
    for v in range(4):
        turned[v * LANES : (v + 1) * LANES, :top_channels] = jnp.transpose(
            top[:, v * LANES : (v + 1) * LANES]
        )
    for v in range(4):
        start = v * LANES + quad * 32 + side
        top_out[0, v * 16 : (v + 1) * 16, :] = turned[pl.ds(start, 16, stride=2), :][
            :, :top_channels
        ]

    for d in range(1, n_chan):
        pltpu.make_async_remote_copy(
            src_ref=z_send.at[0],
            dst_ref=z_recv.at[lax.rem(c + n_chan - d, n_chan)],
            send_sem=z_send_sem.at[d],
            recv_sem=z_recv_sem.at[d],
            device_id=device(r, c),
            device_id_type=MESH,
        ).wait_recv()
    for img in range(n_chan):
        z = z_recv[img]
        mid_out[img, :8, :] = z[:, :width]
        mid_out[img, 8:, :] = z[:4, width : 2 * width]
    for copy in z_copies:
        copy.wait_send()
    for ref, sem in (
        (stage.at[pl.ds(0, n_rows - 1)], stage_send),
        (inbox.at[pl.ds(0, n_chan - 1)], piece_send),
    ):
        pltpu.make_async_remote_copy(
            src_ref=ref,
            dst_ref=ref,
            send_sem=sem,
            recv_sem=hello_sem.at[0],
            device_id=device(r, c),
            device_id_type=MESH,
        ).wait_send()


def deliver(mid, top, lik, mid_out, top_out, lik_out):
    for img in range(mid.shape[0]):
        mid_out[img, :, 0, :] = mid[img]
    top_out[...] = top[...]
    lik_out[...] = lik[0, :1]


def body(sizes, images, *params):
    n_rows, n_chan = sizes
    n_imgs, channels, own_rows, width = images.shape
    peers = n_rows * n_chan
    height = own_rows * peers
    params = parameters(params)
    hidden = params[6].shape[1]
    steps_mid, steps_top = params[0].shape[0], params[11].shape[0]
    top_channels = params[11].shape[1]
    half = channels // 2
    cells = height * width
    own = cells // 4 // n_rows
    operands = (images.reshape(n_imgs, channels, width),) + params
    vmem = pl.BlockSpec(memory_space=pltpu.VMEM)
    count = len(operands)
    work = work_scratch(steps_mid, steps_top, hidden, channels, top_channels, cells)
    mid, top, lik = pl.pallas_call(
        functools.partial(kernel, (n_rows, n_chan, height, width, count), list(work)),
        out_shape=(
            pltpu.VMEM((n_imgs, half, width), f32),
            pltpu.VMEM((1, own, top_channels), f32),
            pltpu.VMEM((8, LANES), f32),
        ),
        in_specs=[pl.BlockSpec(memory_space=pl.ANY)] * count,
        out_specs=(vmem, vmem, vmem),
        scratch_shapes=[pltpu.VMEM(x.shape, x.dtype) for x in operands]
        + list(work.values())
        + [
            pltpu.VMEM((n_chan, 8, LANES), bf16),
            pltpu.VMEM((n_rows, n_chan, 8, LANES), bf16),
            pltpu.VMEM((n_chan, n_rows, 8, LANES), bf16),
            pltpu.VMEM((n_chan, 8, LANES), f32),
            pltpu.VMEM((n_chan, 8, LANES), f32),
            pltpu.SemaphoreType.DMA((count,)),
            pltpu.SemaphoreType.DMA,
            pltpu.SemaphoreType.DMA,
            pltpu.SemaphoreType.DMA((n_rows,)),
            pltpu.SemaphoreType.DMA((n_chan,)),
            pltpu.SemaphoreType.DMA((n_chan,)),
            pltpu.SemaphoreType.DMA((n_chan,)),
            pltpu.SemaphoreType.DMA((n_chan,)),
        ],
        compiler_params=pltpu.CompilerParams(
            collective_id=0, has_side_effects=True, vmem_limit_bytes=56 * 1024 * 1024
        ),
        name="flow",
    )(*operands)
    latent_mid, top, lik = pl.pallas_call(
        deliver,
        out_shape=(
            jax.ShapeDtypeStruct((n_imgs, half, own_rows, width), f32),
            jax.ShapeDtypeStruct(top.shape, f32),
            jax.ShapeDtypeStruct((1,), f32),
        ),
        in_specs=[vmem, vmem, vmem],
        out_specs=(vmem, vmem, vmem),
        compiler_params=pltpu.CompilerParams(vmem_limit_bytes=4 * 1024 * 1024),
        name="deliver",
    )(mid, top, lik)
    latent_top = top.reshape(1, -1, width // 2, top_channels).transpose(0, 3, 1, 2)
    return latent_mid, latent_top, lik


def solution(mesh):
    sizes = (mesh.shape["rows"], mesh.shape["chan"])
    placed = (P("batch", None, ("rows", "chan"), None),) + (P(),) * 22
    return jax.shard_map(
        functools.partial(body, sizes),
        mesh=mesh,
        in_specs=placed,
        out_specs=(
            P("batch", None, ("rows", "chan"), None),
            P(("batch", "chan"), None, "rows", None),
            P(("batch", "chan")),
        ),
        check_vma=False,
    )
```

```python
import functools
import math

import jax
import jax.numpy as jnp
from jax import lax
from jax.experimental import pallas as pl
from jax.experimental.pallas import tpu as pltpu
from jax.sharding import PartitionSpec as P

MESH = pl.DeviceIdType.MESH
LANES = 128
CHUNK = 1024
FINE = lax.Precision.HIGHEST
log_two_pi = math.log(2.0 * math.pi)
f32 = jnp.float32
bf16 = jnp.bfloat16


def iota(shape, dim):
    return lax.broadcasted_iota(jnp.int32, shape, dim)


def dot_nt(a, b, precision=None):
    return lax.dot_general(
        a, b, (((1,), (1,)), ((), ())), preferred_element_type=f32, precision=precision
    )


def roll(x, amount):
    n = x.shape[1]
    amount = amount % n
    return x if amount == 0 else pltpu.roll(x, amount, 1)


def keep(x, ok):
    return jnp.where(ok, x, 0.0)


def mid_map(channels):
    i = iota((channels, channels), 0)
    j = iota((channels, channels), 1)
    source = jnp.where(i < 12, i, jnp.where(i < 16, i + 8, i - 4))
    return jnp.where(source == j, 1.0, 0.0)


def eye_map(channels):
    return jnp.where(iota((channels, channels), 0) == iota((channels, channels), 1), 1.0, 0.0)


def squeeze_map(channels):
    i = iota((channels, channels), 0)
    j = iota((channels, channels), 1)
    low = 4 * lax.rem(i, 8) + lax.div(i, 8)
    k = i - 32
    place = 2 * lax.div(k, 8) + 1 - lax.div(lax.rem(k + 64, 8), 4)
    high = 4 * (8 + lax.rem(k + 64, 4)) + place
    return jnp.where(jnp.where(i < 32, low, high) == j, 1.0, 0.0)


def split_two(x):
    high = x.astype(bf16).astype(f32)
    return high, x - high


def mixing(lower, upper, diag_row, gain_row, shift_row, out_map, in_map, exact):
    channels = lower.shape[0]
    i = iota((channels, channels), 0)
    j = iota((channels, channels), 1)
    eye = jnp.where(i == j, 1.0, 0.0)
    low = jnp.where(i > j, lower, 0.0) + eye
    upp = (jnp.where(i < j, upper, 0.0) + eye * jnp.exp(diag_row)) * jnp.exp(gain_row)
    rows = jnp.dot(out_map, low, precision=FINE, preferred_element_type=f32)
    mat = jnp.dot(rows, upp, precision=FINE, preferred_element_type=f32)
    bias = jnp.sum(mat * shift_row, axis=1, keepdims=True)
    if in_map is not None:
        mat = dot_nt(mat, in_map, FINE)
    high, rest = split_two(mat)
    parts = [high, rest] if exact else [high, high, rest]
    return jnp.concatenate(parts, axis=1).astype(bf16), bias


def mapped_column(row, mapping):
    return jnp.sum(mapping * row, axis=1, keepdims=True)


def prepare(p, s):
    steps_mid, channels = p["shift_mid"].shape
    steps_top, top_channels = p["shift_top"].shape
    hidden = p["w2_mid"].shape[1]
    half = channels // 2
    mapping = mid_map(channels)
    natural = eye_map(top_channels)
    for k in range(steps_mid):
        mat, bias = mixing(
            p["lower_mid"][k],
            p["upper_mid"][k],
            p["diag_mid"][k : k + 1, :],
            p["gain_mid"][k : k + 1, :],
            p["shift_mid"][k : k + 1, :],
            mapping,
            None if k == 0 else mapping,
            k == 0,
        )
        s["mix_mid"][k, :, : mat.shape[1]] = mat
        s["mix_bias_mid"][k] = jnp.broadcast_to(bias, (channels, LANES))
        s["b3_mid"][k] = jnp.broadcast_to(
            mapped_column(p["third_bias_mid"][k : k + 1, :], mapping), (channels, LANES)
        )
    for k in range(steps_top):
        mat, bias = mixing(
            p["lower_top"][k],
            p["upper_top"][k],
            p["diag_top"][k : k + 1, :],
            p["gain_top"][k : k + 1, :],
            p["shift_top"][k : k + 1, :],
            natural,
            squeeze_map(top_channels) if k == 0 else None,
            False,
        )
        s["mix_top"][k, :, : mat.shape[1]] = mat
        s["mix_bias_top"][k] = jnp.broadcast_to(bias, (top_channels, LANES))
        s["b3_top"][k] = jnp.broadcast_to(
            mapped_column(p["third_bias_top"][k : k + 1, :], natural), (top_channels, LANES)
        )
    for k in range(steps_mid):
        taps = []
        for tap in range(9):
            extra = [jnp.zeros((16 - half, hidden), f32)]
            if tap == 4:
                row = p["first_bias_mid"][k : k + 1, :].astype(f32)
                extra = [row, jnp.zeros((15 - half, hidden), f32)]
            taps.append(jnp.concatenate([p["w1_mid"][k, tap].astype(f32)] + extra, axis=0))
        s["w1t_mid"][k] = jnp.transpose(jnp.concatenate(taps, axis=0)).astype(bf16)
        s["w2t_mid"][k] = jnp.transpose(p["w2_mid"][k].astype(f32)).astype(bf16)
        s["b2_mid"][k] = jnp.transpose(
            jnp.broadcast_to(p["second_bias_mid"][k : k + 1, :], (LANES, hidden))
        )
        for tap in range(9):
            w = p["w3_mid"][k, tap * channels : (tap + 1) * channels, :].astype(f32)
            w = jnp.concatenate([w[:12], w[20:24], w[12:20]], axis=0)
            s["w3f_mid"][tap * channels : (tap + 1) * channels, :] = w
        s["w3p_mid"][k] = s["w3f_mid"][...].astype(bf16)
    for k in range(steps_top):
        row = p["first_bias_top"][k : k + 1, :].astype(f32)
        w = jnp.concatenate(
            [p["w1_top"][k].astype(f32), row, jnp.zeros((7, hidden), f32)], axis=0
        )
        s["w1t_top"][k] = jnp.transpose(w).astype(bf16)
        s["w2t_top"][k] = jnp.transpose(p["w2_top"][k].astype(f32)).astype(bf16)
        s["b2_top"][k] = jnp.transpose(
            jnp.broadcast_to(p["second_bias_top"][k : k + 1, :], (LANES, hidden))
        )


def wide(x, n):
    return jnp.concatenate([x] * (n // LANES), axis=1)


def lane_of(n):
    return lax.rem(iota((1, n), 1), LANES)


def edge_mid(x, dr):
    lane = iota((1, LANES), 1)
    if dr > 0:
        return keep(roll(x, -32), lane < 96)
    return keep(roll(x, 32), lane >= 32)


def edge_top(x, dr):
    lane = iota((1, LANES), 1)
    odd = lax.rem(lane, 2) == 1
    if dr > 0:
        return jnp.where(odd, keep(roll(x, -31), lane < 96), roll(x, -1))
    return jnp.where(odd, roll(x, 1), keep(roll(x, 31), lane >= 32))


def shift_col(x, dc, stride):
    n = x.shape[1]
    col = lax.rem(iota((1, n), 1), 32)
    if dc > 0:
        return keep(roll(x, -stride), col < 32 - stride)
    return keep(roll(x, stride), col >= stride)


def gather(y_ref, tap_rows, lo, hi, n, edge, stride):
    total = None
    for dc in (0, -1, 1):
        base = 4 + dc
        part = y_ref[base * tap_rows : (base + 1) * tap_rows, lo:hi]
        for dr in (-1, 1):
            tap = base + 3 * dr
            rows = slice(tap * tap_rows, (tap + 1) * tap_rows)
            if dr > 0 and hi == n:
                moved = [edge(y_ref[rows, :LANES], dr)]
                if hi - lo > LANES:
                    moved = [y_ref[rows, lo + LANES : hi]] + moved
                moved = jnp.concatenate(moved, axis=1) if len(moved) > 1 else moved[0]
            elif dr < 0 and lo == 0:
                moved = [edge(y_ref[rows, n - LANES : n], dr)]
                if hi - lo > LANES:
                    moved = moved + [y_ref[rows, : hi - LANES]]
                moved = jnp.concatenate(moved, axis=1) if len(moved) > 1 else moved[0]
            else:
                moved = y_ref[rows, lo + dr * LANES : hi + dr * LANES]
            part = part + moved
        if dc != 0:
            part = shift_col(part, dc, stride)
        total = part if total is None else total + part
    return total


def gated(g):
    e = jnp.exp(-jnp.abs(g))
    inv = 1.0 / (1.0 + e)
    gate = jnp.where(g >= 0, inv, e * inv)
    return gate, jnp.minimum(g, 0.0) - jnp.log(1.0 + e)


def fold(x):
    total = x[:, :LANES]
    for at in range(LANES, x.shape[1], LANES):
        total = total + x[:, at : at + LANES]
    return total


def mix(mat, bias, x, exact):
    n = x.shape[1]
    if exact:
        stack = [x, x]
    else:
        high, rest = split_two(x)
        stack = [high, rest, high]
    stack = jnp.concatenate(stack, axis=0).astype(bf16)
    return jnp.dot(mat, stack, preferred_element_type=f32) + wide(bias, n)


def product(first, second, third, bias, spread, y_ref, rows, lo):
    n = spread.shape[1]
    h = jnp.dot(first[...], spread, preferred_element_type=f32)
    h = jnp.maximum(h, 0.0).astype(bf16)
    h = jnp.dot(second[...], h, preferred_element_type=f32)
    h = jnp.maximum(h + wide(bias[...], n), 0.0).astype(bf16)
    y_ref[:rows, lo : lo + n] = jnp.dot(third[...], h, preferred_element_type=f32)


def mid_step(s, k, exact):
    state, u_ref, q_ref, y_ref = s["state"], s["u"], s["q"], s["y"]
    channels, n = state.shape
    block = 4 * LANES
    sub = iota((8, 1), 0)
    mat = s["mix_mid"][k, :, : (2 if exact else 3) * channels]
    for lo in range(0, n, block):
        u_ref[:, lo : lo + block] = mix(
            mat, s["mix_bias_mid"][k], state[:, lo : lo + block], exact
        )
    for lo in range(0, n, block):
        q = u_ref[:16, lo : lo + block]
        q = jnp.concatenate([q[:8], jnp.where(sub == 4, 1.0, q[8:])], axis=0)
        for dc in (-1, 0, 1):
            x = q if dc == 0 else shift_col(q, dc, 1)
            q_ref[dc + 1, :, LANES + lo : LANES + lo + block] = x.astype(bf16)
            if lo == 0:
                q_ref[dc + 1, :, LANES + n :] = edge_mid(x[:, :LANES], 1).astype(bf16)
            if lo + block == n:
                q_ref[dc + 1, :, :LANES] = edge_mid(x[:, block - LANES :], -1).astype(bf16)
    for lo in range(0, n, min(CHUNK, n)):
        taps = []
        for dr in (-1, 0, 1):
            at = lo + LANES * (1 + dr)
            for dc in (-1, 0, 1):
                taps.append(q_ref[dc + 1, :, at : at + min(CHUNK, n)])
        product(
            s["w1t_mid"].at[k],
            s["w2t_mid"].at[k],
            s["w3p_mid"].at[k],
            s["b2_mid"].at[k],
            jnp.concatenate(taps, axis=0),
            y_ref,
            9 * channels,
            lo,
        )
    score = None
    width = 2 * LANES
    for lo in range(0, n, width):
        out = gather(y_ref, channels, lo, lo + width, n, edge_mid, 1) + wide(s["b3_mid"][k], width)
        gate, logs = gated(out[:16] + 2.0)
        logs = fold(logs)
        score = logs if score is None else score + logs
        u = u_ref[:, lo : lo + width]
        state[:8, lo : lo + width] = u[:8]
        late = (u[8:16] + out[8:16]) * pltpu.roll(gate[8:16], 4, 0)
        state[8:16, lo : lo + width] = jnp.where(sub < 4, u[8:16], late)
        state[16:, lo : lo + width] = (u[16:] + out[16:]) * gate[:8]
    return keep(score, iota((16, 1), 0) < channels // 2)


def squeeze(s):
    state, top = s["state"], s["top"]
    odd = lax.rem(iota((1, LANES), 1), 2) == 1
    sub = iota((8, 1), 0)
    for v in range(4):
        tails = []
        for i in range(2):
            t = (2 * v + i) * LANES
            a = state[8:, t : t + LANES]
            t = t + 8 * LANES
            b = state[8:, t : t + LANES]
            even_col = jnp.where(odd, roll(b, 1), a)
            odd_col = jnp.where(odd, b, roll(a, -1))
            cols = slice(v * LANES, (v + 1) * LANES)
            top[16 * i : 16 * i + 8, cols] = even_col[8:]
            top[16 * i + 8 : 16 * i + 16, cols] = odd_col[8:]
            top[32 + 8 * i : 40 + 8 * i, cols] = jnp.where(
                sub < 4, pltpu.roll(odd_col[:8], 4, 0), even_col[:8]
            )


def top_step(s, k):
    state, u_ref, q_ref, y_ref = s["top"], s["u_top"], s["q_top"], s["y_top"]
    channels, n = state.shape
    half = channels // 2
    mat = s["mix_top"][k, :, : 3 * channels]
    u_ref[...] = mix(mat, s["mix_bias_top"][k], state[...], False)
    q = u_ref[:half, :]
    for dc in (-1, 0, 1):
        x = q if dc == 0 else shift_col(q, dc, 2)
        q_ref[dc + 1, :, LANES : LANES + n] = x
        q_ref[dc + 1, :, LANES + n :] = edge_top(x[:, :LANES], 1)
        q_ref[dc + 1, :, :LANES] = edge_top(x[:, n - LANES :], -1)
    ones = jnp.where(iota((8, min(CHUNK, n)), 0) == 0, 1.0, 0.0)
    for lo in range(0, n, min(CHUNK, n)):
        taps = []
        for dr in (-1, 0, 1):
            at = lo + LANES * (1 + dr)
            for dc in (-1, 0, 1):
                taps.append(q_ref[dc + 1, :, at : at + min(CHUNK, n)])
        product(
            s["w1t_top"].at[k],
            s["w2t_top"].at[k],
            s["w3_top"].at[k],
            s["b2_top"].at[k],
            jnp.concatenate(taps + [ones], axis=0).astype(bf16),
            y_ref,
            9 * channels,
            lo,
        )
    score = None
    width = LANES
    for lo in range(0, n, width):
        out = gather(y_ref, channels, lo, lo + width, n, edge_top, 2) + wide(s["b3_top"][k], width)
        gate, logs = gated(out[:half] + 2.0)
        score = logs if score is None else score + logs
        state[:half, lo : lo + width] = u_ref[:half, lo : lo + width]
        state[half:, lo : lo + width] = (u_ref[half:, lo : lo + width] + out[half:]) * gate
    return score


def work_scratch(steps_mid, steps_top, hidden, channels, top_channels, cells):
    n_top = cells // 4
    return {
        "mix_mid": pltpu.VMEM((steps_mid, channels, 3 * channels), bf16),
        "mix_bias_mid": pltpu.VMEM((steps_mid, channels, LANES), f32),
        "b3_mid": pltpu.VMEM((steps_mid, channels, LANES), f32),
        "mix_top": pltpu.VMEM((steps_top, top_channels, 3 * top_channels), bf16),
        "mix_bias_top": pltpu.VMEM((steps_top, top_channels, LANES), f32),
        "b3_top": pltpu.VMEM((steps_top, top_channels, LANES), f32),
        "w1t_mid": pltpu.VMEM((steps_mid, hidden, 144), bf16),
        "w2t_mid": pltpu.VMEM((steps_mid, hidden, hidden), bf16),
        "b2_mid": pltpu.VMEM((steps_mid, hidden, LANES), f32),
        "w3f_mid": pltpu.VMEM((9 * channels, hidden), f32),
        "w3p_mid": pltpu.VMEM((steps_mid, 9 * channels, hidden), bf16),
        "w1t_top": pltpu.VMEM((steps_top, hidden, 9 * top_channels // 2 + 8), bf16),
        "w2t_top": pltpu.VMEM((steps_top, hidden, hidden), bf16),
        "b2_top": pltpu.VMEM((steps_top, hidden, LANES), f32),
        "state": pltpu.VMEM((channels, cells), f32),
        "u": pltpu.VMEM((channels, cells), f32),
        "q": pltpu.VMEM((3, 16, cells + 2 * LANES), bf16),
        "y": pltpu.VMEM((9 * channels, cells), f32),
        "top": pltpu.VMEM((top_channels, n_top), f32),
        "u_top": pltpu.VMEM((top_channels, n_top), f32),
        "q_top": pltpu.VMEM((3, top_channels // 2, n_top + 2 * LANES), f32),
        "y_top": pltpu.VMEM((9 * top_channels, n_top), f32),
        "turned": pltpu.VMEM((n_top, LANES), f32),
    }


NAMES = (
    "shift_mid",
    "gain_mid",
    "lower_mid",
    "upper_mid",
    "diag_mid",
    "w1_mid",
    "first_bias_mid",
    "w2_mid",
    "second_bias_mid",
    "w3_mid",
    "third_bias_mid",
    "shift_top",
    "gain_top",
    "lower_top",
    "upper_top",
    "diag_top",
    "w1_top",
    "first_bias_top",
    "w2_top",
    "second_bias_top",
    "w3_top",
    "third_bias_top",
)


def parameters(params):
    (
        shift_mid, gain_mid, lower_mid, upper_mid, diag_mid, first_mid, first_bias_mid, second_mid,
        second_bias_mid, third_mid, third_bias_mid, shift_top, gain_top, lower_top, upper_top,
        diag_top, first_top, first_bias_top, second_top, second_bias_top, third_top, third_bias_top,
    ) = params
    steps_mid, hidden = first_bias_mid.shape
    steps_top = first_bias_top.shape[0]
    w1_top = first_top.reshape(steps_top, -1, hidden)
    w3_mid = third_mid.transpose(0, 1, 3, 2).reshape(steps_mid, -1, hidden)
    w3_top = third_top.transpose(0, 1, 3, 2).reshape(steps_top, -1, hidden)
    return (
        shift_mid, gain_mid, lower_mid, upper_mid, diag_mid, first_mid, first_bias_mid, second_mid,
        second_bias_mid, w3_mid, third_bias_mid, shift_top, gain_top, lower_top, upper_top,
        diag_top, w1_top, first_bias_top, second_top, second_bias_top, w3_top, third_bias_top,
    )


def kernel(dims, keys, *refs):
    n_rows, n_chan, height, width, count = dims
    sources, refs = refs[:count], refs[count:]
    (mid_out, top_out, lik_out), refs = refs[:3], refs[3:]
    held, refs = refs[:count], refs[count:]
    s, refs = dict(zip(keys, refs)), refs[len(keys) :]
    outbox, stage, inbox, z_send, z_recv, w_sem, refs = *refs[:6], refs[6:]
    stage_send, piece_send, stage_sem, hello_sem, piece_sem, z_send_sem, z_recv_sem = refs
    images = held[0]
    p = dict(zip(NAMES, held[1:]))
    s["w3_top"] = p["w3_top"]
    b = lax.axis_index("batch")
    r = lax.axis_index("rows")
    c = lax.axis_index("chan")
    quad = lax.div(r, 2)
    side = lax.rem(r, 2)

    def device(row, chan):
        return {"batch": b, "rows": row, "chan": chan}

    chans = []
    for q in range(n_chan):
        y = q // 2
        chans.append(2 * (y + y // 2 * (5 - 2 * y)) + 1 - q % 2)
    y = lax.div(c, 2)
    spot = 2 * (y + lax.div(y, 2) * (5 - 2 * y)) + 1 - lax.rem(c, 2)

    first = pltpu.make_async_copy(sources[0], held[0], w_sem.at[0])
    first.start()
    barrier = pltpu.get_barrier_semaphore()
    for row in range(1, n_rows):

        @pl.when(row > r)
        def _():
            pl.semaphore_signal(barrier, inc=1, device_id=device(row, c), device_id_type=MESH)

    for q in range(1, n_chan):

        @pl.when(q > spot)
        def _():
            pl.semaphore_signal(
                barrier, inc=1, device_id=device(r, chans[q]), device_id_type=MESH
            )

    first.wait()
    for dest in range(n_chan):
        x = images[dest]
        x = jnp.concatenate([x[:8], x[8:16], x[16:], jnp.zeros((8, width), f32)], axis=1)
        outbox[dest] = pltpu.roll(x, quad * 32, 1).astype(bf16)

    @pl.when(r + spot > 0)
    def _():
        pl.semaphore_wait(barrier, r + spot)

    def send_row(row):
        pltpu.make_async_remote_copy(
            src_ref=outbox,
            dst_ref=stage.at[r],
            send_sem=stage_send,
            recv_sem=stage_sem.at[r],
            device_id=device(row, c),
            device_id_type=MESH,
        ).start()

    def send_hello(q):
        pltpu.make_async_remote_copy(
            src_ref=outbox.at[chans[q]],
            dst_ref=inbox.at[c, r],
            send_sem=piece_send,
            recv_sem=hello_sem.at[c],
            device_id=device(r, chans[q]),
            device_id_type=MESH,
        ).start()

    def send_piece(row, q):
        pltpu.make_async_remote_copy(
            src_ref=stage.at[row, chans[q]],
            dst_ref=inbox.at[c, row],
            send_sem=piece_send,
            recv_sem=piece_sem.at[c],
            device_id=device(r, chans[q]),
            device_id_type=MESH,
        ).start()

    def await_copy(ref, sem):
        pltpu.make_async_remote_copy(
            src_ref=ref,
            dst_ref=ref,
            send_sem=stage_send,
            recv_sem=sem,
            device_id=device(r, c),
            device_id_type=MESH,
        ).wait_recv()

    for row in range(n_rows - 1):
        pl.when(row < r)(functools.partial(send_row, row))
    for q in range(n_chan - 1):
        pl.when(q < spot)(functools.partial(send_hello, q))
    copies = []
    for at in range(1, count):
        copy = pltpu.make_async_copy(sources[at], held[at], w_sem.at[at])
        copy.start()
        copies.append(copy)
    stage[r] = outbox[...]
    for copy in copies:
        copy.wait()
    prepare(p, s)
    channels = p["shift_mid"].shape[1]
    top_channels = p["shift_top"].shape[1]
    half = channels // 2
    cells = height * width
    fixed = cells * (jnp.sum(p["gain_mid"][...]) + jnp.sum(p["diag_mid"][...]))
    fixed = fixed + cells // 4 * (jnp.sum(p["gain_top"][...]) + jnp.sum(p["diag_top"][...]))
    fixed = fixed - 0.5 * log_two_pi * channels * cells

    for row in range(1, n_rows):

        @pl.when(row > r)
        def _():
            await_copy(stage.at[row], stage_sem.at[row])
            send_row(row)
            for q in range(n_chan - 1):
                pl.when(q < spot)(functools.partial(send_piece, row, q))

    for q in range(1, n_chan):

        @pl.when(q > spot)
        def _():
            await_copy(inbox.at[chans[q], 0], hello_sem.at[chans[q]])
            send_hello(q)
            for row in range(1, n_rows):
                pl.when(row > r)(functools.partial(send_piece, row, q))

    for row in range(n_rows - 1):

        @pl.when(row < r)
        def _():
            await_copy(stage.at[row], stage_sem.at[row])
            for q in range(n_chan):
                pl.when(q != spot)(functools.partial(send_piece, row, q))

    for row in range(n_rows):
        inbox[c, row] = stage[row, c]
    for q in range(n_chan):

        @pl.when(q < spot)
        def _():
            await_copy(inbox.at[chans[q], 0], hello_sem.at[chans[q]])

        @pl.when(q != spot)
        def _():
            await_copy(inbox.at[chans[q], pl.ds(0, n_rows - 1)], piece_sem.at[chans[q]])

    state = s["state"]
    lane = iota((1, LANES), 1)
    for t in range(height // 4):
        letters = [inbox[t % 8, 2 * k + t // 8].astype(f32) for k in range(4)]
        for slab in range(3):
            x = letters[(3 - slab) % 4]
            for k in range(3):
                x = jnp.where(lax.div(lane, 32) == k, letters[(k - slab) % 4], x)
            state[8 * slab : 8 * slab + 8, t * LANES : (t + 1) * LANES] = roll(x, -32 * slab)

    score = None
    for k in range(p["shift_mid"].shape[0]):
        logs = mid_step(s, k, k == 0)
        score = logs if score is None else score + logs

    for to in range(n_chan):
        start = pl.multiple_of((side * n_chan + to) * LANES, LANES)
        z = state[:16, pl.ds(start, LANES)]
        z_send[to] = jnp.where(
            lane < 32,
            pltpu.roll(z[:8], LANES - quad * 32, 1),
            pltpu.roll(z[8:], LANES + 32 - quad * 32, 1),
        )
    z_copies = []
    for d in range(1, n_chan):
        other = lax.rem(c + d, n_chan)
        copy = pltpu.make_async_remote_copy(
            src_ref=z_send.at[other],
            dst_ref=z_recv.at[c],
            send_sem=z_send_sem.at[d],
            recv_sem=z_recv_sem.at[d],
            device_id=device(r, other),
            device_id_type=MESH,
        )
        copy.start()
        z_copies.append(copy)
    z_recv[c] = z_send[c]

    squares = fold(state[:16, :] * state[:16, :])
    score = score - 0.5 * keep(squares, iota((16, 1), 0) < half)
    squeeze(s)
    score_top = None
    for k in range(p["shift_top"].shape[0]):
        logs = top_step(s, k)
        score_top = logs if score_top is None else score_top + logs
    top = s["top"]
    squares = fold(top[...] * top[...])
    total = jnp.sum(score, axis=0, keepdims=True) + jnp.sum(score_top, axis=0, keepdims=True)
    total = total - 0.5 * jnp.sum(squares, axis=0, keepdims=True)
    total = jnp.sum(total, axis=1, keepdims=True)
    lik_out[...] = jnp.broadcast_to((total + fixed) / (channels * cells), (8, LANES))
    turned = s["turned"]
    for v in range(4):
        turned[v * LANES : (v + 1) * LANES, :top_channels] = jnp.transpose(
            top[:, v * LANES : (v + 1) * LANES]
        )
    for v in range(4):
        start = v * LANES + quad * 32 + side
        top_out[0, v * 16 : (v + 1) * 16, :] = turned[pl.ds(start, 16, stride=2), :][
            :, :top_channels
        ]

    for d in range(1, n_chan):
        pltpu.make_async_remote_copy(
            src_ref=z_send.at[0],
            dst_ref=z_recv.at[lax.rem(c + n_chan - d, n_chan)],
            send_sem=z_send_sem.at[d],
            recv_sem=z_recv_sem.at[d],
            device_id=device(r, c),
            device_id_type=MESH,
        ).wait_recv()
    for img in range(n_chan):
        z = z_recv[img]
        mid_out[img, :8, :] = z[:, :width]
        mid_out[img, 8:, :] = z[:4, width : 2 * width]
    for copy in z_copies:
        copy.wait_send()
    for ref, sem in (
        (stage.at[pl.ds(0, n_rows - 1)], stage_send),
        (inbox.at[pl.ds(0, n_chan - 1)], piece_send),
    ):
        pltpu.make_async_remote_copy(
            src_ref=ref,
            dst_ref=ref,
            send_sem=sem,
            recv_sem=hello_sem.at[0],
            device_id=device(r, c),
            device_id_type=MESH,
        ).wait_send()


def deliver(mid, top, lik, mid_out, top_out, lik_out):
    for img in range(mid.shape[0]):
        mid_out[img, :, 0, :] = mid[img]
    top_out[...] = top[...]
    lik_out[...] = lik[0, :1]


def body(sizes, images, *params):
    n_rows, n_chan = sizes
    n_imgs, channels, own_rows, width = images.shape
    peers = n_rows * n_chan
    height = own_rows * peers
    params = parameters(params)
    hidden = params[6].shape[1]
    steps_mid, steps_top = params[0].shape[0], params[11].shape[0]
    top_channels = params[11].shape[1]
    half = channels // 2
    cells = height * width
    own = cells // 4 // n_rows
    operands = (images.reshape(n_imgs, channels, width),) + params
    vmem = pl.BlockSpec(memory_space=pltpu.VMEM)
    count = len(operands)
    work = work_scratch(steps_mid, steps_top, hidden, channels, top_channels, cells)
    mid, top, lik = pl.pallas_call(
        functools.partial(kernel, (n_rows, n_chan, height, width, count), list(work)),
        out_shape=(
            pltpu.VMEM((n_imgs, half, width), f32),
            pltpu.VMEM((1, own, top_channels), f32),
            pltpu.VMEM((8, LANES), f32),
        ),
        in_specs=[pl.BlockSpec(memory_space=pl.ANY)] * count,
        out_specs=(vmem, vmem, vmem),
        scratch_shapes=[pltpu.VMEM(x.shape, x.dtype) for x in operands]
        + list(work.values())
        + [
            pltpu.VMEM((n_chan, 8, LANES), bf16),
            pltpu.VMEM((n_rows, n_chan, 8, LANES), bf16),
            pltpu.VMEM((n_chan, n_rows, 8, LANES), bf16),
            pltpu.VMEM((n_chan, 8, LANES), f32),
            pltpu.VMEM((n_chan, 8, LANES), f32),
            pltpu.SemaphoreType.DMA((count,)),
            pltpu.SemaphoreType.DMA,
            pltpu.SemaphoreType.DMA,
            pltpu.SemaphoreType.DMA((n_rows,)),
            pltpu.SemaphoreType.DMA((n_chan,)),
            pltpu.SemaphoreType.DMA((n_chan,)),
            pltpu.SemaphoreType.DMA((n_chan,)),
            pltpu.SemaphoreType.DMA((n_chan,)),
        ],
        compiler_params=pltpu.CompilerParams(
            collective_id=0, has_side_effects=True, vmem_limit_bytes=56 * 1024 * 1024
        ),
        name="flow",
    )(*operands)
    latent_mid, top, lik = pl.pallas_call(
        deliver,
        out_shape=(
            jax.ShapeDtypeStruct((n_imgs, half, own_rows, width), f32),
            jax.ShapeDtypeStruct(top.shape, f32),
            jax.ShapeDtypeStruct((1,), f32),
        ),
        in_specs=[vmem, vmem, vmem],
        out_specs=(vmem, vmem, vmem),
        compiler_params=pltpu.CompilerParams(vmem_limit_bytes=4 * 1024 * 1024),
        name="deliver",
    )(mid, top, lik)
    latent_top = top.reshape(1, -1, width // 2, top_channels).transpose(0, 3, 1, 2)
    return latent_mid, latent_top, lik


def solution(mesh):
    sizes = (mesh.shape["rows"], mesh.shape["chan"])
    placed = (P("batch", None, ("rows", "chan"), None),) + (P(),) * 22
    return jax.shard_map(
        functools.partial(body, sizes),
        mesh=mesh,
        in_specs=placed,
        out_specs=(
            P("batch", None, ("rows", "chan"), None),
            P(("batch", "chan"), None, "rows", None),
            P(("batch", "chan")),
        ),
        check_vma=False,
    )
```

```python
import functools
import math

import jax
import jax.numpy as jnp
from jax import lax
from jax.experimental import pallas as pl
from jax.experimental.pallas import tpu as pltpu
from jax.sharding import PartitionSpec as P

MESH = pl.DeviceIdType.MESH
LANES = 128
CHUNK = 1024
FINE = lax.Precision.HIGHEST
log_two_pi = math.log(2.0 * math.pi)
f32 = jnp.float32
bf16 = jnp.bfloat16


def iota(shape, dim):
    return lax.broadcasted_iota(jnp.int32, shape, dim)


def dot_nt(a, b, precision=None):
    return lax.dot_general(
        a, b, (((1,), (1,)), ((), ())), preferred_element_type=f32, precision=precision
    )


def roll(x, amount):
    n = x.shape[1]
    amount = amount % n
    return x if amount == 0 else pltpu.roll(x, amount, 1)


def keep(x, ok):
    return jnp.where(ok, x, 0.0)


def mid_map(channels):
    i = iota((channels, channels), 0)
    j = iota((channels, channels), 1)
    source = jnp.where(i < 12, i, jnp.where(i < 16, i + 8, i - 4))
    return jnp.where(source == j, 1.0, 0.0)


def eye_map(channels):
    return jnp.where(iota((channels, channels), 0) == iota((channels, channels), 1), 1.0, 0.0)


def squeeze_map(channels):
    i = iota((channels, channels), 0)
    j = iota((channels, channels), 1)
    low = 4 * lax.rem(i, 8) + lax.div(i, 8)
    k = i - 32
    place = 2 * lax.div(k, 8) + 1 - lax.div(lax.rem(k + 64, 8), 4)
    high = 4 * (8 + lax.rem(k + 64, 4)) + place
    return jnp.where(jnp.where(i < 32, low, high) == j, 1.0, 0.0)


def split_two(x):
    high = x.astype(bf16).astype(f32)
    return high, x - high


def mixing(lower, upper, diag_row, gain_row, shift_row, out_map, in_map, exact):
    channels = lower.shape[0]
    i = iota((channels, channels), 0)
    j = iota((channels, channels), 1)
    eye = jnp.where(i == j, 1.0, 0.0)
    low = jnp.where(i > j, lower, 0.0) + eye
    upp = (jnp.where(i < j, upper, 0.0) + eye * jnp.exp(diag_row)) * jnp.exp(gain_row)
    rows = jnp.dot(out_map, low, precision=FINE, preferred_element_type=f32)
    mat = jnp.dot(rows, upp, precision=FINE, preferred_element_type=f32)
    bias = jnp.sum(mat * shift_row, axis=1, keepdims=True)
    if in_map is not None:
        mat = dot_nt(mat, in_map, FINE)
    high, rest = split_two(mat)
    parts = [high, rest] if exact else [high, high, rest]
    return jnp.concatenate(parts, axis=1).astype(bf16), bias


def mapped_column(row, mapping):
    return jnp.sum(mapping * row, axis=1, keepdims=True)


def prepare(p, s):
    steps_mid, channels = p["shift_mid"].shape
    steps_top, top_channels = p["shift_top"].shape
    hidden = p["w2_mid"].shape[1]
    half = channels // 2
    mapping = mid_map(channels)
    natural = eye_map(top_channels)
    for name in ("u", "y"):
        shape = s[name].shape
        for at in (0, shape[2] - LANES):
            s[name][:, :, at : at + LANES] = jnp.zeros(shape[:2] + (LANES,), f32)
    for k in range(steps_mid):
        mat, bias = mixing(
            p["lower_mid"][k],
            p["upper_mid"][k],
            p["diag_mid"][k : k + 1, :],
            p["gain_mid"][k : k + 1, :],
            p["shift_mid"][k : k + 1, :],
            mapping,
            None if k == 0 else mapping,
            k == 0,
        )
        s["mix_mid"][k, :, : mat.shape[1]] = mat
        s["mix_bias_mid"][k] = jnp.broadcast_to(bias, (channels, LANES))
        s["b3_mid"][k] = jnp.broadcast_to(
            mapped_column(p["third_bias_mid"][k : k + 1, :], mapping), (channels, LANES)
        )
    for k in range(steps_top):
        mat, bias = mixing(
            p["lower_top"][k],
            p["upper_top"][k],
            p["diag_top"][k : k + 1, :],
            p["gain_top"][k : k + 1, :],
            p["shift_top"][k : k + 1, :],
            natural,
            squeeze_map(top_channels) if k == 0 else None,
            False,
        )
        s["mix_top"][k, :, : mat.shape[1]] = mat
        s["mix_bias_top"][k] = jnp.broadcast_to(bias, (top_channels, LANES))
        s["b3_top"][k] = jnp.broadcast_to(
            mapped_column(p["third_bias_top"][k : k + 1, :], natural), (top_channels, LANES)
        )
    for k in range(steps_mid):
        taps = []
        for tap in range(9):
            extra = [jnp.zeros((16 - half, hidden), f32)]
            if tap == 4:
                row = p["first_bias_mid"][k : k + 1, :].astype(f32)
                extra = [row, jnp.zeros((15 - half, hidden), f32)]
            taps.append(jnp.concatenate([p["w1_mid"][k, tap].astype(f32)] + extra, axis=0))
        s["w1t_mid"][k] = jnp.transpose(jnp.concatenate(taps, axis=0)).astype(bf16)
        s["w2t_mid"][k] = jnp.transpose(p["w2_mid"][k].astype(f32)).astype(bf16)
        s["b2_mid"][k] = jnp.transpose(
            jnp.broadcast_to(p["second_bias_mid"][k : k + 1, :], (LANES, hidden))
        )
        for tap in range(9):
            w = p["w3_mid"][k, tap * channels : (tap + 1) * channels, :].astype(f32)
            w = jnp.concatenate([w[:12], w[20:24], w[12:20]], axis=0)
            s["w3f_mid"][tap * channels : (tap + 1) * channels, :] = w
        s["w3p_mid"][k] = s["w3f_mid"][...].astype(bf16)
    for k in range(steps_top):
        row = p["first_bias_top"][k : k + 1, :].astype(f32)
        w = jnp.concatenate(
            [p["w1_top"][k].astype(f32), row, jnp.zeros((7, hidden), f32)], axis=0
        )
        s["w1t_top"][k] = jnp.transpose(w).astype(bf16)
        s["w2t_top"][k] = jnp.transpose(p["w2_top"][k].astype(f32)).astype(bf16)
        s["b2_top"][k] = jnp.transpose(
            jnp.broadcast_to(p["second_bias_top"][k : k + 1, :], (LANES, hidden))
        )


def wide(x, n):
    return jnp.concatenate([x] * (n // LANES), axis=1)


def lane_of(n):
    return lax.rem(iota((1, n), 1), LANES)


def edge_top(x, dr):
    lane = iota((1, LANES), 1)
    odd = lax.rem(lane, 2) == 1
    if dr > 0:
        return jnp.where(odd, keep(roll(x, -31), lane < 96), roll(x, -1))
    return jnp.where(odd, roll(x, 1), keep(roll(x, 31), lane >= 32))


def shift_col(x, dc, stride):
    n = x.shape[1]
    col = lax.rem(iota((1, n), 1), 32)
    if dc > 0:
        return keep(roll(x, -stride), col < 32 - stride)
    return keep(roll(x, stride), col >= stride)


def gather(y_ref, tap_rows, lo, hi, n, edge, stride):
    total = None
    for dc in (0, -1, 1):
        base = 4 + dc
        part = y_ref[base * tap_rows : (base + 1) * tap_rows, lo:hi]
        for dr in (-1, 1):
            tap = base + 3 * dr
            rows = slice(tap * tap_rows, (tap + 1) * tap_rows)
            if dr > 0 and hi == n:
                moved = [edge(y_ref[rows, :LANES], dr)]
                if hi - lo > LANES:
                    moved = [y_ref[rows, lo + LANES : hi]] + moved
                moved = jnp.concatenate(moved, axis=1) if len(moved) > 1 else moved[0]
            elif dr < 0 and lo == 0:
                moved = [edge(y_ref[rows, n - LANES : n], dr)]
                if hi - lo > LANES:
                    moved = moved + [y_ref[rows, : hi - LANES]]
                moved = jnp.concatenate(moved, axis=1) if len(moved) > 1 else moved[0]
            else:
                moved = y_ref[rows, lo + dr * LANES : hi + dr * LANES]
            part = part + moved
        if dc != 0:
            part = shift_col(part, dc, stride)
        total = part if total is None else total + part
    return total


def gated(g):
    e = jnp.exp(-jnp.abs(g))
    inv = 1.0 / (1.0 + e)
    gate = jnp.where(g >= 0, inv, e * inv)
    return gate, jnp.minimum(g, 0.0) - jnp.log(1.0 + e)


def fold(x):
    total = x[:, :LANES]
    for at in range(LANES, x.shape[1], LANES):
        total = total + x[:, at : at + LANES]
    return total


def mix(mat, bias, x, exact):
    n = x.shape[1]
    if exact:
        stack = [x, x]
    else:
        high, rest = split_two(x)
        stack = [high, rest, high]
    stack = jnp.concatenate(stack, axis=0).astype(bf16)
    return jnp.dot(mat, stack, preferred_element_type=f32) + wide(bias, n)


def product(first, second, third, bias, spread, y_ref, rows, lo):
    n = spread.shape[1]
    h = jnp.dot(first[...], spread, preferred_element_type=f32)
    h = jnp.maximum(h, 0.0).astype(bf16)
    h = jnp.dot(second[...], h, preferred_element_type=f32)
    h = jnp.maximum(h + wide(bias[...], n), 0.0).astype(bf16)
    y_ref[:rows, lo : lo + n] = jnp.dot(third[...], h, preferred_element_type=f32)


def row_sum(y_ref, k, tap_rows, lo, hi):
    total = None
    n = hi - lo
    for dc in (0, -1, 1):
        base = 4 + dc
        rows = slice(base * tap_rows, (base + 1) * tap_rows)
        part = y_ref[k, rows, LANES + lo : LANES + hi]
        rows = slice((base + 3) * tap_rows, (base + 4) * tap_rows)
        part = part + roll(y_ref[k, rows, LANES + lo : 2 * LANES + hi], -32)[:, :n]
        rows = slice((base - 3) * tap_rows, (base - 2) * tap_rows)
        part = part + roll(y_ref[k, rows, lo : LANES + hi], 32)[:, LANES:]
        if dc != 0:
            part = shift_col(part, dc, 1)
        total = part if total is None else total + part
    return total


def mid_step(s, k, exact, fresh, spread, done):
    state, u_ref, q_ref, y_ref = s["state"], s["u"], s["q"], s["y"]
    channels = u_ref.shape[1]
    sub = iota((8, 1), 0)
    mat = s["mix_mid"][k, :, : (2 if exact else 3) * channels]
    lo, hi = fresh[0] * LANES, fresh[1] * LANES
    u_ref[k, :, LANES + lo : LANES + hi] = mix(
        mat, s["mix_bias_mid"][k], state[k, :, lo:hi], exact
    )
    for lo in range(spread[0] * LANES, spread[1] * LANES, 2 * LANES):
        hi = lo + 2 * LANES
        rows = [
            roll(u_ref[k, :16, lo : LANES + hi], 32)[:, LANES:],
            u_ref[k, :16, LANES + lo : LANES + hi],
            roll(u_ref[k, :16, LANES + lo : 2 * LANES + hi], -32)[:, : hi - lo],
        ]
        for dr in range(3):
            for dc in range(3):
                x = rows[dr]
                if dr == 1 and dc == 1:
                    x = jnp.concatenate([x[:8], jnp.where(sub == 4, 1.0, x[8:])], axis=0)
                elif dc != 1:
                    x = shift_col(x, dc - 1, 1)
                tap = 3 * dr + dc
                q_ref[16 * tap : 16 * tap + 16, lo:hi] = x.astype(bf16)
    lo, hi = spread[0] * LANES, spread[1] * LANES
    product(
        s["w1t_mid"].at[k],
        s["w2t_mid"].at[k],
        s["w3p_mid"].at[k],
        s["b2_mid"].at[k],
        q_ref[:, lo:hi],
        y_ref.at[k],
        9 * channels,
        LANES + lo,
    )
    score = None
    for tile in range(done[0], done[1]):
        lo, hi = tile * LANES, (tile + 1) * LANES
        out = row_sum(y_ref, k, channels, lo, hi) + s["b3_mid"][k]
        gate, logs = gated(out[:16] + 2.0)
        score = logs if score is None else score + logs
        u = u_ref[k, :, LANES + lo : LANES + hi]
        state[k + 1, :8, lo:hi] = u[:8]
        late = (u[8:16] + out[8:16]) * pltpu.roll(gate[8:16], 4, 0)
        state[k + 1, 8:16, lo:hi] = jnp.where(sub < 4, u[8:16], late)
        state[k + 1, 16:, lo:hi] = (u[16:] + out[16:]) * gate[:8]
    return keep(score, iota((16, 1), 0) < channels // 2)


def squeeze(state, top):
    lane = iota((1, LANES), 1)
    odd = lax.rem(lane, 2) == 1
    block = lax.div(lane, 32)
    sub = iota((8, 1), 0)
    for v in range(4):
        for i in range(2):
            both = []
            for j in range(2):
                x = None
                for b in range(4):
                    tile = (4 * b + v // 2) * LANES
                    shift = 32 * (b - 2 * (v % 2) - i) - j
                    near = roll(state[8:, tile : tile + LANES], shift)
                    tile = tile + 2 * LANES
                    far = roll(state[8:, tile : tile + LANES], shift + 1)
                    near = jnp.where(odd, far, near)
                    x = near if x is None else jnp.where(block == b, near, x)
                both.append(x)
            cols = slice(v * LANES, (v + 1) * LANES)
            top[16 * i : 16 * i + 8, cols] = both[0][8:]
            top[16 * i + 8 : 16 * i + 16, cols] = both[1][8:]
            top[32 + 8 * i : 40 + 8 * i, cols] = jnp.where(
                sub < 4, pltpu.roll(both[1][:8], 4, 0), both[0][:8]
            )


def top_step(s, k):
    state, u_ref, q_ref, y_ref = s["top"], s["u_top"], s["q_top"], s["y_top"]
    channels, n = state.shape
    half = channels // 2
    mat = s["mix_top"][k, :, : 3 * channels]
    u_ref[...] = mix(mat, s["mix_bias_top"][k], state[...], False)
    q = u_ref[:half, :]
    for dc in (-1, 0, 1):
        x = q if dc == 0 else shift_col(q, dc, 2)
        q_ref[dc + 1, :, LANES : LANES + n] = x
        q_ref[dc + 1, :, LANES + n :] = edge_top(x[:, :LANES], 1)
        q_ref[dc + 1, :, :LANES] = edge_top(x[:, n - LANES :], -1)
    ones = jnp.where(iota((8, min(CHUNK, n)), 0) == 0, 1.0, 0.0)
    for lo in range(0, n, min(CHUNK, n)):
        taps = []
        for dr in (-1, 0, 1):
            at = lo + LANES * (1 + dr)
            for dc in (-1, 0, 1):
                taps.append(q_ref[dc + 1, :, at : at + min(CHUNK, n)])
        product(
            s["w1t_top"].at[k],
            s["w2t_top"].at[k],
            s["w3_top"].at[k],
            s["b2_top"].at[k],
            jnp.concatenate(taps + [ones], axis=0).astype(bf16),
            y_ref,
            9 * channels,
            lo,
        )
    score = None
    width = LANES
    for lo in range(0, n, width):
        out = gather(y_ref, channels, lo, lo + width, n, edge_top, 2) + wide(s["b3_top"][k], width)
        gate, logs = gated(out[:half] + 2.0)
        score = logs if score is None else score + logs
        state[:half, lo : lo + width] = u_ref[:half, lo : lo + width]
        state[half:, lo : lo + width] = (u_ref[half:, lo : lo + width] + out[half:]) * gate
    return score


def work_scratch(steps_mid, steps_top, hidden, channels, top_channels, cells):
    n_top = cells // 4
    return {
        "mix_mid": pltpu.VMEM((steps_mid, channels, 3 * channels), bf16),
        "mix_bias_mid": pltpu.VMEM((steps_mid, channels, LANES), f32),
        "b3_mid": pltpu.VMEM((steps_mid, channels, LANES), f32),
        "mix_top": pltpu.VMEM((steps_top, top_channels, 3 * top_channels), bf16),
        "mix_bias_top": pltpu.VMEM((steps_top, top_channels, LANES), f32),
        "b3_top": pltpu.VMEM((steps_top, top_channels, LANES), f32),
        "w1t_mid": pltpu.VMEM((steps_mid, hidden, 144), bf16),
        "w2t_mid": pltpu.VMEM((steps_mid, hidden, hidden), bf16),
        "b2_mid": pltpu.VMEM((steps_mid, hidden, LANES), f32),
        "w3f_mid": pltpu.VMEM((9 * channels, hidden), f32),
        "w3p_mid": pltpu.VMEM((steps_mid, 9 * channels, hidden), bf16),
        "w1t_top": pltpu.VMEM((steps_top, hidden, 9 * top_channels // 2 + 8), bf16),
        "w2t_top": pltpu.VMEM((steps_top, hidden, hidden), bf16),
        "b2_top": pltpu.VMEM((steps_top, hidden, LANES), f32),
        "state": pltpu.VMEM((steps_mid + 1, channels, cells), f32),
        "u": pltpu.VMEM((steps_mid, channels, cells + 2 * LANES), f32),
        "q": pltpu.VMEM((144, cells), bf16),
        "y": pltpu.VMEM((steps_mid, 9 * channels, cells + 2 * LANES), f32),
        "top": pltpu.VMEM((top_channels, n_top), f32),
        "u_top": pltpu.VMEM((top_channels, n_top), f32),
        "q_top": pltpu.VMEM((3, top_channels // 2, n_top + 2 * LANES), f32),
        "y_top": pltpu.VMEM((9 * top_channels, n_top), f32),
        "turned": pltpu.VMEM((n_top, LANES), f32),
    }


NAMES = (
    "shift_mid",
    "gain_mid",
    "lower_mid",
    "upper_mid",
    "diag_mid",
    "w1_mid",
    "first_bias_mid",
    "w2_mid",
    "second_bias_mid",
    "w3_mid",
    "third_bias_mid",
    "shift_top",
    "gain_top",
    "lower_top",
    "upper_top",
    "diag_top",
    "w1_top",
    "first_bias_top",
    "w2_top",
    "second_bias_top",
    "w3_top",
    "third_bias_top",
)


def parameters(params):
    (
        shift_mid, gain_mid, lower_mid, upper_mid, diag_mid, first_mid, first_bias_mid, second_mid,
        second_bias_mid, third_mid, third_bias_mid, shift_top, gain_top, lower_top, upper_top,
        diag_top, first_top, first_bias_top, second_top, second_bias_top, third_top, third_bias_top,
    ) = params
    steps_mid, hidden = first_bias_mid.shape
    steps_top = first_bias_top.shape[0]
    w1_top = first_top.reshape(steps_top, -1, hidden)
    w3_mid = third_mid.transpose(0, 1, 3, 2).reshape(steps_mid, -1, hidden)
    w3_top = third_top.transpose(0, 1, 3, 2).reshape(steps_top, -1, hidden)
    return (
        shift_mid, gain_mid, lower_mid, upper_mid, diag_mid, first_mid, first_bias_mid, second_mid,
        second_bias_mid, w3_mid, third_bias_mid, shift_top, gain_top, lower_top, upper_top,
        diag_top, w1_top, first_bias_top, second_top, second_bias_top, w3_top, third_bias_top,
    )


def kernel(dims, keys, *refs):
    n_rows, n_chan, height, width, count = dims
    sources, refs = refs[:count], refs[count:]
    (mid_out, top_out, lik_out), refs = refs[:3], refs[3:]
    held, refs = refs[:count], refs[count:]
    s, refs = dict(zip(keys, refs)), refs[len(keys) :]
    outbox, stage, inbox, z_send, z_recv, w_sem, refs = *refs[:6], refs[6:]
    stage_send, piece_send, stage_sem, hello_sem, piece_sem, z_send_sem, z_recv_sem = refs
    images = held[0]
    p = dict(zip(NAMES, held[1:]))
    s["w3_top"] = p["w3_top"]
    b = lax.axis_index("batch")
    r = lax.axis_index("rows")
    c = lax.axis_index("chan")
    quad = lax.div(r, 2)
    side = lax.rem(r, 2)

    def device(row, chan):
        return {"batch": b, "rows": row, "chan": chan}

    chans = []
    for q in range(n_chan):
        y = q // 2
        chans.append(2 * (y + y // 2 * (5 - 2 * y)) + 1 - q % 2)
    y = lax.div(c, 2)
    spot = 2 * (y + lax.div(y, 2) * (5 - 2 * y)) + 1 - lax.rem(c, 2)

    first = pltpu.make_async_copy(sources[0], held[0], w_sem.at[0])
    first.start()
    barrier = pltpu.get_barrier_semaphore()
    for row in range(1, n_rows):

        @pl.when(row > r)
        def _():
            pl.semaphore_signal(barrier, inc=1, device_id=device(row, c), device_id_type=MESH)

    for q in range(1, n_chan):

        @pl.when(q > spot)
        def _():
            pl.semaphore_signal(
                barrier, inc=1, device_id=device(r, chans[q]), device_id_type=MESH
            )

    first.wait()
    for dest in range(n_chan):
        x = images[dest]
        x = jnp.concatenate([x[:8], x[8:16], x[16:], jnp.zeros((8, width), f32)], axis=1)
        outbox[dest] = pltpu.roll(x, lax.rem(c, 4) * 32, 1).astype(bf16)

    @pl.when(r + spot > 0)
    def _():
        pl.semaphore_wait(barrier, r + spot)

    def send_row(row):
        pltpu.make_async_remote_copy(
            src_ref=outbox,
            dst_ref=stage.at[r],
            send_sem=stage_send,
            recv_sem=stage_sem.at[r],
            device_id=device(row, c),
            device_id_type=MESH,
        ).start()

    def send_hello(q):
        pltpu.make_async_remote_copy(
            src_ref=outbox.at[chans[q]],
            dst_ref=inbox.at[c, r],
            send_sem=piece_send,
            recv_sem=hello_sem.at[c],
            device_id=device(r, chans[q]),
            device_id_type=MESH,
        ).start()

    def send_piece(row, q):
        pltpu.make_async_remote_copy(
            src_ref=stage.at[row, chans[q]],
            dst_ref=inbox.at[c, row],
            send_sem=piece_send,
            recv_sem=piece_sem.at[row // 4, c],
            device_id=device(r, chans[q]),
            device_id_type=MESH,
        ).start()

    def await_copy(ref, sem):
        pltpu.make_async_remote_copy(
            src_ref=ref,
            dst_ref=ref,
            send_sem=stage_send,
            recv_sem=sem,
            device_id=device(r, c),
            device_id_type=MESH,
        ).wait_recv()

    for row in range(n_rows - 1):
        pl.when(row < r)(functools.partial(send_row, row))
    for q in range(n_chan - 1):
        pl.when(q < spot)(functools.partial(send_hello, q))
    copies = []
    for at in range(1, count):
        copy = pltpu.make_async_copy(sources[at], held[at], w_sem.at[at])
        copy.start()
        copies.append(copy)
    stage[r] = outbox[...]
    for copy in copies:
        copy.wait()
    prepare(p, s)
    channels = p["shift_mid"].shape[1]
    top_channels = p["shift_top"].shape[1]
    half = channels // 2
    cells = height * width
    fixed = cells * (jnp.sum(p["gain_mid"][...]) + jnp.sum(p["diag_mid"][...]))
    fixed = fixed + cells // 4 * (jnp.sum(p["gain_top"][...]) + jnp.sum(p["diag_top"][...]))
    fixed = fixed - 0.5 * log_two_pi * channels * cells

    for row in range(1, n_rows):

        @pl.when(row > r)
        def _():
            await_copy(stage.at[row], stage_sem.at[row])
            send_row(row)
            for q in range(n_chan - 1):
                pl.when(q < spot)(functools.partial(send_piece, row, q))

    for q in range(1, n_chan):

        @pl.when(q > spot)
        def _():
            await_copy(inbox.at[chans[q], 0], hello_sem.at[chans[q]])
            send_hello(q)
            for row in range(1, n_rows):
                pl.when(row > r)(functools.partial(send_piece, row, q))

    for row in range(n_rows - 1):

        @pl.when(row < r)
        def _():
            await_copy(stage.at[row], stage_sem.at[row])
            for q in range(n_chan):
                pl.when(q != spot)(functools.partial(send_piece, row, q))

    for row in range(n_rows):
        inbox[c, row] = stage[row, c]
    state = s["state"]
    lane = iota((1, LANES), 1)
    upper = n_rows // 2

    def collect(part):
        for q in range(n_chan):

            @pl.when((q < spot) & (lax.div(r, upper) == part))
            def _():
                await_copy(inbox.at[chans[q], 0], hello_sem.at[chans[q]])

            for own, pieces in ((part, upper - 1), (1 - part, upper)):

                @pl.when((q != spot) & (lax.div(r, upper) == own))
                def _():
                    await_copy(
                        inbox.at[chans[q], pl.ds(upper * part, pieces)],
                        piece_sem.at[part, chans[q]],
                    )

        for t in range(2 * upper * part, 2 * upper * (part + 1)):
            letters = [inbox[4 * (t % 2) + k, t // 2].astype(f32) for k in range(4)]
            for slab in range(3):
                x = letters[(3 - slab) % 4]
                for k in range(3):
                    x = jnp.where(lax.div(lane, 32) == k, letters[(k - slab) % 4], x)
                x = roll(x, -32 * slab)
                state[0, 8 * slab : 8 * slab + 8, t * LANES : (t + 1) * LANES] = x

    def send_latent():
        start = pl.multiple_of(2 * r * LANES, LANES)
        for to in range(n_chan):
            z = state[3, :16, pl.ds(start + to // 4 * LANES, LANES)]
            shift = -32 * (to % 4)
            z_send[to] = jnp.where(lane < 32, roll(z[:8], shift), roll(z[8:], shift + 32))
        for q in range(n_chan):

            @pl.when(q != spot)
            def _():
                pltpu.make_async_remote_copy(
                    src_ref=z_send.at[chans[q]],
                    dst_ref=z_recv.at[c],
                    send_sem=z_send_sem,
                    recv_sem=z_recv_sem.at[c],
                    device_id=device(r, chans[q]),
                    device_id_type=MESH,
                ).start()

        z_recv[c] = z_send[c]

    collect(0)
    score = mid_step(s, 0, True, (0, 8), (0, 8), (0, 7))
    score = score + mid_step(s, 1, False, (0, 7), (0, 8), (0, 6))
    score = score + mid_step(s, 2, False, (0, 6), (0, 6), (0, 5))
    pl.when(r < 2)(send_latent)
    collect(1)
    score = score + mid_step(s, 0, True, (8, 16), (6, 16), (7, 16))
    score = score + mid_step(s, 1, False, (7, 16), (6, 16), (6, 16))
    score = score + mid_step(s, 2, False, (6, 16), (4, 16), (5, 16))
    pl.when(r >= 2)(send_latent)

    squares = fold(state[3, :16, :] * state[3, :16, :])
    score = score - 0.5 * keep(squares, iota((16, 1), 0) < half)
    squeeze(state.at[3], s["top"])
    score_top = None
    for k in range(p["shift_top"].shape[0]):
        logs = top_step(s, k)
        score_top = logs if score_top is None else score_top + logs
    top = s["top"]
    squares = fold(top[...] * top[...])
    total = jnp.sum(score, axis=0, keepdims=True) + jnp.sum(score_top, axis=0, keepdims=True)
    total = total - 0.5 * jnp.sum(squares, axis=0, keepdims=True)
    total = jnp.sum(total, axis=1, keepdims=True)
    lik_out[...] = jnp.broadcast_to((total + fixed) / (channels * cells), (8, LANES))
    turned = s["turned"]
    for v in range(4):
        turned[v * LANES : (v + 1) * LANES, :top_channels] = jnp.transpose(
            top[:, v * LANES : (v + 1) * LANES]
        )
    for v in range(4):
        start = v * LANES + quad * 32 + side
        top_out[0, v * 16 : (v + 1) * 16, :] = turned[pl.ds(start, 16, stride=2), :][
            :, :top_channels
        ]

    for q in range(n_chan):

        @pl.when(q != spot)
        def _():
            await_copy(z_recv.at[chans[q]], z_recv_sem.at[chans[q]])

    for img in range(n_chan):
        z = z_recv[img]
        mid_out[img, :8, :] = z[:, :width]
        mid_out[img, 8:, :] = z[:4, width : 2 * width]
    for ref, sem in (
        (stage.at[pl.ds(0, n_rows - 1)], stage_send),
        (inbox.at[pl.ds(0, n_chan - 1)], piece_send),
        (z_recv.at[pl.ds(0, n_chan - 1)], z_send_sem),
    ):
        pltpu.make_async_remote_copy(
            src_ref=ref,
            dst_ref=ref,
            send_sem=sem,
            recv_sem=hello_sem.at[0],
            device_id=device(r, c),
            device_id_type=MESH,
        ).wait_send()


def deliver(mid, top, lik, mid_out, top_out, lik_out):
    for img in range(mid.shape[0]):
        mid_out[img, :, 0, :] = mid[img]
    top_out[...] = top[...]
    lik_out[...] = lik[0, :1]


def body(sizes, images, *params):
    n_rows, n_chan = sizes
    n_imgs, channels, own_rows, width = images.shape
    peers = n_rows * n_chan
    height = own_rows * peers
    params = parameters(params)
    hidden = params[6].shape[1]
    steps_mid, steps_top = params[0].shape[0], params[11].shape[0]
    top_channels = params[11].shape[1]
    half = channels // 2
    cells = height * width
    own = cells // 4 // n_rows
    operands = (images.reshape(n_imgs, channels, width),) + params
    vmem = pl.BlockSpec(memory_space=pltpu.VMEM)
    count = len(operands)
    work = work_scratch(steps_mid, steps_top, hidden, channels, top_channels, cells)
    mid, top, lik = pl.pallas_call(
        functools.partial(kernel, (n_rows, n_chan, height, width, count), list(work)),
        out_shape=(
            pltpu.VMEM((n_imgs, half, width), f32),
            pltpu.VMEM((1, own, top_channels), f32),
            pltpu.VMEM((8, LANES), f32),
        ),
        in_specs=[pl.BlockSpec(memory_space=pl.ANY)] * count,
        out_specs=(vmem, vmem, vmem),
        scratch_shapes=[pltpu.VMEM(x.shape, x.dtype) for x in operands]
        + list(work.values())
        + [
            pltpu.VMEM((n_chan, 8, LANES), bf16),
            pltpu.VMEM((n_rows, n_chan, 8, LANES), bf16),
            pltpu.VMEM((n_chan, n_rows, 8, LANES), bf16),
            pltpu.VMEM((n_chan, 8, LANES), f32),
            pltpu.VMEM((n_chan, 8, LANES), f32),
            pltpu.SemaphoreType.DMA((count,)),
            pltpu.SemaphoreType.DMA,
            pltpu.SemaphoreType.DMA,
            pltpu.SemaphoreType.DMA((n_rows,)),
            pltpu.SemaphoreType.DMA((n_chan,)),
            pltpu.SemaphoreType.DMA((2, n_chan)),
            pltpu.SemaphoreType.DMA,
            pltpu.SemaphoreType.DMA((n_chan,)),
        ],
        compiler_params=pltpu.CompilerParams(
            collective_id=0, has_side_effects=True, vmem_limit_bytes=56 * 1024 * 1024
        ),
        name="flow",
    )(*operands)
    latent_mid, top, lik = pl.pallas_call(
        deliver,
        out_shape=(
            jax.ShapeDtypeStruct((n_imgs, half, own_rows, width), f32),
            jax.ShapeDtypeStruct(top.shape, f32),
            jax.ShapeDtypeStruct((1,), f32),
        ),
        in_specs=[vmem, vmem, vmem],
        out_specs=(vmem, vmem, vmem),
        compiler_params=pltpu.CompilerParams(vmem_limit_bytes=4 * 1024 * 1024),
        name="deliver",
    )(mid, top, lik)
    latent_top = top.reshape(1, -1, width // 2, top_channels).transpose(0, 3, 1, 2)
    return latent_mid, latent_top, lik


def solution(mesh):
    sizes = (mesh.shape["rows"], mesh.shape["chan"])
    placed = (P("batch", None, ("rows", "chan"), None),) + (P(),) * 22
    return jax.shard_map(
        functools.partial(body, sizes),
        mesh=mesh,
        in_specs=placed,
        out_specs=(
            P("batch", None, ("rows", "chan"), None),
            P(("batch", "chan"), None, "rows", None),
            P(("batch", "chan")),
        ),
        check_vma=False,
    )
```

```python
import functools
import math

import jax
import jax.numpy as jnp
from jax import lax
from jax.experimental import pallas as pl
from jax.experimental.pallas import tpu as pltpu
from jax.sharding import PartitionSpec as P

MESH = pl.DeviceIdType.MESH
LANES = 128
CHUNK = 1024
FINE = lax.Precision.HIGHEST
log_two_pi = math.log(2.0 * math.pi)
f32 = jnp.float32
bf16 = jnp.bfloat16


def iota(shape, dim):
    return lax.broadcasted_iota(jnp.int32, shape, dim)


def dot_nt(a, b, precision=None):
    return lax.dot_general(
        a, b, (((1,), (1,)), ((), ())), preferred_element_type=f32, precision=precision
    )


def roll(x, amount):
    n = x.shape[1]
    amount = amount % n
    return x if amount == 0 else pltpu.roll(x, amount, 1)


def keep(x, ok):
    return jnp.where(ok, x, 0.0)


def mid_map(channels):
    i = iota((channels, channels), 0)
    j = iota((channels, channels), 1)
    source = jnp.where(i < 12, i, jnp.where(i < 16, i + 8, i - 4))
    return jnp.where(source == j, 1.0, 0.0)


def eye_map(channels):
    return jnp.where(iota((channels, channels), 0) == iota((channels, channels), 1), 1.0, 0.0)


def squeeze_map(channels):
    i = iota((channels, channels), 0)
    j = iota((channels, channels), 1)
    low = 4 * lax.rem(i, 8) + lax.div(i, 8)
    k = i - 32
    place = 2 * lax.div(k, 8) + 1 - lax.div(lax.rem(k + 64, 8), 4)
    high = 4 * (8 + lax.rem(k + 64, 4)) + place
    return jnp.where(jnp.where(i < 32, low, high) == j, 1.0, 0.0)


def split_two(x):
    high = x.astype(bf16).astype(f32)
    return high, x - high


def mixing(lower, upper, diag_row, gain_row, shift_row, out_map, in_map, exact):
    channels = lower.shape[0]
    i = iota((channels, channels), 0)
    j = iota((channels, channels), 1)
    eye = jnp.where(i == j, 1.0, 0.0)
    low = jnp.where(i > j, lower, 0.0) + eye
    upp = (jnp.where(i < j, upper, 0.0) + eye * jnp.exp(diag_row)) * jnp.exp(gain_row)
    rows = jnp.dot(out_map, low, precision=FINE, preferred_element_type=f32)
    mat = jnp.dot(rows, upp, precision=FINE, preferred_element_type=f32)
    bias = jnp.sum(mat * shift_row, axis=1, keepdims=True)
    if in_map is not None:
        mat = dot_nt(mat, in_map, FINE)
    high, rest = split_two(mat)
    parts = [high, rest] if exact else [high, high, rest]
    return jnp.concatenate(parts, axis=1).astype(bf16), bias


def mapped_column(row, mapping):
    return jnp.sum(mapping * row, axis=1, keepdims=True)


def prepare(p, s):
    steps_mid, channels = p["shift_mid"].shape
    steps_top, top_channels = p["shift_top"].shape
    hidden = p["w2_mid"].shape[1]
    half = channels // 2
    mapping = mid_map(channels)
    natural = eye_map(top_channels)
    for k in range(steps_mid):
        mat, bias = mixing(
            p["lower_mid"][k],
            p["upper_mid"][k],
            p["diag_mid"][k : k + 1, :],
            p["gain_mid"][k : k + 1, :],
            p["shift_mid"][k : k + 1, :],
            mapping,
            None if k == 0 else mapping,
            k == 0,
        )
        s["mix_mid"][k, :, : mat.shape[1]] = mat
        s["mix_bias_mid"][k] = jnp.broadcast_to(bias, (channels, LANES))
        s["b3_mid"][k] = jnp.broadcast_to(
            mapped_column(p["third_bias_mid"][k : k + 1, :], mapping), (channels, LANES)
        )
    for k in range(steps_top):
        mat, bias = mixing(
            p["lower_top"][k],
            p["upper_top"][k],
            p["diag_top"][k : k + 1, :],
            p["gain_top"][k : k + 1, :],
            p["shift_top"][k : k + 1, :],
            natural,
            squeeze_map(top_channels) if k == 0 else None,
            False,
        )
        s["mix_top"][k, :, : mat.shape[1]] = mat
        s["mix_bias_top"][k] = jnp.broadcast_to(bias, (top_channels, LANES))
        s["b3_top"][k] = jnp.broadcast_to(
            mapped_column(p["third_bias_top"][k : k + 1, :], natural), (top_channels, LANES)
        )
    for k in range(steps_mid):
        taps = []
        for tap in range(9):
            extra = [jnp.zeros((16 - half, hidden), f32)]
            if tap == 4:
                row = p["first_bias_mid"][k : k + 1, :].astype(f32)
                extra = [row, jnp.zeros((15 - half, hidden), f32)]
            taps.append(jnp.concatenate([p["w1_mid"][k, tap].astype(f32)] + extra, axis=0))
        s["w1t_mid"][k] = jnp.transpose(jnp.concatenate(taps, axis=0)).astype(bf16)
        s["w2t_mid"][k] = jnp.transpose(p["w2_mid"][k].astype(f32)).astype(bf16)
        s["b2_mid"][k] = jnp.transpose(
            jnp.broadcast_to(p["second_bias_mid"][k : k + 1, :], (LANES, hidden))
        )
        for tap in range(9):
            w = p["w3_mid"][k, tap * channels : (tap + 1) * channels, :].astype(f32)
            w = jnp.concatenate([w[:12], w[20:24], w[12:20]], axis=0)
            s["w3f_mid"][tap * channels : (tap + 1) * channels, :] = w
        s["w3p_mid"][k] = s["w3f_mid"][...].astype(bf16)
    for k in range(steps_top):
        row = p["first_bias_top"][k : k + 1, :].astype(f32)
        w = jnp.concatenate(
            [p["w1_top"][k].astype(f32), row, jnp.zeros((7, hidden), f32)], axis=0
        )
        s["w1t_top"][k] = jnp.transpose(w).astype(bf16)
        s["w2t_top"][k] = jnp.transpose(p["w2_top"][k].astype(f32)).astype(bf16)
        s["b2_top"][k] = jnp.transpose(
            jnp.broadcast_to(p["second_bias_top"][k : k + 1, :], (LANES, hidden))
        )


def wide(x, n):
    return jnp.concatenate([x] * (n // LANES), axis=1)


def lane_of(n):
    return lax.rem(iota((1, n), 1), LANES)


def edge_mid(x, dr):
    lane = iota((1, LANES), 1)
    if dr > 0:
        return keep(roll(x, -32), lane < 96)
    return keep(roll(x, 32), lane >= 32)


def edge_top(x, dr):
    lane = iota((1, LANES), 1)
    odd = lax.rem(lane, 2) == 1
    if dr > 0:
        return jnp.where(odd, keep(roll(x, -31), lane < 96), roll(x, -1))
    return jnp.where(odd, roll(x, 1), keep(roll(x, 31), lane >= 32))


def shift_col(x, dc, stride):
    n = x.shape[1]
    col = lax.rem(iota((1, n), 1), 32)
    if dc > 0:
        return keep(roll(x, -stride), col < 32 - stride)
    return keep(roll(x, stride), col >= stride)


def gather(y_ref, tap_rows, lo, hi, n, edge, stride):
    total = None
    for dc in (0, -1, 1):
        base = 4 + dc
        part = y_ref[base * tap_rows : (base + 1) * tap_rows, lo:hi]
        for dr in (-1, 1):
            tap = base + 3 * dr
            rows = slice(tap * tap_rows, (tap + 1) * tap_rows)
            if dr > 0 and hi == n:
                moved = [edge(y_ref[rows, :LANES], dr)]
                if hi - lo > LANES:
                    moved = [y_ref[rows, lo + LANES : hi]] + moved
                moved = jnp.concatenate(moved, axis=1) if len(moved) > 1 else moved[0]
            elif dr < 0 and lo == 0:
                moved = [edge(y_ref[rows, n - LANES : n], dr)]
                if hi - lo > LANES:
                    moved = moved + [y_ref[rows, : hi - LANES]]
                moved = jnp.concatenate(moved, axis=1) if len(moved) > 1 else moved[0]
            else:
                moved = y_ref[rows, lo + dr * LANES : hi + dr * LANES]
            part = part + moved
        if dc != 0:
            part = shift_col(part, dc, stride)
        total = part if total is None else total + part
    return total


def gated(g):
    e = jnp.exp(-jnp.abs(g))
    inv = 1.0 / (1.0 + e)
    gate = jnp.where(g >= 0, inv, e * inv)
    return gate, jnp.minimum(g, 0.0) - jnp.log(1.0 + e)


def fold(x):
    total = x[:, :LANES]
    for at in range(LANES, x.shape[1], LANES):
        total = total + x[:, at : at + LANES]
    return total


def mix(mat, bias, x, exact):
    n = x.shape[1]
    if exact:
        stack = [x, x]
    else:
        high, rest = split_two(x)
        stack = [high, rest, high]
    stack = jnp.concatenate(stack, axis=0).astype(bf16)
    return jnp.dot(mat, stack, preferred_element_type=f32) + wide(bias, n)


def product(first, second, third, bias, spread, y_ref, rows, lo):
    n = spread.shape[1]
    h = jnp.dot(first[...], spread, preferred_element_type=f32)
    h = jnp.maximum(h, 0.0).astype(bf16)
    h = jnp.dot(second[...], h, preferred_element_type=f32)
    h = jnp.maximum(h + wide(bias[...], n), 0.0).astype(bf16)
    y_ref[:rows, lo : lo + n] = jnp.dot(third[...], h, preferred_element_type=f32)


def mid_step(s, k, exact, mixed=None):
    state, u_ref, q_ref, y_ref = s["state"], s["u"], s["q"], s["y"]
    channels, n = state.shape
    block = 4 * LANES
    sub = iota((8, 1), 0)
    mat = s["mix_mid"][k, :, : (2 if exact else 3) * channels]
    for lo in range(0, n, block):
        u_ref[:, lo : lo + block] = mix(
            mat, s["mix_bias_mid"][k], state[:, lo : lo + block], exact
        )
    if mixed is not None:
        mixed()
    for lo in range(0, n, block):
        q = u_ref[:16, lo : lo + block]
        q = jnp.concatenate([q[:8], jnp.where(sub == 4, 1.0, q[8:])], axis=0)
        for dc in (-1, 0, 1):
            x = q if dc == 0 else shift_col(q, dc, 1)
            q_ref[dc + 1, :, LANES + lo : LANES + lo + block] = x.astype(bf16)
            if lo == 0:
                q_ref[dc + 1, :, LANES + n :] = edge_mid(x[:, :LANES], 1).astype(bf16)
            if lo + block == n:
                q_ref[dc + 1, :, :LANES] = edge_mid(x[:, block - LANES :], -1).astype(bf16)
    for lo in range(0, n, min(CHUNK, n)):
        taps = []
        for dr in (-1, 0, 1):
            at = lo + LANES * (1 + dr)
            for dc in (-1, 0, 1):
                taps.append(q_ref[dc + 1, :, at : at + min(CHUNK, n)])
        product(
            s["w1t_mid"].at[k],
            s["w2t_mid"].at[k],
            s["w3p_mid"].at[k],
            s["b2_mid"].at[k],
            jnp.concatenate(taps, axis=0),
            y_ref,
            9 * channels,
            lo,
        )
    score = None
    width = 2 * LANES
    for lo in range(0, n, width):
        out = gather(y_ref, channels, lo, lo + width, n, edge_mid, 1) + wide(s["b3_mid"][k], width)
        gate, logs = gated(out[:16] + 2.0)
        logs = fold(logs)
        score = logs if score is None else score + logs
        u = u_ref[:, lo : lo + width]
        state[:8, lo : lo + width] = u[:8]
        late = (u[8:16] + out[8:16]) * pltpu.roll(gate[8:16], 4, 0)
        state[8:16, lo : lo + width] = jnp.where(sub < 4, u[8:16], late)
        state[16:, lo : lo + width] = (u[16:] + out[16:]) * gate[:8]
    return keep(score, iota((16, 1), 0) < channels // 2)


def squeeze(s):
    state, top = s["state"], s["top"]
    odd = lax.rem(iota((1, LANES), 1), 2) == 1
    sub = iota((8, 1), 0)
    for v in range(4):
        tails = []
        for i in range(2):
            t = (2 * v + i) * LANES
            a = state[8:, t : t + LANES]
            t = t + 8 * LANES
            b = state[8:, t : t + LANES]
            even_col = jnp.where(odd, roll(b, 1), a)
            odd_col = jnp.where(odd, b, roll(a, -1))
            cols = slice(v * LANES, (v + 1) * LANES)
            top[16 * i : 16 * i + 8, cols] = even_col[8:]
            top[16 * i + 8 : 16 * i + 16, cols] = odd_col[8:]
            top[32 + 8 * i : 40 + 8 * i, cols] = jnp.where(
                sub < 4, pltpu.roll(odd_col[:8], 4, 0), even_col[:8]
            )


def top_step(s, k):
    state, u_ref, q_ref, y_ref = s["top"], s["u_top"], s["q_top"], s["y_top"]
    channels, n = state.shape
    half = channels // 2
    mat = s["mix_top"][k, :, : 3 * channels]
    u_ref[...] = mix(mat, s["mix_bias_top"][k], state[...], False)
    q = u_ref[:half, :]
    for dc in (-1, 0, 1):
        x = q if dc == 0 else shift_col(q, dc, 2)
        q_ref[dc + 1, :, LANES : LANES + n] = x
        q_ref[dc + 1, :, LANES + n :] = edge_top(x[:, :LANES], 1)
        q_ref[dc + 1, :, :LANES] = edge_top(x[:, n - LANES :], -1)
    ones = jnp.where(iota((8, min(CHUNK, n)), 0) == 0, 1.0, 0.0)
    for lo in range(0, n, min(CHUNK, n)):
        taps = []
        for dr in (-1, 0, 1):
            at = lo + LANES * (1 + dr)
            for dc in (-1, 0, 1):
                taps.append(q_ref[dc + 1, :, at : at + min(CHUNK, n)])
        product(
            s["w1t_top"].at[k],
            s["w2t_top"].at[k],
            s["w3_top"].at[k],
            s["b2_top"].at[k],
            jnp.concatenate(taps + [ones], axis=0).astype(bf16),
            y_ref,
            9 * channels,
            lo,
        )
    score = None
    width = LANES
    for lo in range(0, n, width):
        out = gather(y_ref, channels, lo, lo + width, n, edge_top, 2) + wide(s["b3_top"][k], width)
        gate, logs = gated(out[:half] + 2.0)
        score = logs if score is None else score + logs
        state[:half, lo : lo + width] = u_ref[:half, lo : lo + width]
        state[half:, lo : lo + width] = (u_ref[half:, lo : lo + width] + out[half:]) * gate
    return score


def work_scratch(steps_mid, steps_top, hidden, channels, top_channels, cells):
    n_top = cells // 4
    return {
        "mix_mid": pltpu.VMEM((steps_mid, channels, 3 * channels), bf16),
        "mix_bias_mid": pltpu.VMEM((steps_mid, channels, LANES), f32),
        "b3_mid": pltpu.VMEM((steps_mid, channels, LANES), f32),
        "mix_top": pltpu.VMEM((steps_top, top_channels, 3 * top_channels), bf16),
        "mix_bias_top": pltpu.VMEM((steps_top, top_channels, LANES), f32),
        "b3_top": pltpu.VMEM((steps_top, top_channels, LANES), f32),
        "w1t_mid": pltpu.VMEM((steps_mid, hidden, 144), bf16),
        "w2t_mid": pltpu.VMEM((steps_mid, hidden, hidden), bf16),
        "b2_mid": pltpu.VMEM((steps_mid, hidden, LANES), f32),
        "w3f_mid": pltpu.VMEM((9 * channels, hidden), f32),
        "w3p_mid": pltpu.VMEM((steps_mid, 9 * channels, hidden), bf16),
        "w1t_top": pltpu.VMEM((steps_top, hidden, 9 * top_channels // 2 + 8), bf16),
        "w2t_top": pltpu.VMEM((steps_top, hidden, hidden), bf16),
        "b2_top": pltpu.VMEM((steps_top, hidden, LANES), f32),
        "state": pltpu.VMEM((channels, cells), f32),
        "u": pltpu.VMEM((channels, cells), f32),
        "q": pltpu.VMEM((3, 16, cells + 2 * LANES), bf16),
        "y": pltpu.VMEM((9 * channels, cells), f32),
        "top": pltpu.VMEM((top_channels, n_top), f32),
        "u_top": pltpu.VMEM((top_channels, n_top), f32),
        "q_top": pltpu.VMEM((3, top_channels // 2, n_top + 2 * LANES), f32),
        "y_top": pltpu.VMEM((9 * top_channels, n_top), f32),
        "turned": pltpu.VMEM((n_top, LANES), f32),
    }


NAMES = (
    "shift_mid",
    "gain_mid",
    "lower_mid",
    "upper_mid",
    "diag_mid",
    "w1_mid",
    "first_bias_mid",
    "w2_mid",
    "second_bias_mid",
    "w3_mid",
    "third_bias_mid",
    "shift_top",
    "gain_top",
    "lower_top",
    "upper_top",
    "diag_top",
    "w1_top",
    "first_bias_top",
    "w2_top",
    "second_bias_top",
    "w3_top",
    "third_bias_top",
)


def parameters(params):
    (
        shift_mid, gain_mid, lower_mid, upper_mid, diag_mid, first_mid, first_bias_mid, second_mid,
        second_bias_mid, third_mid, third_bias_mid, shift_top, gain_top, lower_top, upper_top,
        diag_top, first_top, first_bias_top, second_top, second_bias_top, third_top, third_bias_top,
    ) = params
    steps_mid, hidden = first_bias_mid.shape
    steps_top = first_bias_top.shape[0]
    w1_top = first_top.reshape(steps_top, -1, hidden)
    w3_mid = third_mid.transpose(0, 1, 3, 2).reshape(steps_mid, -1, hidden)
    w3_top = third_top.transpose(0, 1, 3, 2).reshape(steps_top, -1, hidden)
    return (
        shift_mid, gain_mid, lower_mid, upper_mid, diag_mid, first_mid, first_bias_mid, second_mid,
        second_bias_mid, w3_mid, third_bias_mid, shift_top, gain_top, lower_top, upper_top,
        diag_top, w1_top, first_bias_top, second_top, second_bias_top, w3_top, third_bias_top,
    )


def kernel(dims, keys, *refs):
    n_rows, n_chan, height, width, count = dims
    sources, refs = refs[:count], refs[count:]
    (mid_out, top_out, lik_out), refs = refs[:3], refs[3:]
    held, refs = refs[:count], refs[count:]
    s, refs = dict(zip(keys, refs)), refs[len(keys) :]
    outbox, stage, inbox, z_send, z_recv, w_sem, refs = *refs[:6], refs[6:]
    stage_send, piece_send, stage_sem, hello_sem, piece_sem, z_send_sem, z_recv_sem = refs
    images = held[0]
    p = dict(zip(NAMES, held[1:]))
    s["w3_top"] = p["w3_top"]
    b = lax.axis_index("batch")
    r = lax.axis_index("rows")
    c = lax.axis_index("chan")
    quad = lax.div(r, 2)
    side = lax.rem(r, 2)

    def device(row, chan):
        return {"batch": b, "rows": row, "chan": chan}

    chans = []
    for q in range(n_chan):
        y = q // 2
        chans.append(2 * (y + y // 2 * (5 - 2 * y)) + 1 - q % 2)
    y = lax.div(c, 2)
    spot = 2 * (y + lax.div(y, 2) * (5 - 2 * y)) + 1 - lax.rem(c, 2)

    first = pltpu.make_async_copy(sources[0], held[0], w_sem.at[0])
    first.start()
    barrier = pltpu.get_barrier_semaphore()
    for row in range(1, n_rows):

        @pl.when(row > r)
        def _():
            pl.semaphore_signal(barrier, inc=1, device_id=device(row, c), device_id_type=MESH)

    for q in range(1, n_chan):

        @pl.when(q > spot)
        def _():
            pl.semaphore_signal(
                barrier, inc=1, device_id=device(r, chans[q]), device_id_type=MESH
            )

    first.wait()
    for dest in range(n_chan):
        x = images[dest]
        x = jnp.concatenate([x[:8], x[8:16], x[16:], jnp.zeros((8, width), f32)], axis=1)
        outbox[dest] = pltpu.roll(x, quad * 32, 1).astype(bf16)

    @pl.when(r + spot > 0)
    def _():
        pl.semaphore_wait(barrier, r + spot)

    def send_row(row):
        pltpu.make_async_remote_copy(
            src_ref=outbox,
            dst_ref=stage.at[r],
            send_sem=stage_send,
            recv_sem=stage_sem.at[r],
            device_id=device(row, c),
            device_id_type=MESH,
        ).start()

    def send_hello(q):
        pltpu.make_async_remote_copy(
            src_ref=outbox.at[chans[q]],
            dst_ref=inbox.at[c, r],
            send_sem=piece_send,
            recv_sem=hello_sem.at[c],
            device_id=device(r, chans[q]),
            device_id_type=MESH,
        ).start()

    def send_piece(row, q):
        pltpu.make_async_remote_copy(
            src_ref=stage.at[row, chans[q]],
            dst_ref=inbox.at[c, row],
            send_sem=piece_send,
            recv_sem=piece_sem.at[c],
            device_id=device(r, chans[q]),
            device_id_type=MESH,
        ).start()

    def await_copy(ref, sem):
        pltpu.make_async_remote_copy(
            src_ref=ref,
            dst_ref=ref,
            send_sem=stage_send,
            recv_sem=sem,
            device_id=device(r, c),
            device_id_type=MESH,
        ).wait_recv()

    for row in range(n_rows - 1):
        pl.when(row < r)(functools.partial(send_row, row))
    for q in range(n_chan - 1):
        pl.when(q < spot)(functools.partial(send_hello, q))
    copies = []
    for at in range(1, count):
        copy = pltpu.make_async_copy(sources[at], held[at], w_sem.at[at])
        copy.start()
        copies.append(copy)
    stage[r] = outbox[...]
    for copy in copies:
        copy.wait()
    prepare(p, s)
    channels = p["shift_mid"].shape[1]
    top_channels = p["shift_top"].shape[1]
    half = channels // 2
    cells = height * width
    fixed = cells * (jnp.sum(p["gain_mid"][...]) + jnp.sum(p["diag_mid"][...]))
    fixed = fixed + cells // 4 * (jnp.sum(p["gain_top"][...]) + jnp.sum(p["diag_top"][...]))
    fixed = fixed - 0.5 * log_two_pi * channels * cells

    for row in range(1, n_rows):

        @pl.when(row > r)
        def _():
            await_copy(stage.at[row], stage_sem.at[row])
            send_row(row)
            for q in range(n_chan - 1):
                pl.when(q < spot)(functools.partial(send_piece, row, q))

    for q in range(1, n_chan):

        @pl.when(q > spot)
        def _():
            await_copy(inbox.at[chans[q], 0], hello_sem.at[chans[q]])
            send_hello(q)
            for row in range(1, n_rows):
                pl.when(row > r)(functools.partial(send_piece, row, q))

    for row in range(n_rows - 1):

        @pl.when(row < r)
        def _():
            await_copy(stage.at[row], stage_sem.at[row])
            for q in range(n_chan):
                pl.when(q != spot)(functools.partial(send_piece, row, q))

    for row in range(n_rows):
        inbox[c, row] = stage[row, c]
    for q in range(n_chan):

        @pl.when(q < spot)
        def _():
            await_copy(inbox.at[chans[q], 0], hello_sem.at[chans[q]])

        @pl.when(q != spot)
        def _():
            await_copy(inbox.at[chans[q], pl.ds(0, n_rows - 1)], piece_sem.at[chans[q]])

    state = s["state"]
    lane = iota((1, LANES), 1)
    for t in range(height // 4):
        letters = [inbox[t % 8, 2 * k + t // 8].astype(f32) for k in range(4)]
        for slab in range(3):
            x = letters[(3 - slab) % 4]
            for k in range(3):
                x = jnp.where(lax.div(lane, 32) == k, letters[(k - slab) % 4], x)
            state[8 * slab : 8 * slab + 8, t * LANES : (t + 1) * LANES] = roll(x, -32 * slab)

    z_copies = []

    def send_latent():
        for to in range(n_chan):
            start = pl.multiple_of((side * n_chan + to) * LANES, LANES)
            z = s["u"][:16, pl.ds(start, LANES)]
            z_send[to] = jnp.where(
                lane < 32,
                pltpu.roll(z[:8], LANES - quad * 32, 1),
                pltpu.roll(z[8:], LANES + 32 - quad * 32, 1),
            )
        for d in range(1, n_chan):
            other = lax.rem(c + d, n_chan)
            copy = pltpu.make_async_remote_copy(
                src_ref=z_send.at[other],
                dst_ref=z_recv.at[c],
                send_sem=z_send_sem.at[d],
                recv_sem=z_recv_sem.at[d],
                device_id=device(r, other),
                device_id_type=MESH,
            )
            copy.start()
            z_copies.append(copy)
        z_recv[c] = z_send[c]

    score = None
    last = p["shift_mid"].shape[0] - 1
    for k in range(last + 1):
        logs = mid_step(s, k, k == 0, send_latent if k == last else None)
        score = logs if score is None else score + logs

    squares = fold(state[:16, :] * state[:16, :])
    score = score - 0.5 * keep(squares, iota((16, 1), 0) < half)
    squeeze(s)
    score_top = None
    for k in range(p["shift_top"].shape[0]):
        logs = top_step(s, k)
        score_top = logs if score_top is None else score_top + logs
    top = s["top"]
    squares = fold(top[...] * top[...])
    total = jnp.sum(score, axis=0, keepdims=True) + jnp.sum(score_top, axis=0, keepdims=True)
    total = total - 0.5 * jnp.sum(squares, axis=0, keepdims=True)
    total = jnp.sum(total, axis=1, keepdims=True)
    lik_out[...] = jnp.broadcast_to((total + fixed) / (channels * cells), (8, LANES))
    turned = s["turned"]
    for v in range(4):
        turned[v * LANES : (v + 1) * LANES, :top_channels] = jnp.transpose(
            top[:, v * LANES : (v + 1) * LANES]
        )
    for v in range(4):
        start = v * LANES + quad * 32 + side
        top_out[0, v * 16 : (v + 1) * 16, :] = turned[pl.ds(start, 16, stride=2), :][
            :, :top_channels
        ]

    for d in range(1, n_chan):
        pltpu.make_async_remote_copy(
            src_ref=z_send.at[0],
            dst_ref=z_recv.at[lax.rem(c + n_chan - d, n_chan)],
            send_sem=z_send_sem.at[d],
            recv_sem=z_recv_sem.at[d],
            device_id=device(r, c),
            device_id_type=MESH,
        ).wait_recv()
    for img in range(n_chan):
        z = z_recv[img]
        mid_out[img, :8, :] = z[:, :width]
        mid_out[img, 8:, :] = z[:4, width : 2 * width]
    for copy in z_copies:
        copy.wait_send()
    for ref, sem in (
        (stage.at[pl.ds(0, n_rows - 1)], stage_send),
        (inbox.at[pl.ds(0, n_chan - 1)], piece_send),
    ):
        pltpu.make_async_remote_copy(
            src_ref=ref,
            dst_ref=ref,
            send_sem=sem,
            recv_sem=hello_sem.at[0],
            device_id=device(r, c),
            device_id_type=MESH,
        ).wait_send()


def deliver(mid, top, lik, mid_out, top_out, lik_out):
    for img in range(mid.shape[0]):
        mid_out[img, :, 0, :] = mid[img]
    top_out[...] = top[...]
    lik_out[...] = lik[0, :1]


def body(sizes, images, *params):
    n_rows, n_chan = sizes
    n_imgs, channels, own_rows, width = images.shape
    peers = n_rows * n_chan
    height = own_rows * peers
    params = parameters(params)
    hidden = params[6].shape[1]
    steps_mid, steps_top = params[0].shape[0], params[11].shape[0]
    top_channels = params[11].shape[1]
    half = channels // 2
    cells = height * width
    own = cells // 4 // n_rows
    operands = (images.reshape(n_imgs, channels, width),) + params
    vmem = pl.BlockSpec(memory_space=pltpu.VMEM)
    count = len(operands)
    work = work_scratch(steps_mid, steps_top, hidden, channels, top_channels, cells)
    mid, top, lik = pl.pallas_call(
        functools.partial(kernel, (n_rows, n_chan, height, width, count), list(work)),
        out_shape=(
            pltpu.VMEM((n_imgs, half, width), f32),
            pltpu.VMEM((1, own, top_channels), f32),
            pltpu.VMEM((8, LANES), f32),
        ),
        in_specs=[pl.BlockSpec(memory_space=pl.ANY)] * count,
        out_specs=(vmem, vmem, vmem),
        scratch_shapes=[pltpu.VMEM(x.shape, x.dtype) for x in operands]
        + list(work.values())
        + [
            pltpu.VMEM((n_chan, 8, LANES), bf16),
            pltpu.VMEM((n_rows, n_chan, 8, LANES), bf16),
            pltpu.VMEM((n_chan, n_rows, 8, LANES), bf16),
            pltpu.VMEM((n_chan, 8, LANES), f32),
            pltpu.VMEM((n_chan, 8, LANES), f32),
            pltpu.SemaphoreType.DMA((count,)),
            pltpu.SemaphoreType.DMA,
            pltpu.SemaphoreType.DMA,
            pltpu.SemaphoreType.DMA((n_rows,)),
            pltpu.SemaphoreType.DMA((n_chan,)),
            pltpu.SemaphoreType.DMA((n_chan,)),
            pltpu.SemaphoreType.DMA((n_chan,)),
            pltpu.SemaphoreType.DMA((n_chan,)),
        ],
        compiler_params=pltpu.CompilerParams(
            collective_id=0, has_side_effects=True, vmem_limit_bytes=56 * 1024 * 1024
        ),
        name="flow",
    )(*operands)
    latent_mid, top, lik = pl.pallas_call(
        deliver,
        out_shape=(
            jax.ShapeDtypeStruct((n_imgs, half, own_rows, width), f32),
            jax.ShapeDtypeStruct(top.shape, f32),
            jax.ShapeDtypeStruct((1,), f32),
        ),
        in_specs=[vmem, vmem, vmem],
        out_specs=(vmem, vmem, vmem),
        compiler_params=pltpu.CompilerParams(vmem_limit_bytes=4 * 1024 * 1024),
        name="deliver",
    )(mid, top, lik)
    latent_top = top.reshape(1, -1, width // 2, top_channels).transpose(0, 3, 1, 2)
    return latent_mid, latent_top, lik


def solution(mesh):
    sizes = (mesh.shape["rows"], mesh.shape["chan"])
    placed = (P("batch", None, ("rows", "chan"), None),) + (P(),) * 22
    return jax.shard_map(
        functools.partial(body, sizes),
        mesh=mesh,
        in_specs=placed,
        out_specs=(
            P("batch", None, ("rows", "chan"), None),
            P(("batch", "chan"), None, "rows", None),
            P(("batch", "chan")),
        ),
        check_vma=False,
    )
```

```python
import functools
import math

import jax
import jax.numpy as jnp
from jax import lax
from jax.experimental import pallas as pl
from jax.experimental.pallas import tpu as pltpu
from jax.sharding import PartitionSpec as P

MESH = pl.DeviceIdType.MESH
LANES = 128
CHUNK = 1024
FINE = lax.Precision.HIGHEST
log_two_pi = math.log(2.0 * math.pi)
f32 = jnp.float32
bf16 = jnp.bfloat16


def iota(shape, dim):
    return lax.broadcasted_iota(jnp.int32, shape, dim)


def dot_nt(a, b, precision=None):
    return lax.dot_general(
        a, b, (((1,), (1,)), ((), ())), preferred_element_type=f32, precision=precision
    )


def roll(x, amount):
    n = x.shape[1]
    amount = amount % n
    return x if amount == 0 else pltpu.roll(x, amount, 1)


def keep(x, ok):
    return jnp.where(ok, x, 0.0)


def mid_map(channels):
    i = iota((channels, channels), 0)
    j = iota((channels, channels), 1)
    source = jnp.where(i < 12, i, jnp.where(i < 16, i + 8, i - 4))
    return jnp.where(source == j, 1.0, 0.0)


def eye_map(channels):
    return jnp.where(iota((channels, channels), 0) == iota((channels, channels), 1), 1.0, 0.0)


def squeeze_map(channels):
    i = iota((channels, channels), 0)
    j = iota((channels, channels), 1)
    low = 4 * lax.rem(i, 8) + lax.div(i, 8)
    k = i - 32
    place = 2 * lax.div(k, 8) + 1 - lax.div(lax.rem(k + 64, 8), 4)
    high = 4 * (8 + lax.rem(k + 64, 4)) + place
    return jnp.where(jnp.where(i < 32, low, high) == j, 1.0, 0.0)


def split_two(x):
    high = x.astype(bf16).astype(f32)
    return high, x - high


def mixing(lower, upper, diag_row, gain_row, shift_row, out_map, in_map, exact):
    channels = lower.shape[0]
    i = iota((channels, channels), 0)
    j = iota((channels, channels), 1)
    eye = jnp.where(i == j, 1.0, 0.0)
    low = jnp.where(i > j, lower, 0.0) + eye
    upp = (jnp.where(i < j, upper, 0.0) + eye * jnp.exp(diag_row)) * jnp.exp(gain_row)
    rows = jnp.dot(out_map, low, precision=FINE, preferred_element_type=f32)
    mat = jnp.dot(rows, upp, precision=FINE, preferred_element_type=f32)
    bias = jnp.sum(mat * shift_row, axis=1, keepdims=True)
    if in_map is not None:
        mat = dot_nt(mat, in_map, FINE)
    high, rest = split_two(mat)
    parts = [high, rest] if exact else [high, high, rest]
    return jnp.concatenate(parts, axis=1).astype(bf16), bias


def mapped_column(row, mapping):
    return jnp.sum(mapping * row, axis=1, keepdims=True)


def prepare(p, s):
    steps_mid, channels = p["shift_mid"].shape
    steps_top, top_channels = p["shift_top"].shape
    hidden = p["w2_mid"].shape[1]
    half = channels // 2
    mapping = mid_map(channels)
    natural = eye_map(top_channels)
    for k in range(steps_mid):
        mat, bias = mixing(
            p["lower_mid"][k],
            p["upper_mid"][k],
            p["diag_mid"][k : k + 1, :],
            p["gain_mid"][k : k + 1, :],
            p["shift_mid"][k : k + 1, :],
            mapping,
            None if k == 0 else mapping,
            k == 0,
        )
        s["mix_mid"][k, :, : mat.shape[1]] = mat
        s["mix_bias_mid"][k] = jnp.broadcast_to(bias, (channels, LANES))
        s["b3_mid"][k] = jnp.broadcast_to(
            mapped_column(p["third_bias_mid"][k : k + 1, :], mapping), (channels, LANES)
        )
    for k in range(steps_top):
        mat, bias = mixing(
            p["lower_top"][k],
            p["upper_top"][k],
            p["diag_top"][k : k + 1, :],
            p["gain_top"][k : k + 1, :],
            p["shift_top"][k : k + 1, :],
            natural,
            squeeze_map(top_channels) if k == 0 else None,
            False,
        )
        s["mix_top"][k, :, : mat.shape[1]] = mat
        s["mix_bias_top"][k] = jnp.broadcast_to(bias, (top_channels, LANES))
        s["b3_top"][k] = jnp.broadcast_to(
            mapped_column(p["third_bias_top"][k : k + 1, :], natural), (top_channels, LANES)
        )
    for k in range(steps_mid):
        taps = []
        for tap in range(9):
            extra = [jnp.zeros((16 - half, hidden), f32)]
            if tap == 4:
                row = p["first_bias_mid"][k : k + 1, :].astype(f32)
                extra = [row, jnp.zeros((15 - half, hidden), f32)]
            taps.append(jnp.concatenate([p["w1_mid"][k, tap].astype(f32)] + extra, axis=0))
        s["w1t_mid"][k] = jnp.transpose(jnp.concatenate(taps, axis=0)).astype(bf16)
        s["w2t_mid"][k] = jnp.transpose(p["w2_mid"][k].astype(f32)).astype(bf16)
        s["b2_mid"][k] = jnp.transpose(
            jnp.broadcast_to(p["second_bias_mid"][k : k + 1, :], (LANES, hidden))
        )
        for tap in range(9):
            w = p["w3_mid"][k, tap * channels : (tap + 1) * channels, :].astype(f32)
            w = jnp.concatenate([w[:12], w[20:24], w[12:20]], axis=0)
            s["w3f_mid"][tap * channels : (tap + 1) * channels, :] = w
        s["w3p_mid"][k] = s["w3f_mid"][...].astype(bf16)
    for k in range(steps_top):
        row = p["first_bias_top"][k : k + 1, :].astype(f32)
        w = jnp.concatenate(
            [p["w1_top"][k].astype(f32), row, jnp.zeros((7, hidden), f32)], axis=0
        )
        s["w1t_top"][k] = jnp.transpose(w).astype(bf16)
        s["w2t_top"][k] = jnp.transpose(p["w2_top"][k].astype(f32)).astype(bf16)
        s["b2_top"][k] = jnp.transpose(
            jnp.broadcast_to(p["second_bias_top"][k : k + 1, :], (LANES, hidden))
        )


def wide(x, n):
    return jnp.concatenate([x] * (n // LANES), axis=1)


def lane_of(n):
    return lax.rem(iota((1, n), 1), LANES)


def edge_mid(x, dr):
    lane = iota((1, LANES), 1)
    if dr > 0:
        return keep(roll(x, -32), lane < 96)
    return keep(roll(x, 32), lane >= 32)


def edge_top(x, dr):
    lane = iota((1, LANES), 1)
    odd = lax.rem(lane, 2) == 1
    if dr > 0:
        return jnp.where(odd, keep(roll(x, -31), lane < 96), roll(x, -1))
    return jnp.where(odd, roll(x, 1), keep(roll(x, 31), lane >= 32))


def shift_col(x, dc, stride):
    n = x.shape[1]
    col = lax.rem(iota((1, n), 1), 32)
    if dc > 0:
        return keep(roll(x, -stride), col < 32 - stride)
    return keep(roll(x, stride), col >= stride)


def gather(y_ref, tap_rows, lo, hi, n, edge, stride):
    total = None
    for dc in (0, -1, 1):
        base = 4 + dc
        part = y_ref[base * tap_rows : (base + 1) * tap_rows, lo:hi]
        for dr in (-1, 1):
            tap = base + 3 * dr
            rows = slice(tap * tap_rows, (tap + 1) * tap_rows)
            if dr > 0 and hi == n:
                moved = [edge(y_ref[rows, :LANES], dr)]
                if hi - lo > LANES:
                    moved = [y_ref[rows, lo + LANES : hi]] + moved
                moved = jnp.concatenate(moved, axis=1) if len(moved) > 1 else moved[0]
            elif dr < 0 and lo == 0:
                moved = [edge(y_ref[rows, n - LANES : n], dr)]
                if hi - lo > LANES:
                    moved = moved + [y_ref[rows, : hi - LANES]]
                moved = jnp.concatenate(moved, axis=1) if len(moved) > 1 else moved[0]
            else:
                moved = y_ref[rows, lo + dr * LANES : hi + dr * LANES]
            part = part + moved
        if dc != 0:
            part = shift_col(part, dc, stride)
        total = part if total is None else total + part
    return total


def gated(g):
    e = jnp.exp(-jnp.abs(g))
    inv = 1.0 / (1.0 + e)
    gate = jnp.where(g >= 0, inv, e * inv)
    return gate, jnp.minimum(g, 0.0) - jnp.log(1.0 + e)


def fold(x):
    total = x[:, :LANES]
    for at in range(LANES, x.shape[1], LANES):
        total = total + x[:, at : at + LANES]
    return total


def mix(mat, bias, x, exact):
    n = x.shape[1]
    if exact:
        stack = [x, x]
    else:
        high, rest = split_two(x)
        stack = [high, rest, high]
    stack = jnp.concatenate(stack, axis=0).astype(bf16)
    return jnp.dot(mat, stack, preferred_element_type=f32) + wide(bias, n)


def product(first, second, third, bias, spread, y_ref, rows, lo):
    n = spread.shape[1]
    h = jnp.dot(first[...], spread, preferred_element_type=f32)
    h = jnp.maximum(h, 0.0).astype(bf16)
    h = jnp.dot(second[...], h, preferred_element_type=f32)
    h = jnp.maximum(h + wide(bias[...], n), 0.0).astype(bf16)
    y_ref[:rows, lo : lo + n] = jnp.dot(third[...], h, preferred_element_type=f32)


def mid_step(s, k, exact, mixed=None):
    state, u_ref, q_ref, y_ref = s["state"], s["u"], s["q"], s["y"]
    channels, n = state.shape
    block = 4 * LANES
    sub = iota((8, 1), 0)
    mat = s["mix_mid"][k, :, : (2 if exact else 3) * channels]
    for lo in range(0, n, block):
        u_ref[:, lo : lo + block] = mix(
            mat, s["mix_bias_mid"][k], state[:, lo : lo + block], exact
        )
    if mixed is not None:
        mixed()
    for lo in range(0, n, block):
        q = u_ref[:16, lo : lo + block]
        q = jnp.concatenate([q[:8], jnp.where(sub == 4, 1.0, q[8:])], axis=0)
        for dc in (-1, 0, 1):
            x = q if dc == 0 else shift_col(q, dc, 1)
            q_ref[dc + 1, :, LANES + lo : LANES + lo + block] = x.astype(bf16)
            if lo == 0:
                q_ref[dc + 1, :, LANES + n :] = edge_mid(x[:, :LANES], 1).astype(bf16)
            if lo + block == n:
                q_ref[dc + 1, :, :LANES] = edge_mid(x[:, block - LANES :], -1).astype(bf16)
    for lo in range(0, n, min(CHUNK, n)):
        taps = []
        for dr in (-1, 0, 1):
            at = lo + LANES * (1 + dr)
            for dc in (-1, 0, 1):
                taps.append(q_ref[dc + 1, :, at : at + min(CHUNK, n)])
        product(
            s["w1t_mid"].at[k],
            s["w2t_mid"].at[k],
            s["w3p_mid"].at[k],
            s["b2_mid"].at[k],
            jnp.concatenate(taps, axis=0),
            y_ref,
            9 * channels,
            lo,
        )
    score = None
    width = 2 * LANES
    for lo in range(0, n, width):
        out = gather(y_ref, channels, lo, lo + width, n, edge_mid, 1) + wide(s["b3_mid"][k], width)
        gate, logs = gated(out[:16] + 2.0)
        logs = fold(logs)
        score = logs if score is None else score + logs
        u = u_ref[:, lo : lo + width]
        state[:8, lo : lo + width] = u[:8]
        late = (u[8:16] + out[8:16]) * pltpu.roll(gate[8:16], 4, 0)
        state[8:16, lo : lo + width] = jnp.where(sub < 4, u[8:16], late)
        state[16:, lo : lo + width] = (u[16:] + out[16:]) * gate[:8]
    return keep(score, iota((16, 1), 0) < channels // 2)


def squeeze(s):
    state, top = s["state"], s["top"]
    odd = lax.rem(iota((1, LANES), 1), 2) == 1
    sub = iota((8, 1), 0)
    for v in range(4):
        tails = []
        for i in range(2):
            t = (2 * v + i) * LANES
            a = state[8:, t : t + LANES]
            t = t + 8 * LANES
            b = state[8:, t : t + LANES]
            even_col = jnp.where(odd, roll(b, 1), a)
            odd_col = jnp.where(odd, b, roll(a, -1))
            cols = slice(v * LANES, (v + 1) * LANES)
            top[16 * i : 16 * i + 8, cols] = even_col[8:]
            top[16 * i + 8 : 16 * i + 16, cols] = odd_col[8:]
            top[32 + 8 * i : 40 + 8 * i, cols] = jnp.where(
                sub < 4, pltpu.roll(odd_col[:8], 4, 0), even_col[:8]
            )


def top_step(s, k):
    state, u_ref, q_ref, y_ref = s["top"], s["u_top"], s["q_top"], s["y_top"]
    channels, n = state.shape
    half = channels // 2
    mat = s["mix_top"][k, :, : 3 * channels]
    u_ref[...] = mix(mat, s["mix_bias_top"][k], state[...], False)
    q = u_ref[:half, :]
    for dc in (-1, 0, 1):
        x = q if dc == 0 else shift_col(q, dc, 2)
        q_ref[dc + 1, :, LANES : LANES + n] = x
        q_ref[dc + 1, :, LANES + n :] = edge_top(x[:, :LANES], 1)
        q_ref[dc + 1, :, :LANES] = edge_top(x[:, n - LANES :], -1)
    ones = jnp.where(iota((8, min(CHUNK, n)), 0) == 0, 1.0, 0.0)
    for lo in range(0, n, min(CHUNK, n)):
        taps = []
        for dr in (-1, 0, 1):
            at = lo + LANES * (1 + dr)
            for dc in (-1, 0, 1):
                taps.append(q_ref[dc + 1, :, at : at + min(CHUNK, n)])
        product(
            s["w1t_top"].at[k],
            s["w2t_top"].at[k],
            s["w3_top"].at[k],
            s["b2_top"].at[k],
            jnp.concatenate(taps + [ones], axis=0).astype(bf16),
            y_ref,
            9 * channels,
            lo,
        )
    score = None
    width = LANES
    for lo in range(0, n, width):
        out = gather(y_ref, channels, lo, lo + width, n, edge_top, 2) + wide(s["b3_top"][k], width)
        gate, logs = gated(out[:half] + 2.0)
        score = logs if score is None else score + logs
        state[:half, lo : lo + width] = u_ref[:half, lo : lo + width]
        state[half:, lo : lo + width] = (u_ref[half:, lo : lo + width] + out[half:]) * gate
    return score


def work_scratch(steps_mid, steps_top, hidden, channels, top_channels, cells):
    n_top = cells // 4
    return {
        "mix_mid": pltpu.VMEM((steps_mid, channels, 3 * channels), bf16),
        "mix_bias_mid": pltpu.VMEM((steps_mid, channels, LANES), f32),
        "b3_mid": pltpu.VMEM((steps_mid, channels, LANES), f32),
        "mix_top": pltpu.VMEM((steps_top, top_channels, 3 * top_channels), bf16),
        "mix_bias_top": pltpu.VMEM((steps_top, top_channels, LANES), f32),
        "b3_top": pltpu.VMEM((steps_top, top_channels, LANES), f32),
        "w1t_mid": pltpu.VMEM((steps_mid, hidden, 144), bf16),
        "w2t_mid": pltpu.VMEM((steps_mid, hidden, hidden), bf16),
        "b2_mid": pltpu.VMEM((steps_mid, hidden, LANES), f32),
        "w3f_mid": pltpu.VMEM((9 * channels, hidden), f32),
        "w3p_mid": pltpu.VMEM((steps_mid, 9 * channels, hidden), bf16),
        "w1t_top": pltpu.VMEM((steps_top, hidden, 9 * top_channels // 2 + 8), bf16),
        "w2t_top": pltpu.VMEM((steps_top, hidden, hidden), bf16),
        "b2_top": pltpu.VMEM((steps_top, hidden, LANES), f32),
        "state": pltpu.VMEM((channels, cells), f32),
        "u": pltpu.VMEM((channels, cells), f32),
        "q": pltpu.VMEM((3, 16, cells + 2 * LANES), bf16),
        "y": pltpu.VMEM((9 * channels, cells), f32),
        "top": pltpu.VMEM((top_channels, n_top), f32),
        "u_top": pltpu.VMEM((top_channels, n_top), f32),
        "q_top": pltpu.VMEM((3, top_channels // 2, n_top + 2 * LANES), f32),
        "y_top": pltpu.VMEM((9 * top_channels, n_top), f32),
        "turned": pltpu.VMEM((n_top, LANES), f32),
    }


NAMES = (
    "shift_mid",
    "gain_mid",
    "lower_mid",
    "upper_mid",
    "diag_mid",
    "w1_mid",
    "first_bias_mid",
    "w2_mid",
    "second_bias_mid",
    "w3_mid",
    "third_bias_mid",
    "shift_top",
    "gain_top",
    "lower_top",
    "upper_top",
    "diag_top",
    "w1_top",
    "first_bias_top",
    "w2_top",
    "second_bias_top",
    "w3_top",
    "third_bias_top",
)


def parameters(params):
    (
        shift_mid, gain_mid, lower_mid, upper_mid, diag_mid, first_mid, first_bias_mid, second_mid,
        second_bias_mid, third_mid, third_bias_mid, shift_top, gain_top, lower_top, upper_top,
        diag_top, first_top, first_bias_top, second_top, second_bias_top, third_top, third_bias_top,
    ) = params
    steps_mid, hidden = first_bias_mid.shape
    steps_top = first_bias_top.shape[0]
    w1_top = first_top.reshape(steps_top, -1, hidden)
    w3_mid = third_mid.transpose(0, 1, 3, 2).reshape(steps_mid, -1, hidden)
    w3_top = third_top.transpose(0, 1, 3, 2).reshape(steps_top, -1, hidden)
    return (
        shift_mid, gain_mid, lower_mid, upper_mid, diag_mid, first_mid, first_bias_mid, second_mid,
        second_bias_mid, w3_mid, third_bias_mid, shift_top, gain_top, lower_top, upper_top,
        diag_top, w1_top, first_bias_top, second_top, second_bias_top, w3_top, third_bias_top,
    )


def kernel(dims, keys, *refs):
    n_rows, n_chan, height, width, count = dims
    sources, refs = refs[:count], refs[count:]
    (mid_out, top_out, lik_out), refs = refs[:3], refs[3:]
    held, refs = refs[:count], refs[count:]
    s, refs = dict(zip(keys, refs)), refs[len(keys) :]
    outbox, stage, inbox, z_send, z_recv, w_sem, refs = *refs[:6], refs[6:]
    stage_send, piece_send, stage_sem, hello_sem, piece_sem, z_send_sem, z_recv_sem = refs
    images = held[0]
    p = dict(zip(NAMES, held[1:]))
    s["w3_top"] = p["w3_top"]
    b = lax.axis_index("batch")
    r = lax.axis_index("rows")
    c = lax.axis_index("chan")
    quad = lax.div(r, 2)
    side = lax.rem(r, 2)

    def device(row, chan):
        return {"batch": b, "rows": row, "chan": chan}

    chans = []
    for q in range(n_chan):
        y = q // 2
        chans.append(2 * (y + y // 2 * (5 - 2 * y)) + 1 - q % 2)
    y = lax.div(c, 2)
    spot = 2 * (y + lax.div(y, 2) * (5 - 2 * y)) + 1 - lax.rem(c, 2)

    first = pltpu.make_async_copy(sources[0], held[0], w_sem.at[0])
    first.start()
    barrier = pltpu.get_barrier_semaphore()
    for row in range(1, n_rows):

        @pl.when(row > r)
        def _():
            pl.semaphore_signal(barrier, inc=1, device_id=device(row, c), device_id_type=MESH)

    for q in range(1, n_chan):

        @pl.when(q > spot)
        def _():
            pl.semaphore_signal(
                barrier, inc=1, device_id=device(r, chans[q]), device_id_type=MESH
            )

    first.wait()
    for dest in range(n_chan):
        x = images[dest]
        x = jnp.concatenate([x[:8], x[8:16], x[16:], jnp.zeros((8, width), f32)], axis=1)
        outbox[dest] = pltpu.roll(x, quad * 32, 1).astype(bf16)

    @pl.when(r + spot > 0)
    def _():
        pl.semaphore_wait(barrier, r + spot)

    def send_row(row):
        pltpu.make_async_remote_copy(
            src_ref=outbox,
            dst_ref=stage.at[r],
            send_sem=stage_send,
            recv_sem=stage_sem.at[r],
            device_id=device(row, c),
            device_id_type=MESH,
        ).start()

    def send_hello(q):
        pltpu.make_async_remote_copy(
            src_ref=outbox.at[chans[q]],
            dst_ref=inbox.at[c, r],
            send_sem=piece_send,
            recv_sem=hello_sem.at[c],
            device_id=device(r, chans[q]),
            device_id_type=MESH,
        ).start()

    def send_piece(row, q):
        pltpu.make_async_remote_copy(
            src_ref=stage.at[row, chans[q]],
            dst_ref=inbox.at[c, row],
            send_sem=piece_send,
            recv_sem=piece_sem.at[c],
            device_id=device(r, chans[q]),
            device_id_type=MESH,
        ).start()

    def await_copy(ref, sem):
        pltpu.make_async_remote_copy(
            src_ref=ref,
            dst_ref=ref,
            send_sem=stage_send,
            recv_sem=sem,
            device_id=device(r, c),
            device_id_type=MESH,
        ).wait_recv()

    pl.when(r > 0)(functools.partial(send_row, 0))
    for q in range(n_chan - 1):
        pl.when(q < spot)(functools.partial(send_hello, q))
    copies = []
    for at in range(1, count):
        copy = pltpu.make_async_copy(sources[at], held[at], w_sem.at[at])
        copy.start()
        copies.append(copy)
    stage[r] = outbox[...]
    copies[0].wait()
    for row in range(1, n_rows - 1):
        pl.when(row < r)(functools.partial(send_row, row))
    for copy in copies[1:]:
        copy.wait()
    prepare(p, s)
    channels = p["shift_mid"].shape[1]
    top_channels = p["shift_top"].shape[1]
    half = channels // 2
    cells = height * width
    fixed = cells * (jnp.sum(p["gain_mid"][...]) + jnp.sum(p["diag_mid"][...]))
    fixed = fixed + cells // 4 * (jnp.sum(p["gain_top"][...]) + jnp.sum(p["diag_top"][...]))
    fixed = fixed - 0.5 * log_two_pi * channels * cells

    for row in range(1, n_rows):

        @pl.when(row > r)
        def _():
            await_copy(stage.at[row], stage_sem.at[row])
            send_row(row)
            for q in range(n_chan - 1):
                pl.when(q < spot)(functools.partial(send_piece, row, q))

    for q in range(1, n_chan):

        @pl.when(q > spot)
        def _():
            await_copy(inbox.at[chans[q], 0], hello_sem.at[chans[q]])
            send_hello(q)
            for row in range(1, n_rows):
                pl.when(row > r)(functools.partial(send_piece, row, q))

    for row in range(n_rows - 1):

        @pl.when(row < r)
        def _():
            await_copy(stage.at[row], stage_sem.at[row])
            for q in range(n_chan):
                pl.when(q != spot)(functools.partial(send_piece, row, q))

    for row in range(n_rows):
        inbox[c, row] = stage[row, c]
    for q in range(n_chan):

        @pl.when(q < spot)
        def _():
            await_copy(inbox.at[chans[q], 0], hello_sem.at[chans[q]])

        @pl.when(q != spot)
        def _():
            await_copy(inbox.at[chans[q], pl.ds(0, n_rows - 1)], piece_sem.at[chans[q]])

    state = s["state"]
    lane = iota((1, LANES), 1)
    for t in range(height // 4):
        letters = [inbox[t % 8, 2 * k + t // 8].astype(f32) for k in range(4)]
        for slab in range(3):
            x = letters[(3 - slab) % 4]
            for k in range(3):
                x = jnp.where(lax.div(lane, 32) == k, letters[(k - slab) % 4], x)
            state[8 * slab : 8 * slab + 8, t * LANES : (t + 1) * LANES] = roll(x, -32 * slab)

    z_copies = []

    def send_latent():
        for to in range(n_chan):
            start = pl.multiple_of((side * n_chan + to) * LANES, LANES)
            z = s["u"][:16, pl.ds(start, LANES)]
            z_send[to] = jnp.where(
                lane < 32,
                pltpu.roll(z[:8], LANES - quad * 32, 1),
                pltpu.roll(z[8:], LANES + 32 - quad * 32, 1),
            )
        for d in range(1, n_chan):
            other = lax.rem(c + d, n_chan)
            copy = pltpu.make_async_remote_copy(
                src_ref=z_send.at[other],
                dst_ref=z_recv.at[c],
                send_sem=z_send_sem.at[d],
                recv_sem=z_recv_sem.at[d],
                device_id=device(r, other),
                device_id_type=MESH,
            )
            copy.start()
            z_copies.append(copy)
        z_recv[c] = z_send[c]

    score = None
    last = p["shift_mid"].shape[0] - 1
    for k in range(last + 1):
        logs = mid_step(s, k, k == 0, send_latent if k == last else None)
        score = logs if score is None else score + logs

    squares = fold(state[:16, :] * state[:16, :])
    score = score - 0.5 * keep(squares, iota((16, 1), 0) < half)
    squeeze(s)
    score_top = None
    for k in range(p["shift_top"].shape[0]):
        logs = top_step(s, k)
        score_top = logs if score_top is None else score_top + logs
    top = s["top"]
    squares = fold(top[...] * top[...])
    total = jnp.sum(score, axis=0, keepdims=True) + jnp.sum(score_top, axis=0, keepdims=True)
    total = total - 0.5 * jnp.sum(squares, axis=0, keepdims=True)
    total = jnp.sum(total, axis=1, keepdims=True)
    lik_out[...] = jnp.broadcast_to((total + fixed) / (channels * cells), (8, LANES))
    turned = s["turned"]
    for v in range(4):
        turned[v * LANES : (v + 1) * LANES, :top_channels] = jnp.transpose(
            top[:, v * LANES : (v + 1) * LANES]
        )
    for v in range(4):
        start = v * LANES + quad * 32 + side
        top_out[0, v * 16 : (v + 1) * 16, :] = turned[pl.ds(start, 16, stride=2), :][
            :, :top_channels
        ]

    for d in range(1, n_chan):
        pltpu.make_async_remote_copy(
            src_ref=z_send.at[0],
            dst_ref=z_recv.at[lax.rem(c + n_chan - d, n_chan)],
            send_sem=z_send_sem.at[d],
            recv_sem=z_recv_sem.at[d],
            device_id=device(r, c),
            device_id_type=MESH,
        ).wait_recv()
    for img in range(n_chan):
        z = z_recv[img]
        mid_out[img, :8, :] = z[:, :width]
        mid_out[img, 8:, :] = z[:4, width : 2 * width]
    for copy in z_copies:
        copy.wait_send()
    for ref, sem in (
        (stage.at[pl.ds(0, n_rows - 1)], stage_send),
        (inbox.at[pl.ds(0, n_chan - 1)], piece_send),
    ):
        pltpu.make_async_remote_copy(
            src_ref=ref,
            dst_ref=ref,
            send_sem=sem,
            recv_sem=hello_sem.at[0],
            device_id=device(r, c),
            device_id_type=MESH,
        ).wait_send()


def deliver(mid, top, lik, mid_out, top_out, lik_out):
    for img in range(mid.shape[0]):
        mid_out[img, :, 0, :] = mid[img]
    top_out[...] = top[...]
    lik_out[...] = lik[0, :1]


def body(sizes, images, *params):
    n_rows, n_chan = sizes
    n_imgs, channels, own_rows, width = images.shape
    peers = n_rows * n_chan
    height = own_rows * peers
    params = parameters(params)
    hidden = params[6].shape[1]
    steps_mid, steps_top = params[0].shape[0], params[11].shape[0]
    top_channels = params[11].shape[1]
    half = channels // 2
    cells = height * width
    own = cells // 4 // n_rows
    operands = (images.reshape(n_imgs, channels, width),) + params
    vmem = pl.BlockSpec(memory_space=pltpu.VMEM)
    count = len(operands)
    work = work_scratch(steps_mid, steps_top, hidden, channels, top_channels, cells)
    mid, top, lik = pl.pallas_call(
        functools.partial(kernel, (n_rows, n_chan, height, width, count), list(work)),
        out_shape=(
            pltpu.VMEM((n_imgs, half, width), f32),
            pltpu.VMEM((1, own, top_channels), f32),
            pltpu.VMEM((8, LANES), f32),
        ),
        in_specs=[pl.BlockSpec(memory_space=pl.ANY)] * count,
        out_specs=(vmem, vmem, vmem),
        scratch_shapes=[pltpu.VMEM(x.shape, x.dtype) for x in operands]
        + list(work.values())
        + [
            pltpu.VMEM((n_chan, 8, LANES), bf16),
            pltpu.VMEM((n_rows, n_chan, 8, LANES), bf16),
            pltpu.VMEM((n_chan, n_rows, 8, LANES), bf16),
            pltpu.VMEM((n_chan, 8, LANES), f32),
            pltpu.VMEM((n_chan, 8, LANES), f32),
            pltpu.SemaphoreType.DMA((count,)),
            pltpu.SemaphoreType.DMA,
            pltpu.SemaphoreType.DMA,
            pltpu.SemaphoreType.DMA((n_rows,)),
            pltpu.SemaphoreType.DMA((n_chan,)),
            pltpu.SemaphoreType.DMA((n_chan,)),
            pltpu.SemaphoreType.DMA((n_chan,)),
            pltpu.SemaphoreType.DMA((n_chan,)),
        ],
        compiler_params=pltpu.CompilerParams(
            collective_id=0, has_side_effects=True, vmem_limit_bytes=56 * 1024 * 1024
        ),
        name="flow",
    )(*operands)
    latent_mid, top, lik = pl.pallas_call(
        deliver,
        out_shape=(
            jax.ShapeDtypeStruct((n_imgs, half, own_rows, width), f32),
            jax.ShapeDtypeStruct(top.shape, f32),
            jax.ShapeDtypeStruct((1,), f32),
        ),
        in_specs=[vmem, vmem, vmem],
        out_specs=(vmem, vmem, vmem),
        compiler_params=pltpu.CompilerParams(vmem_limit_bytes=4 * 1024 * 1024),
        name="deliver",
    )(mid, top, lik)
    latent_top = top.reshape(1, -1, width // 2, top_channels).transpose(0, 3, 1, 2)
    return latent_mid, latent_top, lik


def solution(mesh):
    sizes = (mesh.shape["rows"], mesh.shape["chan"])
    placed = (P("batch", None, ("rows", "chan"), None),) + (P(),) * 22
    return jax.shard_map(
        functools.partial(body, sizes),
        mesh=mesh,
        in_specs=placed,
        out_specs=(
            P("batch", None, ("rows", "chan"), None),
            P(("batch", "chan"), None, "rows", None),
            P(("batch", "chan")),
        ),
        check_vma=False,
    )
```

```python
import functools
import math

import jax
import jax.numpy as jnp
from jax import lax
from jax.experimental import pallas as pl
from jax.experimental.pallas import tpu as pltpu
from jax.sharding import PartitionSpec as P

MESH = pl.DeviceIdType.MESH
LANES = 128
CHUNK = 1024
FINE = lax.Precision.HIGHEST
log_two_pi = math.log(2.0 * math.pi)
f32 = jnp.float32
bf16 = jnp.bfloat16


def iota(shape, dim):
    return lax.broadcasted_iota(jnp.int32, shape, dim)


def dot_nt(a, b, precision=None):
    return lax.dot_general(
        a, b, (((1,), (1,)), ((), ())), preferred_element_type=f32, precision=precision
    )


def roll(x, amount):
    n = x.shape[1]
    amount = amount % n
    return x if amount == 0 else pltpu.roll(x, amount, 1)


def keep(x, ok):
    return jnp.where(ok, x, 0.0)


def mid_map(channels):
    i = iota((channels, channels), 0)
    j = iota((channels, channels), 1)
    source = jnp.where(i < 12, i, jnp.where(i < 16, i + 8, i - 4))
    return jnp.where(source == j, 1.0, 0.0)


def eye_map(channels):
    return jnp.where(iota((channels, channels), 0) == iota((channels, channels), 1), 1.0, 0.0)


def squeeze_map(channels):
    i = iota((channels, channels), 0)
    j = iota((channels, channels), 1)
    low = 4 * lax.rem(i, 8) + lax.div(i, 8)
    k = i - 32
    place = 2 * lax.div(k, 8) + 1 - lax.div(lax.rem(k + 64, 8), 4)
    high = 4 * (8 + lax.rem(k + 64, 4)) + place
    return jnp.where(jnp.where(i < 32, low, high) == j, 1.0, 0.0)


def split_two(x):
    high = x.astype(bf16).astype(f32)
    return high, x - high


def mixing(lower, upper, diag_row, gain_row, shift_row, out_map, in_map, exact):
    channels = lower.shape[0]
    i = iota((channels, channels), 0)
    j = iota((channels, channels), 1)
    eye = jnp.where(i == j, 1.0, 0.0)
    low = jnp.where(i > j, lower, 0.0) + eye
    upp = (jnp.where(i < j, upper, 0.0) + eye * jnp.exp(diag_row)) * jnp.exp(gain_row)
    rows = jnp.dot(out_map, low, precision=FINE, preferred_element_type=f32)
    mat = jnp.dot(rows, upp, precision=FINE, preferred_element_type=f32)
    bias = jnp.sum(mat * shift_row, axis=1, keepdims=True)
    if in_map is not None:
        mat = dot_nt(mat, in_map, FINE)
    high, rest = split_two(mat)
    parts = [high, rest] if exact else [high, high, rest]
    return jnp.concatenate(parts, axis=1).astype(bf16), bias


def mapped_column(row, mapping):
    return jnp.sum(mapping * row, axis=1, keepdims=True)


def prepare(p, s):
    steps_mid, channels = p["shift_mid"].shape
    steps_top, top_channels = p["shift_top"].shape
    hidden = p["w2_mid"].shape[1]
    half = channels // 2
    mapping = mid_map(channels)
    natural = eye_map(top_channels)
    for k in range(steps_mid):
        mat, bias = mixing(
            p["lower_mid"][k],
            p["upper_mid"][k],
            p["diag_mid"][k : k + 1, :],
            p["gain_mid"][k : k + 1, :],
            p["shift_mid"][k : k + 1, :],
            mapping,
            None if k == 0 else mapping,
            k == 0,
        )
        s["mix_mid"][k, :, : mat.shape[1]] = mat
        s["mix_bias_mid"][k] = jnp.broadcast_to(bias, (channels, LANES))
        s["b3_mid"][k] = jnp.broadcast_to(
            mapped_column(p["third_bias_mid"][k : k + 1, :], mapping), (channels, LANES)
        )
    for k in range(steps_top):
        mat, bias = mixing(
            p["lower_top"][k],
            p["upper_top"][k],
            p["diag_top"][k : k + 1, :],
            p["gain_top"][k : k + 1, :],
            p["shift_top"][k : k + 1, :],
            natural,
            squeeze_map(top_channels) if k == 0 else None,
            False,
        )
        s["mix_top"][k, :, : mat.shape[1]] = mat
        s["mix_bias_top"][k] = jnp.broadcast_to(bias, (top_channels, LANES))
        s["b3_top"][k] = jnp.broadcast_to(
            mapped_column(p["third_bias_top"][k : k + 1, :], natural), (top_channels, LANES)
        )
    for k in range(steps_mid):
        taps = []
        for tap in range(9):
            extra = [jnp.zeros((16 - half, hidden), f32)]
            if tap == 4:
                row = p["first_bias_mid"][k : k + 1, :].astype(f32)
                extra = [row, jnp.zeros((15 - half, hidden), f32)]
            taps.append(jnp.concatenate([p["w1_mid"][k, tap].astype(f32)] + extra, axis=0))
        s["w1t_mid"][k] = jnp.transpose(jnp.concatenate(taps, axis=0)).astype(bf16)
        s["w2t_mid"][k] = jnp.transpose(p["w2_mid"][k].astype(f32)).astype(bf16)
        s["b2_mid"][k] = jnp.transpose(
            jnp.broadcast_to(p["second_bias_mid"][k : k + 1, :], (LANES, hidden))
        )
        for tap in range(9):
            w = p["w3_mid"][k, tap * channels : (tap + 1) * channels, :].astype(f32)
            w = jnp.concatenate([w[:12], w[20:24], w[12:20]], axis=0)
            s["w3f_mid"][tap * channels : (tap + 1) * channels, :] = w
        s["w3p_mid"][k] = s["w3f_mid"][...].astype(bf16)
    for k in range(steps_top):
        row = p["first_bias_top"][k : k + 1, :].astype(f32)
        w = jnp.concatenate(
            [p["w1_top"][k].astype(f32), row, jnp.zeros((7, hidden), f32)], axis=0
        )
        s["w1t_top"][k] = jnp.transpose(w).astype(bf16)
        s["w2t_top"][k] = jnp.transpose(p["w2_top"][k].astype(f32)).astype(bf16)
        s["b2_top"][k] = jnp.transpose(
            jnp.broadcast_to(p["second_bias_top"][k : k + 1, :], (LANES, hidden))
        )


def wide(x, n):
    return jnp.concatenate([x] * (n // LANES), axis=1)


def lane_of(n):
    return lax.rem(iota((1, n), 1), LANES)


def edge_mid(x, dr):
    lane = iota((1, LANES), 1)
    if dr > 0:
        return keep(roll(x, -32), lane < 96)
    return keep(roll(x, 32), lane >= 32)


def edge_top(x, dr):
    lane = iota((1, LANES), 1)
    odd = lax.rem(lane, 2) == 1
    if dr > 0:
        return jnp.where(odd, keep(roll(x, -31), lane < 96), roll(x, -1))
    return jnp.where(odd, roll(x, 1), keep(roll(x, 31), lane >= 32))


def shift_col(x, dc, stride):
    n = x.shape[1]
    col = lax.rem(iota((1, n), 1), 32)
    if dc > 0:
        return keep(roll(x, -stride), col < 32 - stride)
    return keep(roll(x, stride), col >= stride)


def gather(y_ref, tap_rows, lo, hi, n, edge, stride):
    total = None
    for dc in (0, -1, 1):
        base = 4 + dc
        part = y_ref[base * tap_rows : (base + 1) * tap_rows, lo:hi]
        for dr in (-1, 1):
            tap = base + 3 * dr
            rows = slice(tap * tap_rows, (tap + 1) * tap_rows)
            if dr > 0 and hi == n:
                moved = [edge(y_ref[rows, :LANES], dr)]
                if hi - lo > LANES:
                    moved = [y_ref[rows, lo + LANES : hi]] + moved
                moved = jnp.concatenate(moved, axis=1) if len(moved) > 1 else moved[0]
            elif dr < 0 and lo == 0:
                moved = [edge(y_ref[rows, n - LANES : n], dr)]
                if hi - lo > LANES:
                    moved = moved + [y_ref[rows, : hi - LANES]]
                moved = jnp.concatenate(moved, axis=1) if len(moved) > 1 else moved[0]
            else:
                moved = y_ref[rows, lo + dr * LANES : hi + dr * LANES]
            part = part + moved
        if dc != 0:
            part = shift_col(part, dc, stride)
        total = part if total is None else total + part
    return total


def gated(g):
    e = jnp.exp(-jnp.abs(g))
    inv = 1.0 / (1.0 + e)
    gate = jnp.where(g >= 0, inv, e * inv)
    return gate, jnp.minimum(g, 0.0) - jnp.log(1.0 + e)


def fold(x):
    total = x[:, :LANES]
    for at in range(LANES, x.shape[1], LANES):
        total = total + x[:, at : at + LANES]
    return total


def mix(mat, bias, x, exact):
    n = x.shape[1]
    if exact:
        stack = [x, x]
    else:
        high, rest = split_two(x)
        stack = [high, rest, high]
    stack = jnp.concatenate(stack, axis=0).astype(bf16)
    return jnp.dot(mat, stack, preferred_element_type=f32) + wide(bias, n)


def product(first, second, third, bias, spread, y_ref, rows, lo):
    n = spread.shape[1]
    h = jnp.dot(first[...], spread, preferred_element_type=f32)
    h = jnp.maximum(h, 0.0).astype(bf16)
    h = jnp.dot(second[...], h, preferred_element_type=f32)
    h = jnp.maximum(h + wide(bias[...], n), 0.0).astype(bf16)
    y_ref[:rows, lo : lo + n] = jnp.dot(third[...], h, preferred_element_type=f32)


def mid_step(s, k, exact, mixed=None):
    state, u_ref, q_ref, y_ref = s["state"], s["u"], s["q"], s["y"]
    channels, n = state.shape
    block = 4 * LANES
    sub = iota((8, 1), 0)
    mat = s["mix_mid"][k, :, : (2 if exact else 3) * channels]
    for lo in range(0, n, block):
        u_ref[:, lo : lo + block] = mix(
            mat, s["mix_bias_mid"][k], state[:, lo : lo + block], exact
        )
    if mixed is not None:
        mixed()
    for lo in range(0, n, block):
        q = u_ref[:16, lo : lo + block]
        q = jnp.concatenate([q[:8], jnp.where(sub == 4, 1.0, q[8:])], axis=0)
        for dc in (-1, 0, 1):
            x = q if dc == 0 else shift_col(q, dc, 1)
            q_ref[dc + 1, :, LANES + lo : LANES + lo + block] = x.astype(bf16)
            if lo == 0:
                q_ref[dc + 1, :, LANES + n :] = edge_mid(x[:, :LANES], 1).astype(bf16)
            if lo + block == n:
                q_ref[dc + 1, :, :LANES] = edge_mid(x[:, block - LANES :], -1).astype(bf16)
    for lo in range(0, n, min(CHUNK, n)):
        taps = []
        for dr in (-1, 0, 1):
            at = lo + LANES * (1 + dr)
            for dc in (-1, 0, 1):
                taps.append(q_ref[dc + 1, :, at : at + min(CHUNK, n)])
        product(
            s["w1t_mid"].at[k],
            s["w2t_mid"].at[k],
            s["w3p_mid"].at[k],
            s["b2_mid"].at[k],
            jnp.concatenate(taps, axis=0),
            y_ref,
            9 * channels,
            lo,
        )
    score = None
    width = 2 * LANES
    for lo in range(0, n, width):
        out = gather(y_ref, channels, lo, lo + width, n, edge_mid, 1) + wide(s["b3_mid"][k], width)
        gate, logs = gated(out[:16] + 2.0)
        logs = fold(logs)
        score = logs if score is None else score + logs
        u = u_ref[:, lo : lo + width]
        state[:8, lo : lo + width] = u[:8]
        late = (u[8:16] + out[8:16]) * pltpu.roll(gate[8:16], 4, 0)
        state[8:16, lo : lo + width] = jnp.where(sub < 4, u[8:16], late)
        state[16:, lo : lo + width] = (u[16:] + out[16:]) * gate[:8]
    return keep(score, iota((16, 1), 0) < channels // 2)


def squeeze(s):
    state, top = s["state"], s["top"]
    odd = lax.rem(iota((1, LANES), 1), 2) == 1
    sub = iota((8, 1), 0)
    for v in range(4):
        tails = []
        for i in range(2):
            t = (2 * v + i) * LANES
            a = state[8:, t : t + LANES]
            t = t + 8 * LANES
            b = state[8:, t : t + LANES]
            even_col = jnp.where(odd, roll(b, 1), a)
            odd_col = jnp.where(odd, b, roll(a, -1))
            cols = slice(v * LANES, (v + 1) * LANES)
            top[16 * i : 16 * i + 8, cols] = even_col[8:]
            top[16 * i + 8 : 16 * i + 16, cols] = odd_col[8:]
            top[32 + 8 * i : 40 + 8 * i, cols] = jnp.where(
                sub < 4, pltpu.roll(odd_col[:8], 4, 0), even_col[:8]
            )


def top_step(s, k):
    state, u_ref, q_ref, y_ref = s["top"], s["u_top"], s["q_top"], s["y_top"]
    channels, n = state.shape
    half = channels // 2
    mat = s["mix_top"][k, :, : 3 * channels]
    u_ref[...] = mix(mat, s["mix_bias_top"][k], state[...], False)
    q = u_ref[:half, :]
    for dc in (-1, 0, 1):
        x = q if dc == 0 else shift_col(q, dc, 2)
        q_ref[dc + 1, :, LANES : LANES + n] = x
        q_ref[dc + 1, :, LANES + n :] = edge_top(x[:, :LANES], 1)
        q_ref[dc + 1, :, :LANES] = edge_top(x[:, n - LANES :], -1)
    ones = jnp.where(iota((8, min(CHUNK, n)), 0) == 0, 1.0, 0.0)
    for lo in range(0, n, min(CHUNK, n)):
        taps = []
        for dr in (-1, 0, 1):
            at = lo + LANES * (1 + dr)
            for dc in (-1, 0, 1):
                taps.append(q_ref[dc + 1, :, at : at + min(CHUNK, n)])
        product(
            s["w1t_top"].at[k],
            s["w2t_top"].at[k],
            s["w3_top"].at[k],
            s["b2_top"].at[k],
            jnp.concatenate(taps + [ones], axis=0).astype(bf16),
            y_ref,
            9 * channels,
            lo,
        )
    score = None
    width = LANES
    for lo in range(0, n, width):
        out = gather(y_ref, channels, lo, lo + width, n, edge_top, 2) + wide(s["b3_top"][k], width)
        gate, logs = gated(out[:half] + 2.0)
        score = logs if score is None else score + logs
        state[:half, lo : lo + width] = u_ref[:half, lo : lo + width]
        state[half:, lo : lo + width] = (u_ref[half:, lo : lo + width] + out[half:]) * gate
    return score


def work_scratch(steps_mid, steps_top, hidden, channels, top_channels, cells):
    n_top = cells // 4
    return {
        "mix_mid": pltpu.VMEM((steps_mid, channels, 3 * channels), bf16),
        "mix_bias_mid": pltpu.VMEM((steps_mid, channels, LANES), f32),
        "b3_mid": pltpu.VMEM((steps_mid, channels, LANES), f32),
        "mix_top": pltpu.VMEM((steps_top, top_channels, 3 * top_channels), bf16),
        "mix_bias_top": pltpu.VMEM((steps_top, top_channels, LANES), f32),
        "b3_top": pltpu.VMEM((steps_top, top_channels, LANES), f32),
        "w1t_mid": pltpu.VMEM((steps_mid, hidden, 144), bf16),
        "w2t_mid": pltpu.VMEM((steps_mid, hidden, hidden), bf16),
        "b2_mid": pltpu.VMEM((steps_mid, hidden, LANES), f32),
        "w3f_mid": pltpu.VMEM((9 * channels, hidden), f32),
        "w3p_mid": pltpu.VMEM((steps_mid, 9 * channels, hidden), bf16),
        "w1t_top": pltpu.VMEM((steps_top, hidden, 9 * top_channels // 2 + 8), bf16),
        "w2t_top": pltpu.VMEM((steps_top, hidden, hidden), bf16),
        "b2_top": pltpu.VMEM((steps_top, hidden, LANES), f32),
        "state": pltpu.VMEM((channels, cells), f32),
        "u": pltpu.VMEM((channels, cells), f32),
        "q": pltpu.VMEM((3, 16, cells + 2 * LANES), bf16),
        "y": pltpu.VMEM((9 * channels, cells), f32),
        "top": pltpu.VMEM((top_channels, n_top), f32),
        "u_top": pltpu.VMEM((top_channels, n_top), f32),
        "q_top": pltpu.VMEM((3, top_channels // 2, n_top + 2 * LANES), f32),
        "y_top": pltpu.VMEM((9 * top_channels, n_top), f32),
        "turned": pltpu.VMEM((n_top, LANES), f32),
    }


NAMES = (
    "shift_mid",
    "gain_mid",
    "lower_mid",
    "upper_mid",
    "diag_mid",
    "w1_mid",
    "first_bias_mid",
    "w2_mid",
    "second_bias_mid",
    "w3_mid",
    "third_bias_mid",
    "shift_top",
    "gain_top",
    "lower_top",
    "upper_top",
    "diag_top",
    "w1_top",
    "first_bias_top",
    "w2_top",
    "second_bias_top",
    "w3_top",
    "third_bias_top",
)


def parameters(params):
    (
        shift_mid, gain_mid, lower_mid, upper_mid, diag_mid, first_mid, first_bias_mid, second_mid,
        second_bias_mid, third_mid, third_bias_mid, shift_top, gain_top, lower_top, upper_top,
        diag_top, first_top, first_bias_top, second_top, second_bias_top, third_top, third_bias_top,
    ) = params
    steps_mid, hidden = first_bias_mid.shape
    steps_top = first_bias_top.shape[0]
    w1_top = first_top.reshape(steps_top, -1, hidden)
    w3_mid = third_mid.transpose(0, 1, 3, 2).reshape(steps_mid, -1, hidden)
    w3_top = third_top.transpose(0, 1, 3, 2).reshape(steps_top, -1, hidden)
    return (
        shift_mid, gain_mid, lower_mid, upper_mid, diag_mid, first_mid, first_bias_mid, second_mid,
        second_bias_mid, w3_mid, third_bias_mid, shift_top, gain_top, lower_top, upper_top,
        diag_top, w1_top, first_bias_top, second_top, second_bias_top, w3_top, third_bias_top,
    )


def kernel(dims, keys, *refs):
    n_rows, n_chan, height, width, count = dims
    sources, refs = refs[:count], refs[count:]
    (mid_out, top_out, lik_out), refs = refs[:3], refs[3:]
    held, refs = refs[:count], refs[count:]
    s, refs = dict(zip(keys, refs)), refs[len(keys) :]
    outbox, stage, inbox, z_send, z_recv, w_sem, refs = *refs[:6], refs[6:]
    stage_send, piece_send, stage_sem, hello_sem, piece_sem, z_send_sem, z_recv_sem = refs
    images = held[0]
    p = dict(zip(NAMES, held[1:]))
    s["w3_top"] = p["w3_top"]
    b = lax.axis_index("batch")
    r = lax.axis_index("rows")
    c = lax.axis_index("chan")
    quad = lax.div(r, 2)
    side = lax.rem(r, 2)

    def device(row, chan):
        return {"batch": b, "rows": row, "chan": chan}

    chans = []
    for q in range(n_chan):
        y = q // 2
        chans.append(2 * (y + y // 2 * (5 - 2 * y)) + 1 - q % 2)
    y = lax.div(c, 2)
    spot = 2 * (y + lax.div(y, 2) * (5 - 2 * y)) + 1 - lax.rem(c, 2)

    first = pltpu.make_async_copy(sources[0], held[0], w_sem.at[0])
    first.start()
    barrier = pltpu.get_barrier_semaphore()
    for row in range(1, n_rows):

        @pl.when(row > r)
        def _():
            pl.semaphore_signal(barrier, inc=1, device_id=device(row, c), device_id_type=MESH)

    for q in range(1, n_chan):

        @pl.when(q > spot)
        def _():
            pl.semaphore_signal(
                barrier, inc=1, device_id=device(r, chans[q]), device_id_type=MESH
            )

    first.wait()
    for dest in range(n_chan):
        x = images[dest]
        x = jnp.concatenate([x[:8], x[8:16], x[16:], jnp.zeros((8, width), f32)], axis=1)
        outbox[dest] = pltpu.roll(x, quad * 32, 1).astype(bf16)

    @pl.when(r + spot > 0)
    def _():
        pl.semaphore_wait(barrier, r + spot)

    def send_row(row):
        for part in range(2):
            some = pl.ds(part * n_chan // 2, n_chan // 2)
            pltpu.make_async_remote_copy(
                src_ref=outbox.at[some],
                dst_ref=stage.at[r, some],
                send_sem=stage_send,
                recv_sem=stage_sem.at[part, r],
                device_id=device(row, c),
                device_id_type=MESH,
            ).start()

    def await_part(row, part):
        some = pl.ds(part * n_chan // 2, n_chan // 2)
        await_copy(stage.at[row, some], stage_sem.at[part, row])

    def send_hello(q):
        pltpu.make_async_remote_copy(
            src_ref=outbox.at[chans[q]],
            dst_ref=inbox.at[c, r],
            send_sem=piece_send,
            recv_sem=hello_sem.at[c],
            device_id=device(r, chans[q]),
            device_id_type=MESH,
        ).start()

    def send_piece(row, q):
        pltpu.make_async_remote_copy(
            src_ref=stage.at[row, chans[q]],
            dst_ref=inbox.at[c, row],
            send_sem=piece_send,
            recv_sem=piece_sem.at[c],
            device_id=device(r, chans[q]),
            device_id_type=MESH,
        ).start()

    def await_copy(ref, sem):
        pltpu.make_async_remote_copy(
            src_ref=ref,
            dst_ref=ref,
            send_sem=stage_send,
            recv_sem=sem,
            device_id=device(r, c),
            device_id_type=MESH,
        ).wait_recv()

    pl.when(r > 0)(functools.partial(send_row, 0))
    for q in range(n_chan - 1):
        pl.when(q < spot)(functools.partial(send_hello, q))
    copies = []
    for at in range(1, count):
        copy = pltpu.make_async_copy(sources[at], held[at], w_sem.at[at])
        copy.start()
        copies.append(copy)
    stage[r] = outbox[...]
    copies[0].wait()
    for row in range(1, n_rows - 1):
        pl.when(row < r)(functools.partial(send_row, row))
    for copy in copies[1:]:
        copy.wait()
    prepare(p, s)
    channels = p["shift_mid"].shape[1]
    top_channels = p["shift_top"].shape[1]
    half = channels // 2
    cells = height * width
    fixed = cells * (jnp.sum(p["gain_mid"][...]) + jnp.sum(p["diag_mid"][...]))
    fixed = fixed + cells // 4 * (jnp.sum(p["gain_top"][...]) + jnp.sum(p["diag_top"][...]))
    fixed = fixed - 0.5 * log_two_pi * channels * cells

    for row in range(1, n_rows):

        @pl.when(row > r)
        def _():
            await_part(row, 0)
            send_row(row)
            for q in range(n_chan - 1):
                if q == n_chan // 2:
                    await_part(row, 1)
                pl.when(q < spot)(functools.partial(send_piece, row, q))

    for q in range(1, n_chan):

        @pl.when(q > spot)
        def _():
            await_copy(inbox.at[chans[q], 0], hello_sem.at[chans[q]])
            send_hello(q)
            for row in range(1, n_rows):
                pl.when(row > r)(functools.partial(send_piece, row, q))

    for row in range(n_rows - 1):

        @pl.when(row < r)
        def _():
            await_part(row, 0)
            for q in range(n_chan):
                if q == n_chan // 2:
                    await_part(row, 1)
                pl.when(q != spot)(functools.partial(send_piece, row, q))

    for row in range(n_rows):
        inbox[c, row] = stage[row, c]
    for q in range(n_chan):

        @pl.when(q < spot)
        def _():
            await_copy(inbox.at[chans[q], 0], hello_sem.at[chans[q]])

        @pl.when(q != spot)
        def _():
            await_copy(inbox.at[chans[q], pl.ds(0, n_rows - 1)], piece_sem.at[chans[q]])

    state = s["state"]
    lane = iota((1, LANES), 1)
    for t in range(height // 4):
        letters = [inbox[t % 8, 2 * k + t // 8].astype(f32) for k in range(4)]
        for slab in range(3):
            x = letters[(3 - slab) % 4]
            for k in range(3):
                x = jnp.where(lax.div(lane, 32) == k, letters[(k - slab) % 4], x)
            state[8 * slab : 8 * slab + 8, t * LANES : (t + 1) * LANES] = roll(x, -32 * slab)

    z_copies = []

    def send_latent():
        for to in range(n_chan):
            start = pl.multiple_of((side * n_chan + to) * LANES, LANES)
            z = s["u"][:16, pl.ds(start, LANES)]
            z_send[to] = jnp.where(
                lane < 32,
                pltpu.roll(z[:8], LANES - quad * 32, 1),
                pltpu.roll(z[8:], LANES + 32 - quad * 32, 1),
            )
        for d in range(1, n_chan):
            other = lax.rem(c + d, n_chan)
            copy = pltpu.make_async_remote_copy(
                src_ref=z_send.at[other],
                dst_ref=z_recv.at[c],
                send_sem=z_send_sem.at[d],
                recv_sem=z_recv_sem.at[d],
                device_id=device(r, other),
                device_id_type=MESH,
            )
            copy.start()
            z_copies.append(copy)
        z_recv[c] = z_send[c]

    score = None
    last = p["shift_mid"].shape[0] - 1
    for k in range(last + 1):
        logs = mid_step(s, k, k == 0, send_latent if k == last else None)
        score = logs if score is None else score + logs

    squares = fold(state[:16, :] * state[:16, :])
    score = score - 0.5 * keep(squares, iota((16, 1), 0) < half)
    squeeze(s)
    score_top = None
    for k in range(p["shift_top"].shape[0]):
        logs = top_step(s, k)
        score_top = logs if score_top is None else score_top + logs
    top = s["top"]
    squares = fold(top[...] * top[...])
    total = jnp.sum(score, axis=0, keepdims=True) + jnp.sum(score_top, axis=0, keepdims=True)
    total = total - 0.5 * jnp.sum(squares, axis=0, keepdims=True)
    total = jnp.sum(total, axis=1, keepdims=True)
    lik_out[...] = jnp.broadcast_to((total + fixed) / (channels * cells), (8, LANES))
    turned = s["turned"]
    for v in range(4):
        turned[v * LANES : (v + 1) * LANES, :top_channels] = jnp.transpose(
            top[:, v * LANES : (v + 1) * LANES]
        )
    for v in range(4):
        start = v * LANES + quad * 32 + side
        top_out[0, v * 16 : (v + 1) * 16, :] = turned[pl.ds(start, 16, stride=2), :][
            :, :top_channels
        ]

    for d in range(1, n_chan):
        pltpu.make_async_remote_copy(
            src_ref=z_send.at[0],
            dst_ref=z_recv.at[lax.rem(c + n_chan - d, n_chan)],
            send_sem=z_send_sem.at[d],
            recv_sem=z_recv_sem.at[d],
            device_id=device(r, c),
            device_id_type=MESH,
        ).wait_recv()
    for img in range(n_chan):
        z = z_recv[img]
        mid_out[img, :8, :] = z[:, :width]
        mid_out[img, 8:, :] = z[:4, width : 2 * width]
    for copy in z_copies:
        copy.wait_send()
    for ref, sem in (
        (stage.at[pl.ds(0, n_rows - 1)], stage_send),
        (inbox.at[pl.ds(0, n_chan - 1)], piece_send),
    ):
        pltpu.make_async_remote_copy(
            src_ref=ref,
            dst_ref=ref,
            send_sem=sem,
            recv_sem=hello_sem.at[0],
            device_id=device(r, c),
            device_id_type=MESH,
        ).wait_send()


def deliver(mid, top, lik, mid_out, top_out, lik_out):
    for img in range(mid.shape[0]):
        mid_out[img, :, 0, :] = mid[img]
    top_out[...] = top[...]
    lik_out[...] = lik[0, :1]


def body(sizes, images, *params):
    n_rows, n_chan = sizes
    n_imgs, channels, own_rows, width = images.shape
    peers = n_rows * n_chan
    height = own_rows * peers
    params = parameters(params)
    hidden = params[6].shape[1]
    steps_mid, steps_top = params[0].shape[0], params[11].shape[0]
    top_channels = params[11].shape[1]
    half = channels // 2
    cells = height * width
    own = cells // 4 // n_rows
    operands = (images.reshape(n_imgs, channels, width),) + params
    vmem = pl.BlockSpec(memory_space=pltpu.VMEM)
    count = len(operands)
    work = work_scratch(steps_mid, steps_top, hidden, channels, top_channels, cells)
    mid, top, lik = pl.pallas_call(
        functools.partial(kernel, (n_rows, n_chan, height, width, count), list(work)),
        out_shape=(
            pltpu.VMEM((n_imgs, half, width), f32),
            pltpu.VMEM((1, own, top_channels), f32),
            pltpu.VMEM((8, LANES), f32),
        ),
        in_specs=[pl.BlockSpec(memory_space=pl.ANY)] * count,
        out_specs=(vmem, vmem, vmem),
        scratch_shapes=[pltpu.VMEM(x.shape, x.dtype) for x in operands]
        + list(work.values())
        + [
            pltpu.VMEM((n_chan, 8, LANES), bf16),
            pltpu.VMEM((n_rows, n_chan, 8, LANES), bf16),
            pltpu.VMEM((n_chan, n_rows, 8, LANES), bf16),
            pltpu.VMEM((n_chan, 8, LANES), f32),
            pltpu.VMEM((n_chan, 8, LANES), f32),
            pltpu.SemaphoreType.DMA((count,)),
            pltpu.SemaphoreType.DMA,
            pltpu.SemaphoreType.DMA,
            pltpu.SemaphoreType.DMA((2, n_rows)),
            pltpu.SemaphoreType.DMA((n_chan,)),
            pltpu.SemaphoreType.DMA((n_chan,)),
            pltpu.SemaphoreType.DMA((n_chan,)),
            pltpu.SemaphoreType.DMA((n_chan,)),
        ],
        compiler_params=pltpu.CompilerParams(
            collective_id=0,
            has_side_effects=True,
            vmem_limit_bytes=56 * 1024 * 1024,
        ),
        name="flow",
    )(*operands)
    latent_mid, top, lik = pl.pallas_call(
        deliver,
        out_shape=(
            jax.ShapeDtypeStruct((n_imgs, half, own_rows, width), f32),
            jax.ShapeDtypeStruct(top.shape, f32),
            jax.ShapeDtypeStruct((1,), f32),
        ),
        in_specs=[vmem, vmem, vmem],
        out_specs=(vmem, vmem, vmem),
        compiler_params=pltpu.CompilerParams(vmem_limit_bytes=4 * 1024 * 1024),
        name="deliver",
    )(mid, top, lik)
    latent_top = top.reshape(1, -1, width // 2, top_channels).transpose(0, 3, 1, 2)
    return latent_mid, latent_top, lik


def solution(mesh):
    sizes = (mesh.shape["rows"], mesh.shape["chan"])
    placed = (P("batch", None, ("rows", "chan"), None),) + (P(),) * 22
    return jax.shard_map(
        functools.partial(body, sizes),
        mesh=mesh,
        in_specs=placed,
        out_specs=(
            P("batch", None, ("rows", "chan"), None),
            P(("batch", "chan"), None, "rows", None),
            P(("batch", "chan")),
        ),
        check_vma=False,
    )
```
